32 devices in a mesh: gx: 2 (over x), gy: 4 (over y, core), gz: 4 (over z).
Axes of the slice: x: 2, y: 2, z: 4, core: 2. Of those that a mesh axis runs over, the one named last changes fastest.
Arguments:
- charges: bfloat16 [8, 16, 16, 32, 128], P('gx', 'gy', 'gz'), may hold values from -6 to 6
- counts: int32 [8, 16, 16], P('gx', 'gy', 'gz'), may hold values from 32 to 128, as said below
- near_offsets: int32 [27, 3], replicated, may hold values from -1 to 1, as said below
- near_blocks: bfloat16 [27, 128, 128], replicated, may hold values from -0.109375 to 0.109375
- leaf_basis: bfloat16 [48, 128], replicated, may hold values from -0.5 to 0.5
- transfer: bfloat16 [8, 48, 48], replicated, may hold values from -0.625 to 0.625
- far_offsets: int32 [2, 32, 3], replicated, may hold values from -2 to 2, as said below
- coupling: bfloat16 [2, 32, 48, 48], replicated, may hold values from -0.15625 to 0.15625
- coarse_coupling: bfloat16 [2, 4, 4, 48, 48], replicated, may hold values from -0.3125 to 0.3125
Outputs:
- potentials: float32 [8, 16, 16, 32, 128], P('gx', 'gy', 'gz')
The draws below stay inside these ranges and needn't reach their ends.
Inputs may be any that keep to these rules, and one draw needn't show every extreme that they name: `counts`: in each device's block of 4 x 4 x 4 leaf boxes some box holds 128 points. `near_offsets`: each of the 27 offsets with components in -1, 0, 1 appears once. `far_offsets`: each level lists 32 distinct offsets whose largest component in magnitude is 2.
All inputs are finite; a program needn't handle non-finite values.
Results may differ from the reference program's by a relative error of at most 0.008.
Values may be sent and summed in bfloat16 or wider, within the bound.
No kernel may reach another device: no remote copies, remote signals or barrier semaphores. Data moves between devices by JAX's collectives and lax.ppermute only.
A program may use at most 128 MiB of HBM per device.

```python
import jax
import jax.numpy as jnp
import numpy as np
from jax import lax

PTS = 128
RANK = 48
RHS = 32
STENCIL = 27
LIST = 32
BX = 4
BY = 4
BZ = 4
LX = 8
LY = 16
LZ = 16
CGX = 2
CGY = 4
CGZ = 4


def candidate_table():
    entries = []
    for first in range(-2, 3):
        for second in range(-2, 3):
            for third in range(-2, 3):
                if max(abs(first), abs(second), abs(third)) == 2:
                    entries.append([first, second, third])
    return np.array(entries, dtype=np.int32)


def draw_counts(key, part):
    base = jax.random.randint(jax.random.fold_in(key, 1), (LX, LY, LZ), PTS // 4, PTS + 1)
    chosen = jax.random.randint(jax.random.fold_in(key, 2), (LX // BX, LY // BY, LZ // BZ), 0, BX * BY * BZ)
    spread = jnp.repeat(jnp.repeat(jnp.repeat(chosen, BX, axis=0), BY, axis=1), BZ, axis=2)
    pos_x = (jnp.arange(LX, dtype=jnp.int32) % BX)[:, None, None]
    pos_y = (jnp.arange(LY, dtype=jnp.int32) % BY)[None, :, None]
    pos_z = (jnp.arange(LZ, dtype=jnp.int32) % BZ)[None, None, :]
    within = (pos_x * BY + pos_y) * BZ + pos_z
    return jnp.where(within == spread, PTS, base).astype(jnp.int32)


def draw_near_offsets(key, part):
    order = jax.random.permutation(jax.random.fold_in(key, 3), 27).astype(jnp.int32)
    return jnp.stack([order // 9 - 1, order // 3 % 3 - 1, order % 3 - 1], axis=1).astype(jnp.int32)


def draw_far_offsets(key, part):
    table = jnp.asarray(candidate_table())
    levels = []
    for level in range(2):
        picked = jax.random.permutation(jax.random.fold_in(key, 10 + level), table.shape[0])[:LIST]
        levels.append(table[picked])
    return jnp.stack(levels).astype(jnp.int32)


def block_levels(stream_key, extent, cuts, least, largest):
    factor_of, own = 1.0, jax.random.fold_in(stream_key, 6)
    for position, parts in cuts:
        draws = jnp.exp(jax.random.uniform(jax.random.fold_in(own, position), (parts,), jnp.float32, least / len(cuts), largest / len(cuts)))
        factor_of = factor_of * jnp.repeat(draws, extent[position] // parts).reshape([-1 if axis == position else 1 for axis in range(len(extent))])
    return factor_of


def centred(key, extent, deviation, limit, cuts=(), kind=jnp.bfloat16):
    values = jax.random.normal(key, extent, jnp.float32) * deviation
    if len(cuts) > 0:
        values = block_levels(key, extent, cuts, -0.22, 0.18) * values
    return jnp.clip(values, min=-limit, max=limit).astype(kind)


def setup_inputs(seed: int = 0) -> dict:
    arg_keys = jax.random.split(jax.random.key(seed), 10)
    charges = centred(arg_keys[0], (LX, LY, LZ, RHS, PTS), 1.0, 6.0, ((0, 2), (1, 4), (2, 4)))
    counts = draw_counts(jax.random.fold_in(arg_keys[9], 71), 0)
    near_offsets = draw_near_offsets(jax.random.fold_in(arg_keys[9], 71), 0)
    near_blocks = centred(arg_keys[3], (STENCIL, PTS, PTS), (STENCIL * PTS) ** -0.5, 0.109375)
    leaf_basis = centred(arg_keys[4], (RANK, PTS), PTS ** -0.5, 0.5)
    transfer = centred(arg_keys[5], (8, RANK, RANK), (2 * RANK) ** -0.5, 0.625)
    far_offsets = draw_far_offsets(jax.random.fold_in(arg_keys[9], 71), 0)
    coupling = centred(arg_keys[7], (2, LIST, RANK, RANK), (LIST * RANK) ** -0.5, 0.15625)
    coarse_coupling = centred(arg_keys[8], (CGX, CGY, CGZ, RANK, RANK), (CGX * CGY * CGZ * RANK // 4) ** -0.5, 0.3125)
    return {"charges": charges, "counts": counts, "near_offsets": near_offsets, "near_blocks": near_blocks, "leaf_basis": leaf_basis, "transfer": transfer, "far_offsets": far_offsets, "coupling": coupling, "coarse_coupling": coarse_coupling}


def shifted(field, offset):
    return jnp.roll(field, (-offset[0], -offset[1], -offset[2]), axis=(0, 1, 2))


def upward(moments, transfer):
    first_len, second_len, third_len, rank_count, columns = moments.shape
    split = moments.astype(jnp.float32).reshape(first_len // 2, 2, second_len // 2, 2, third_len // 2, 2, rank_count, columns)
    kids = split.transpose(0, 2, 4, 1, 3, 5, 6, 7).reshape(first_len // 2, second_len // 2, third_len // 2, 8, rank_count, columns)
    return jnp.einsum("ckj,xyzcjr->xyzkr", transfer.astype(jnp.float32), kids).astype(jnp.bfloat16)


def downward(parent, transfer):
    rounded = lax.optimization_barrier(parent.astype(jnp.bfloat16)).astype(jnp.float32)
    kids = jnp.einsum("cjk,xyzjr->xyzckr", transfer.astype(jnp.float32), rounded)
    first_len, second_len, third_len, rank_count, columns = parent.shape
    split = kids.reshape(first_len, second_len, third_len, 2, 2, 2, rank_count, columns)
    return split.transpose(0, 3, 1, 4, 2, 5, 6, 7).reshape(2 * first_len, 2 * second_len, 2 * third_len, rank_count, columns)


def couple_level(moments, offsets, matrices):
    wide = moments.astype(jnp.float32)
    mats = matrices.astype(jnp.float32)

    def step(total, index):
        moved = shifted(wide, offsets[index])
        return total + jnp.einsum("kj,xyzjr->xyzkr", mats[index], moved), None

    start = jnp.zeros(moments.shape, jnp.float32)
    total, unused = lax.scan(step, start, jnp.arange(offsets.shape[0], dtype=jnp.int32))
    return total


def coarse_level(moments, coarse_coupling):
    grid_x, grid_y, grid_z = moments.shape[:3]
    wide = moments.astype(jnp.float32)
    mats = coarse_coupling.astype(jnp.float32)

    def step(total, number):
        off_x = number // (grid_y * grid_z)
        off_y = (number // grid_z) % grid_y
        off_z = number % grid_z
        moved = jnp.roll(wide, (-off_x, -off_y, -off_z), axis=(0, 1, 2))
        return total + jnp.einsum("kj,xyzjr->xyzkr", mats[off_x, off_y, off_z], moved), None

    start = jnp.zeros(moments.shape, jnp.float32)
    total, unused = lax.scan(step, start, jnp.arange(grid_x * grid_y * grid_z, dtype=jnp.int32))
    return total


def reference(charges, counts, near_offsets, near_blocks, leaf_basis, transfer, far_offsets, coupling, coarse_coupling):
    capacity = charges.shape[4]
    live = (jnp.arange(capacity, dtype=jnp.int32) < counts[..., None]).astype(jnp.bfloat16)
    masked = charges * live[:, :, :, None, :]
    masked_wide = masked.astype(jnp.float32)
    blocks = near_blocks.astype(jnp.float32)

    def near_step(total, index):
        moved = shifted(masked_wide, near_offsets[index])
        return total + jnp.einsum("xyzrq,pq->xyzrp", moved, blocks[index]), None

    near, unused = lax.scan(near_step, jnp.zeros(charges.shape, jnp.float32), jnp.arange(near_offsets.shape[0], dtype=jnp.int32))
    basis = leaf_basis.astype(jnp.float32)
    moments_zero = jnp.einsum("kp,xyzrp->xyzkr", basis, masked_wide).astype(jnp.bfloat16)
    moments_one = upward(moments_zero, transfer)
    moments_two = upward(moments_one, transfer)
    local_zero = couple_level(moments_zero, far_offsets[0], coupling[0])
    local_one = couple_level(moments_one, far_offsets[1], coupling[1])
    local_two = coarse_level(moments_two, coarse_coupling)
    total_one = local_one + downward(local_two, transfer)
    total_zero = local_zero + downward(total_one, transfer)
    rounded = lax.optimization_barrier(total_zero.astype(jnp.bfloat16)).astype(jnp.float32)
    far = jnp.einsum("kp,xyzkr->xyzrp", basis, rounded)
    return (near + far) * live[:, :, :, None, :].astype(jnp.float32)
```

```python
import functools

import jax
import jax.numpy as jnp
from jax import lax
from jax.experimental import pallas as pl
from jax.experimental.pallas import tpu as pltpu
from jax.sharding import PartitionSpec as P


F32 = jnp.float32
BF16 = jnp.bfloat16
VMEM_LIMIT = 48 * 1024 * 1024


def from_shift(value, axis, size, shift):
    return lax.ppermute(value, axis, [(i, (i - shift) % size) for i in range(size)])


def spec_vmem():
    return pl.BlockSpec(memory_space=pltpu.VMEM)


def spec_smem():
    return pl.BlockSpec(memory_space=pltpu.SMEM)


def run(kernel, out_shape, args, smem=(), scratch=(), name=None):
    return pl.pallas_call(
        kernel,
        out_shape=out_shape,
        in_specs=[spec_smem() if i in smem else spec_vmem() for i in range(len(args))],
        out_specs=jax.tree.map(lambda _: spec_vmem(), out_shape),
        scratch_shapes=scratch,
        compiler_params=pltpu.CompilerParams(vmem_limit_bytes=VMEM_LIMIT),
        name=name,
    )(*args)


def lane_blocks(rows, width):
    return lax.broadcasted_iota(jnp.int32, (rows, 128), 1) // width


def roll(value, shift):
    shift = shift % 128
    return value if shift == 0 else pltpu.roll(value, shift, 1)


def dot(a, b, dims=((1,), (0,))):
    return lax.dot_general(a, b, (dims, ((), ())), preferred_element_type=F32)


def assemble(sources, width, load):
    per = 128 // width
    out = []
    for start in range(0, len(sources), per):
        total = None
        for d, (key, b) in enumerate(sources[start : start + per]):
            moved = roll(load(key).astype(F32), width * (d - b))
            if total is None:
                total = moved
                blocks = lane_blocks(moved.shape[0], width)
            else:
                total = jnp.where(blocks == d, moved, total)
        out.append(total.astype(BF16))
    return out


def mask_kernel(counts, charges, own, high, low):
    bx, by, bz, rhs, pts = charges.shape
    lane = lax.broadcasted_iota(jnp.int32, (rhs, pts), 1)
    for x in range(bx):
        for y in range(by):
            for z in range(bz):
                keep = lane < counts[x, y, z]
                value = jnp.where(keep, charges[x, y, z].astype(F32), 0.0).astype(BF16)
                own[z, y, x] = value
                if z == 0:
                    low[y, x] = value
                if z == bz - 1:
                    high[y, x] = value


def moment_kernel(own, basis, transfer, mom):
    bz, by, bx, rhs, pts = own.shape
    rank = basis.shape[0]
    width = rhs
    leaf = {}
    for z in range(bz):
        for y in range(0, by, 2):
            rows = own[z, y : y + 2].reshape(2 * bx * rhs, pts)
            value = dot(basis[...], rows, ((1,), (1,))).astype(BF16)
            for k in range(2):
                leaf[z, y + k] = value[:, 128 * k : 128 * (k + 1)]
                mom[z * by + y + k] = leaf[z, y + k]
    sums = [None, None]
    for i in range(2):
        for j in range(2):
            for l in range(2):
                rhs_cols = jnp.concatenate(
                    [leaf[2 * z + l, 2 * y + j] for z in range(bz // 2) for y in range(by // 2)], axis=1
                )
                part = dot(transfer[4 * i + 2 * j + l], rhs_cols)
                sums[i] = part if sums[i] is None else sums[i] + part
    blocks = lane_blocks(rank, width)
    first = bz * by
    one = []
    for z in range(bz // 2):
        whole = []
        for y in range(by // 2):
            at = 128 * (z * (by // 2) + y)
            whole.append(sums[0][:, at : at + 128] + roll(sums[1][:, at : at + 128], -width))
        packed = jnp.where(
            blocks == 0,
            whole[0],
            jnp.where(
                blocks == 1,
                roll(whole[0], -width),
                jnp.where(blocks == 2, roll(whole[1], 2 * width), roll(whole[1], width)),
            ),
        ).astype(BF16)
        one.append(packed)
        mom[first + z] = packed
    two = None
    for j in range(2):
        for i in range(2):
            part = dot(transfer[4 * i + 2 * j], one[0]) + dot(transfer[4 * i + 2 * j + 1], one[1])
            part = roll(part, -width * (2 * j + i))
            two = part if two is None else two + part
    mom[first + bz // 2] = two.astype(BF16)


def pack_z_kernel(geo, *refs):
    nx, xs, bz, by, width = geo["nx"], geo["xs"], geo["bz"], geo["by"], geo["width"]
    sources = refs[:xs]
    far = refs[xs : xs + geo["extra_x"]]
    high, low, two = refs[xs + geo["extra_x"] :]
    leaf = bz * by
    at = 0
    for s in sources:
        for z in range(2):
            for y in range(by):
                high[at] = s[(bz - 2 + z) * by + y]
                low[at] = s[z * by + y]
                at += 1
    for s in sources:
        for z in range(2):
            high[at] = s[leaf + z]
            low[at] = s[leaf + z]
            at += 1

    def load(key):
        if key == 0:
            return sources[0][leaf + 2]
        if key == 1:
            return sources[xs - 1][leaf + 2]
        if key == nx - 1:
            return sources[1][leaf + 2]
        return far[key - 2][...]

    for t, tile in enumerate(assemble([(k, 0) for k in range(nx)], width, load)):
        high[at + t] = tile
        low[at + t] = tile
        two[t] = tile


def pack_y_kernel(geo, *refs):
    nz, nx, xs, bz, by, width = geo["nz"], geo["nx"], geo["xs"], geo["bz"], geo["by"], geo["width"]
    sources = refs[:xs]
    prev, nxt, mine = refs[xs : xs + 3]
    far = refs[xs + 3 : xs + 3 + geo["extra_z"]]
    high, low, two = refs[xs + 3 + geo["extra_z"] :]
    leaf = bz * by
    at = 0
    for k, s in enumerate(sources):
        for z in range(-2, bz + 2):
            for y in range(2):
                for out, yy in ((high, by - 2 + y), (low, y)):
                    if z < 0:
                        out[at] = prev[k * 2 * by + (z + 2) * by + yy]
                    elif z >= bz:
                        out[at] = nxt[k * 2 * by + (z - bz) * by + yy]
                    else:
                        out[at] = s[z * by + yy]
                at += 1
    for k, s in enumerate(sources):
        for zb in range(3):
            for z in range(2):
                if zb == 1:
                    tile = s[leaf + z]
                else:
                    tile = (prev if zb == 0 else nxt)[xs * 2 * by + k * 2 + z]
                high[at] = tile
                low[at] = tile
                at += 1
    base = xs * 2 * by + xs * 2
    per = 128 // width
    order = [((s, b // per), b % per) for s in range(nz) for b in range(nx)]

    def load(key):
        s, t = key
        if s == 0:
            return mine[t]
        if s == 1:
            return nxt[base + t]
        if s == nz - 1:
            return prev[base + t]
        return far[s - 2][t]

    for t, tile in enumerate(assemble(order, width, load)):
        high[at + t] = tile
        low[at + t] = tile
        two[t] = tile


def pack_charge_x_kernel(own, prev, nxt, high, low):
    bz, by, bx = own.shape[:3]
    for y in range(by):
        high[0, y] = prev[y, bx - 1]
        low[0, y] = prev[y, 0]
        high[bz + 1, y] = nxt[y, bx - 1]
        low[bz + 1, y] = nxt[y, 0]
        for z in range(bz):
            high[z + 1, y] = own[z, y, bx - 1]
            low[z + 1, y] = own[z, y, 0]


def pack_charge_y_kernel(own, prev, nxt, before, after, high, low):
    bz, by, bx = own.shape[:3]
    for out, y in ((high, by - 1), (low, 0)):
        for z in range(bz + 2):
            out[z, 0] = before[z, y]
            out[z, bx + 1] = after[z, y]
            for x in range(bx):
                if z == 0:
                    out[z, x + 1] = prev[y, x]
                elif z == bz + 1:
                    out[z, x + 1] = nxt[y, x]
                else:
                    out[z, x + 1] = own[z - 1, y, x]


def final_kernel(geo, *refs):
    nx, ny, nz, xs = geo["nx"], geo["ny"], geo["nz"], geo["xs"]
    bx, by, bz, rhs, rank, width = geo["bx"], geo["by"], geo["bz"], geo["rhs"], geo["rank"], geo["width"]
    it = iter(refs)

    def take(count):
        return [next(it) for _ in range(count)]

    counts, near_offsets, far_offsets = take(3)
    near_blocks, basis, coupling, coarse, down_one, down_zero = take(6)
    own, cz_prev, cz_next, cx_prev, cx_next, cy_prev, cy_next = take(7)
    sources = take(xs)
    mz_prev, mz_next, my_prev, my_next, mine_two = take(5)
    far_two = take(geo["extra_y"])
    (out,) = take(1)
    wide, shifts, ones, columns, local = take(5)
    leaf = bz * by
    blocks = lane_blocks(rank, width)

    for z in range(bz + 2):
        for y in range(by + 2):
            if y == 0 or y == by + 1:
                wide[z, y] = (cy_prev if y == 0 else cy_next)[z].reshape((bx + 2) * rhs, wide.shape[3])
                continue
            if z == 0:
                middle = cz_prev[y - 1]
            elif z == bz + 1:
                middle = cz_next[y - 1]
            else:
                middle = own[z - 1, y - 1]
            wide[z, y, 0:rhs] = cx_prev[z, y - 1]
            wide[z, y, rhs : (bx + 1) * rhs] = middle.reshape(bx * rhs, wide.shape[3])
            wide[z, y, (bx + 1) * rhs :] = cx_next[z, y - 1]

    def leaf_tile(k, z, y):
        if y < 0:
            return my_prev[k * 2 * (bz + 4) + (z + 2) * 2 + y + 2]
        if y >= by:
            return my_next[k * 2 * (bz + 4) + (z + 2) * 2 + y - by]
        if z < 0:
            return mz_prev[k * 2 * by + (z + 2) * by + y]
        if z >= bz:
            return mz_next[k * 2 * by + (z - bz) * by + y]
        return sources[k][z * by + y]

    for z in range(-2, bz + 2):
        for y in range(-2, by + 2):
            mid = leaf_tile(0, z, y)
            shifts[2, z + 2, y + 2] = mid
            mid = mid.astype(F32)
            before = leaf_tile(1, z, y).astype(F32)
            after = before if xs == 2 else leaf_tile(2, z, y).astype(F32)
            shifts[0, z + 2, y + 2] = roll(jnp.where(blocks >= 2, before, mid), 2 * width).astype(BF16)
            shifts[1, z + 2, y + 2] = roll(jnp.where(blocks >= 3, before, mid), width).astype(BF16)
            shifts[3, z + 2, y + 2] = roll(jnp.where(blocks < 1, after, mid), -width).astype(BF16)
            shifts[4, z + 2, y + 2] = roll(jnp.where(blocks < 2, after, mid), -2 * width).astype(BF16)

    def one_tile(k, zb, z, yb):
        if yb != 1:
            at = xs * 2 * (bz + 4) + (k * 3 + zb) * 2 + z
            return (my_prev if yb == 0 else my_next)[at]
        if zb != 1:
            return (mz_prev if zb == 0 else mz_next)[xs * 2 * by + k * 2 + z]
        return sources[k][leaf + z]

    odd = blocks % 2 == 1
    upper = blocks >= 2

    def swap(value):
        return jnp.where(odd, roll(value, width), roll(value, -width))

    for zb in range(3):
        for z in range(2):
            rows = []
            for yb in range(3):
                mid = one_tile(0, zb, z, yb).astype(F32)
                before = one_tile(1, zb, z, yb).astype(F32)
                after = before if xs == 2 else one_tile(2, zb, z, yb).astype(F32)
                rows.append([
                    before,
                    swap(jnp.where(odd, before, mid)),
                    mid,
                    swap(jnp.where(odd, mid, after)),
                    after,
                ])
            for k in range(5):
                low, mid, high = (rows[yb][k] for yb in range(3))
                group = [
                    low,
                    roll(jnp.where(upper, low, mid), 2 * width),
                    mid,
                    roll(jnp.where(upper, mid, high), 2 * width),
                    high,
                ]
                for m in range(5):
                    ones[k, m, 2 * zb + z] = group[m].astype(BF16)

    base = xs * 2 * (bz + 4) + xs * 6
    per = 128 // width

    def two_tile(s, t):
        if s == 0:
            return mine_two[t]
        if s == 1:
            return my_next[base + t]
        if s == ny - 1:
            return my_prev[base + t]
        return far_two[s - 2][t]

    stacked = []
    for s in range(ny):
        for b in range(nz * nx):
            tile = two_tile(s, b // per).astype(F32)
            stacked.append(jnp.where(blocks == b % per, tile, 0.0).astype(BF16))
    two = dot(coarse[...], jnp.concatenate(stacked, axis=0))
    two = two + roll(two, 2 * width)
    two = (two + roll(two, width)).astype(BF16)

    entries = far_offsets.shape[1]
    for e in range(entries):
        ox, oy, oz = (far_offsets[1, e, d] + 2 for d in range(3))
        for z in range(2):
            columns[e * rank : (e + 1) * rank, 128 * z : 128 * (z + 1)] = ones[ox, oy, z + oz]
    local_one = dot(coupling[1], columns[...])
    from_two = dot(down_one[...], two)
    ups = []
    for z in range(2):
        total = local_one[:, 128 * z : 128 * (z + 1)]
        for j in range(2):
            for i in range(2):
                child = 4 * i + 2 * j + z
                part = from_two[child * rank : (child + 1) * rank]
                total = total + jnp.where(blocks == 2 * j + i, part, 0.0)
        total = total.astype(BF16).astype(F32)
        half = roll(total, 2 * width)
        for up in (
            jnp.where(blocks == 0, total, jnp.where(blocks == 3, half, roll(total, width))),
            jnp.where(blocks == 0, half, jnp.where(blocks == 3, total, roll(total, -width))),
        ):
            ups.append(
                jnp.concatenate(
                    [jnp.where(odd, 0.0, up).astype(BF16), jnp.where(odd, up, 0.0).astype(BF16)], axis=0
                )
            )
    ups = jnp.concatenate(ups, axis=1)
    for j in range(2):
        for l in range(2):
            part = dot(down_zero[2 * j + l], ups)
            for z in range(2):
                for y in range(2):
                    at = 128 * (2 * z + y)
                    local[2 * z + l, 2 * y + j] = part[:, at : at + 128]

    lane = lax.broadcasted_iota(jnp.int32, (rhs, 128), 1)
    weights = jnp.concatenate([near_blocks[s] for s in range(near_blocks.shape[0])], axis=1)

    def step(number, carry):
        z = number // (by // 2)
        y = number % (by // 2) * 2
        for e in range(entries):
            ox, oy, oz = (far_offsets[0, e, d] + 2 for d in range(3))
            for k in range(2):
                columns[e * rank : (e + 1) * rank, 128 * k : 128 * (k + 1)] = shifts[ox, z + oz, y + oy + k]
        total = dot(coupling[0], columns[...])
        total = total + jnp.concatenate([local[z, y], local[z, y + 1]], axis=1)
        result = dot(total.astype(BF16), basis[...], ((0,), (0,)))
        windows = []
        for s in range(near_blocks.shape[0]):
            ox, oy, oz = (near_offsets[s, d] + 1 for d in range(3))
            start = pl.multiple_of(ox * rhs, rhs)
            windows.append(
                wide[z + oz, pl.ds(y + oy, 2), pl.ds(start, bx * rhs), :].reshape(2 * bx * rhs, wide.shape[3])
            )
        result = result + dot(jnp.concatenate(windows, axis=1), weights, ((1,), (1,)))
        for k in range(2):
            for x in range(bx):
                at = (k * bx + x) * rhs
                keep = lane < counts[x, y + k, z]
                out[x, y + k, z] = jnp.where(keep, result[at : at + rhs], 0.0)
        return carry

    lax.fori_loop(0, bz * by // 2, step, 0)


def body(charges, counts, near_offsets, near_blocks, leaf_basis, transfer, far_offsets, coupling, coarse_coupling):
    bx, by, bz, rhs, pts = charges.shape
    rank = leaf_basis.shape[0]
    nx, ny, nz = (lax.axis_size(a) for a in ("gx", "gy", "gz"))
    assert (bx, by, bz) == (4, 4, 4) and bx * rhs == 128 and pts == 128
    xs = 2 if nx == 2 else 3
    geo = dict(nx=nx, ny=ny, nz=nz, xs=xs, bx=bx, by=by, bz=bz, rhs=rhs, rank=rank, width=rhs)
    geo["extra_x"] = max(nx - 3, 0)
    geo["extra_z"] = max(nz - 3, 0)
    geo["extra_y"] = max(ny - 3, 0)
    per = 128 // rhs
    tiles_x = -(-nx // per)
    tiles_z = -(-nx * nz // per)

    def shape(*dims, dtype=BF16):
        return jax.ShapeDtypeStruct(dims, dtype)

    coupling_flat = coupling.transpose(0, 2, 1, 3).reshape(2, rank, -1)
    coarse_flat = coarse_coupling.transpose(3, 1, 2, 0, 4).reshape(rank, -1)
    down_one = transfer.transpose(0, 2, 1).reshape(-1, rank)
    down_zero = transfer.reshape(2, 2, 2, rank, rank).transpose(1, 2, 4, 0, 3).reshape(4, rank, 2 * rank)

    face = shape(by, bx, rhs, pts)
    own, high, low = run(
        mask_kernel, (shape(bz, by, bx, rhs, pts), face, face), (counts, charges), smem=(0,), name="mask"
    )
    cz_prev = from_shift(high, "gz", nz, -1)
    cz_next = from_shift(low, "gz", nz, 1)
    mom = run(moment_kernel, shape(bz * by + 3, rank, 128), (own, leaf_basis, transfer), name="moments")
    if nx == 2:
        sources = [mom, from_shift(mom, "gx", nx, 1)]
    else:
        sources = [mom, from_shift(mom, "gx", nx, -1), from_shift(mom, "gx", nx, 1)]
    extra = [from_shift(mom[bz * by + 2], "gx", nx, s) for s in range(2, nx - 1)]

    size = shape(bz + 2, by, rhs, pts)
    high, low = run(pack_charge_x_kernel, (size, size), (own, cz_prev, cz_next), name="pack_charge_x")
    cx_prev = from_shift(high, "gx", nx, -1)
    cx_next = from_shift(low, "gx", nx, 1)

    size = shape(xs * 2 * by + xs * 2 + tiles_x, rank, 128)
    high, low, two_x = run(
        functools.partial(pack_z_kernel, geo),
        (size, size, shape(tiles_x, rank, 128)),
        (*sources, *extra),
        name="pack_z",
    )
    mz_prev = from_shift(high, "gz", nz, -1)
    mz_next = from_shift(low, "gz", nz, 1)
    extra = [from_shift(two_x, "gz", nz, s) for s in range(2, nz - 1)]

    size = shape(bz + 2, bx + 2, rhs, pts)
    high, low = run(
        pack_charge_y_kernel, (size, size), (own, cz_prev, cz_next, cx_prev, cx_next), name="pack_charge_y"
    )
    cy_prev = from_shift(high, "gy", ny, -1)
    cy_next = from_shift(low, "gy", ny, 1)

    size = shape(xs * 2 * (bz + 4) + xs * 6 + tiles_z, rank, 128)
    high, low, two_z = run(
        functools.partial(pack_y_kernel, geo),
        (size, size, shape(tiles_z, rank, 128)),
        (*sources, mz_prev, mz_next, two_x, *extra),
        name="pack_y",
    )
    my_prev = from_shift(high, "gy", ny, -1)
    my_next = from_shift(low, "gy", ny, 1)
    extra = [from_shift(two_z, "gy", ny, s) for s in range(2, ny - 1)]

    return run(
        functools.partial(final_kernel, geo),
        shape(bx, by, bz, rhs, pts, dtype=F32),
        (
            counts,
            near_offsets,
            far_offsets,
            near_blocks,
            leaf_basis,
            coupling_flat,
            coarse_flat,
            down_one,
            down_zero,
            own,
            cz_prev,
            cz_next,
            cx_prev,
            cx_next,
            cy_prev,
            cy_next,
            *sources,
            mz_prev,
            mz_next,
            my_prev,
            my_next,
            two_z,
            *extra,
        ),
        smem=(0, 1, 2),
        scratch=[
            pltpu.VMEM((bz + 2, by + 2, (bx + 2) * rhs, pts), BF16),
            pltpu.VMEM((5, bz + 4, by + 4, rank, 128), BF16),
            pltpu.VMEM((5, 5, 6, rank, 128), BF16),
            pltpu.VMEM((far_offsets.shape[1] * rank, 256), BF16),
            pltpu.VMEM((bz, by, rank, 128), F32),
        ],
        name="final",
    )


def solution(mesh):
    in_specs = (
        P("gx", "gy", "gz", None, None),
        P("gx", "gy", "gz"),
        P(),
        P(),
        P(),
        P(),
        P(),
        P(),
        P(),
    )
    out_specs = P("gx", "gy", "gz", None, None)
    return jax.shard_map(body, mesh=mesh, in_specs=in_specs, out_specs=out_specs, check_vma=False)
```

```python
import functools

import jax
import jax.numpy as jnp
from jax import lax
from jax.experimental import pallas as pl
from jax.experimental.pallas import tpu as pltpu
from jax.sharding import PartitionSpec as P


F32 = jnp.float32
BF16 = jnp.bfloat16
VMEM_LIMIT = 24 * 1024 * 1024


def from_shift(value, axis, size, shift):
    return lax.ppermute(value, axis, [(i, (i - shift) % size) for i in range(size)])


def spec_vmem():
    return pl.BlockSpec(memory_space=pltpu.VMEM)


def spec_smem():
    return pl.BlockSpec(memory_space=pltpu.SMEM)


def run(kernel, out_shape, args, smem=(), hbm=(), scratch=(), flops=None, name=None):
    def spec(i):
        if i in hbm:
            return pl.BlockSpec(memory_space=pl.ANY)
        return spec_smem() if i in smem else spec_vmem()

    cost = None
    if flops is not None:
        cost = pl.CostEstimate(flops=flops, transcendentals=0, bytes_accessed=0)
    return pl.pallas_call(
        kernel,
        out_shape=out_shape,
        in_specs=[spec(i) for i in range(len(args))],
        out_specs=jax.tree.map(lambda _: spec_vmem(), out_shape),
        scratch_shapes=scratch,
        compiler_params=pltpu.CompilerParams(vmem_limit_bytes=VMEM_LIMIT),
        cost_estimate=cost,
        name=name,
    )(*args)


def lane_blocks(rows, width):
    return lax.broadcasted_iota(jnp.int32, (rows, 128), 1) // width


def roll(value, shift):
    shift = shift % 128
    return value if shift == 0 else pltpu.roll(value, shift, 1)


def dot(a, b, dims=((1,), (0,))):
    return lax.dot_general(a, b, (dims, ((), ())), preferred_element_type=F32)


def assemble(sources, width, load):
    per = 128 // width
    out = []
    for start in range(0, len(sources), per):
        total = None
        for d, (key, b) in enumerate(sources[start : start + per]):
            moved = roll(load(key).astype(F32), width * (d - b))
            if total is None:
                total = moved
                blocks = lane_blocks(moved.shape[0], width)
            else:
                total = jnp.where(blocks == d, moved, total)
        out.append(total.astype(BF16))
    return out


def tile_at(ref, start, rank):
    return ref[start : start + rank, :]


def first_kernel(counts_in, charges_in, basis_in, transfer_in, own, z_high, z_low, mom, y_high, y_low, counts, charges, basis, transfer, sems):
    bx, by, bz, rhs, pts = charges.shape
    rank = basis.shape[0]
    width = rhs
    copies = [
        pltpu.make_async_copy(counts_in, counts, sems.at[0]),
        pltpu.make_async_copy(basis_in, basis, sems.at[1]),
        pltpu.make_async_copy(transfer_in, transfer, sems.at[2]),
    ]
    parts = [pltpu.make_async_copy(charges_in.at[x], charges.at[x], sems.at[3 + x]) for x in range(bx)]
    for c in copies[:1] + parts + copies[1:]:
        c.start()
    lane = lax.broadcasted_iota(jnp.int32, (rhs, pts), 1)
    copies[0].wait()
    for x in range(bx):
        parts[x].wait()
        for y in range(by):
            for z in range(bz):
                keep = lane < counts[x, y, z]
                value = jnp.where(keep, charges[x, y, z].astype(F32), 0.0).astype(BF16)
                own[z, y, x] = value
                if z == 0:
                    z_low[y, x] = value
                if z == bz - 1:
                    z_high[y, x] = value
                at = (z * bx + x) * rhs
                if y == 0:
                    y_low[at : at + rhs] = value
                if y == by - 1:
                    y_high[at : at + rhs] = value
    copies[1].wait()
    copies[2].wait()
    base = bz * bx * rhs
    leaf = {}
    for z in range(bz):
        for y in range(0, by, 2):
            rows = own[z, y : y + 2].reshape(2 * bx * rhs, pts)
            value = dot(basis[...], rows, ((1,), (1,))).astype(BF16)
            for k in range(2):
                leaf[z, y + k] = value[:, 128 * k : 128 * (k + 1)]
                mom[z * by + y + k] = leaf[z, y + k]
                at = base + (z * 2 + k) * rank
                (y_low if y == 0 else y_high)[at : at + rank] = leaf[z, y + k]
    sums = [None, None]
    for i in range(2):
        for j in range(2):
            for l in range(2):
                cols = jnp.concatenate([leaf[2 * z + l, 2 * y + j] for z in range(2) for y in range(2)], axis=1)
                part = dot(transfer[4 * i + 2 * j + l], cols)
                sums[i] = part if sums[i] is None else sums[i] + part
    blocks = lane_blocks(rank, width)
    first = bz * by
    one = []
    for z in range(2):
        whole = []
        for y in range(2):
            at = 128 * (z * 2 + y)
            whole.append(sums[0][:, at : at + 128] + roll(sums[1][:, at : at + 128], -width))
        packed = jnp.where(
            blocks == 0,
            whole[0],
            jnp.where(
                blocks == 1,
                roll(whole[0], -width),
                jnp.where(blocks == 2, roll(whole[1], 2 * width), roll(whole[1], width)),
            ),
        ).astype(BF16)
        one.append(packed)
        mom[first + z] = packed
        at = base + (2 * bz + z) * rank
        y_high[at : at + rank] = packed
        y_low[at : at + rank] = packed
    two = None
    for j in range(2):
        for i in range(2):
            part = dot(transfer[4 * i + 2 * j], one[0]) + dot(transfer[4 * i + 2 * j + 1], one[1])
            part = roll(part, -width * (2 * j + i))
            two = part if two is None else two + part
    mom[first + 2] = two.astype(BF16)


def second_kernel(geo, *refs):
    nx, xs, bx, by, bz, rhs, rank = (geo[k] for k in ("nx", "xs", "bx", "by", "bz", "rhs", "rank"))
    it = iter(refs)

    def take(count):
        return [next(it) for _ in range(count)]

    own, prev, nxt = take(3)
    sources = take(xs)
    far = take(geo["extra_x"])
    x_high, x_low, z_high, z_low, y_high, y_low, two = take(7)
    leaf = bz * by
    at = 0
    for s in sources:
        for z in range(2):
            for y in range(by):
                z_high[at] = s[(bz - 2 + z) * by + y]
                z_low[at] = s[z * by + y]
                at += 1
    for s in sources:
        for z in range(2):
            z_high[at] = s[leaf + z]
            z_low[at] = s[leaf + z]
            at += 1

    def load(key):
        if key == 0:
            return sources[0][leaf + 2]
        if key == 1:
            return sources[xs - 1][leaf + 2]
        if key == nx - 1:
            return sources[1][leaf + 2]
        return far[key - 2][...]

    for t, tile in enumerate(assemble([(k, 0) for k in range(nx)], rhs, load)):
        z_high[at + t] = tile
        z_low[at + t] = tile
        two[t] = tile
    for y in range(by):
        for out, x in ((x_high, bx - 1), (x_low, 0)):
            out[0, y] = prev[y, x]
            out[bz + 1, y] = nxt[y, x]
            for z in range(bz):
                out[z + 1, y] = own[z, y, x]
    for out, y in ((y_high, by - 1), (y_low, 0)):
        for k, s in enumerate((prev, nxt)):
            for x in range(bx):
                at = (k * bx + x) * rhs
                out[at : at + rhs] = s[y, x]
    base = 2 * bx * rhs
    for out, start in ((y_high, by - 2), (y_low, 0)):
        for k in range(1, xs):
            for z in range(bz):
                for y in range(2):
                    at = base + (((k - 1) * bz + z) * 2 + y) * rank
                    out[at : at + rank] = sources[k][z * by + start + y]
            for z in range(2):
                at = base + ((xs - 1) * bz * 2 + (k - 1) * 2 + z) * rank
                out[at : at + rank] = sources[k][leaf + z]


def third_kernel(geo, *refs):
    nx, nz, xs, bx, by, bz, rhs, rank = (geo[k] for k in ("nx", "nz", "xs", "bx", "by", "bz", "rhs", "rank"))
    it = iter(refs)

    def take(count):
        return [next(it) for _ in range(count)]

    before, after, prev, nxt, mine = take(5)
    far = take(geo["extra_z"])
    y_high, y_low, two = take(3)
    for out, y in ((y_high, by - 1), (y_low, 0)):
        for k, s in enumerate((before, after)):
            for z in range(bz + 2):
                at = (k * (bz + 2) + z) * rhs
                out[at : at + rhs] = s[z, y]
    base = 2 * (bz + 2) * rhs
    for out, start in ((y_high, by - 2), (y_low, 0)):
        for k in range(xs):
            for zh in range(4):
                s = prev if zh < 2 else nxt
                for y in range(2):
                    at = base + ((k * 4 + zh) * 2 + y) * rank
                    out[at : at + rank] = s[(k * 2 + zh % 2) * by + start + y]
            for side, s in enumerate((prev, nxt)):
                for z in range(2):
                    at = base + (xs * 8 + (k * 2 + side) * 2 + z) * rank
                    out[at : at + rank] = s[xs * 2 * by + k * 2 + z]
    first = xs * 2 * by + xs * 2
    per = 128 // rhs
    order = [((s, b // per), b % per) for s in range(nz) for b in range(nx)]

    def load(key):
        s, t = key
        if s == 0:
            return mine[t]
        if s == 1:
            return nxt[first + t]
        if s == nz - 1:
            return prev[first + t]
        return far[s - 2][t]

    for t, tile in enumerate(assemble(order, rhs, load)):
        at = base + (xs * 12 + t) * rank
        y_high[at : at + rank] = tile
        y_low[at : at + rank] = tile
        two[t] = tile


def near_weights(inverse, near_blocks, codes):
    return jnp.concatenate([near_blocks[inverse[c]] for c in codes], axis=1)


def find_inverse(table, inverse, count):
    for s in range(count):
        ox, oy, oz = (table[3 * s + d] + 1 for d in range(3))
        inverse[(ox * 3 + oy) * 3 + oz] = s


def near_kernel(geo, table, near_blocks, own, cz_prev, cz_next, cx_prev, cx_next, *refs):
    bx, by, bz, rhs = (geo[k] for k in ("bx", "by", "bz", "rhs"))
    y1, y2, (out, wide, inverse) = refs[0:2], refs[2:4], refs[4:]
    pts = wide.shape[3]
    stencil = near_blocks.shape[0]
    find_inverse(table, inverse, stencil)
    zero = jnp.zeros((rhs, pts), BF16)
    for z in range(bz + 2):
        for y in (0, by + 1):
            k = 0 if y == 0 else 1
            if z == 0:
                middle = y2[k][0 : bx * rhs]
            elif z == bz + 1:
                middle = y2[k][bx * rhs : 2 * bx * rhs]
            else:
                middle = y1[k][(z - 1) * bx * rhs : z * bx * rhs]
            wide[z, y, 0:rhs] = zero
            wide[z, y, rhs : (bx + 1) * rhs] = middle
            wide[z, y, (bx + 1) * rhs :] = zero
        for y in range(1, by + 1):
            if z == 0:
                middle = cz_prev[y - 1]
            elif z == bz + 1:
                middle = cz_next[y - 1]
            else:
                middle = own[z - 1, y - 1]
            wide[z, y, 0:rhs] = cx_prev[z, y - 1]
            wide[z, y, rhs : (bx + 1) * rhs] = middle.reshape(bx * rhs, pts)
            wide[z, y, (bx + 1) * rhs :] = cx_next[z, y - 1]
    weights = near_weights(inverse, near_blocks, range(stencil))

    def step(number, carry):
        z = number // (by // 2)
        y = number % (by // 2) * 2
        windows = []
        for ox in range(3):
            for oy in range(3):
                for oz in range(3):
                    window = wide[z + oz, pl.ds(y + oy, 2), ox * rhs : (ox + bx) * rhs, :]
                    windows.append(window.reshape(2 * bx * rhs, pts))
        out[number] = dot(jnp.concatenate(windows, axis=1), weights, ((1,), (1,)))
        return carry

    lax.fori_loop(0, bz * by // 2, step, 0)


def weight_kernel(coupling_in, coarse_in, transfer, coupling, coarse, down_one, down_zero):
    entries, rank = coupling_in.shape[1:3]
    for level in range(2):
        coupling[level] = jnp.concatenate([coupling_in[level, e] for e in range(entries)], axis=1)
    nx, ny, nz = coarse_in.shape[:3]
    coarse[...] = jnp.concatenate(
        [coarse_in[x, y, z] for y in range(ny) for z in range(nz) for x in range(nx)], axis=1
    )
    turned = [transfer[c].astype(F32).T.astype(BF16) for c in range(8)]
    for c in range(8):
        down_one[c * rank : (c + 1) * rank] = turned[c]
    for k in range(4):
        down_zero[k] = jnp.concatenate([turned[k], turned[4 + k]], axis=1)


def final_kernel(geo, *refs):
    nx, ny, nz, xs, bx, by, bz, rhs, rank = (
        geo[k] for k in ("nx", "ny", "nz", "xs", "bx", "by", "bz", "rhs", "rank")
    )
    width = rhs
    it = iter(refs)

    def take(count):
        return [next(it) for _ in range(count)]

    (table, near, near_blocks, basis, coupling, coarse, down_one, down_zero) = take(8)
    sources = take(xs)
    mz_prev, mz_next = take(2)
    y1, y2, y3 = take(2), take(2), take(2)
    (mine_two,) = take(1)
    far_two = take(geo["extra_y"])
    (out,) = take(1)
    shifts, ones, columns, local, corners, inverse = take(6)
    pts = basis.shape[1]
    leaf = bz * by
    blocks = lane_blocks(rank, width)
    stencil = near_blocks.shape[0]
    entries = coupling.shape[2] // rank
    far_at = 3 * stencil
    counts_at = far_at + 6 * entries
    base1 = bz * bx * rhs
    base2 = 2 * bx * rhs
    base3 = 2 * (bz + 2) * rhs

    def far_offset(level, e):
        return [table[far_at + (level * entries + e) * 3 + d] + 2 for d in range(3)]

    find_inverse(table, inverse, stencil)
    for oy, yk in ((0, 0), (2, 1)):
        for ox, xk in ((0, 0), (2, 1)):
            weights = near_weights(inverse, near_blocks, [(ox * 3 + oy) * 3 + oz for oz in range(3)])
            windows = []
            for oz in range(3):
                at = (xk * (bz + 2) + oz) * rhs
                windows.append(y3[yk][at : at + bz * rhs])
            corners[yk, xk] = dot(jnp.concatenate(windows, axis=1), weights, ((1,), (1,)))

    def leaf_tile(k, z, y):
        if 0 <= y < by:
            if z < 0:
                return mz_prev[k * 2 * by + (z + 2) * by + y]
            if z >= bz:
                return mz_next[k * 2 * by + (z - bz) * by + y]
            return sources[k][z * by + y]
        side, yy = (0, y + 2) if y < 0 else (1, y - by)
        if not 0 <= z < bz:
            zh = z + 2 if z < 0 else z - bz + 2
            return tile_at(y3[side], base3 + ((k * 4 + zh) * 2 + yy) * rank, rank)
        if k == 0:
            return tile_at(y1[side], base1 + (z * 2 + yy) * rank, rank)
        return tile_at(y2[side], base2 + (((k - 1) * bz + z) * 2 + yy) * rank, rank)

    for z in range(-2, bz + 2):
        for y in range(-2, by + 2):
            mid = leaf_tile(0, z, y)
            shifts[2, z + 2, y + 2] = mid
            mid = mid.astype(F32)
            before = leaf_tile(1, z, y).astype(F32)
            after = before if xs == 2 else leaf_tile(2, z, y).astype(F32)
            shifts[0, z + 2, y + 2] = roll(jnp.where(blocks >= 2, before, mid), 2 * width).astype(BF16)
            shifts[1, z + 2, y + 2] = roll(jnp.where(blocks >= 3, before, mid), width).astype(BF16)
            shifts[3, z + 2, y + 2] = roll(jnp.where(blocks < 1, after, mid), -width).astype(BF16)
            shifts[4, z + 2, y + 2] = roll(jnp.where(blocks < 2, after, mid), -2 * width).astype(BF16)

    def one_tile(k, zb, z, yb):
        if yb == 1:
            if zb == 1:
                return sources[k][leaf + z]
            return (mz_prev if zb == 0 else mz_next)[xs * 2 * by + k * 2 + z]
        side = yb // 2
        if zb != 1:
            return tile_at(y3[side], base3 + (xs * 8 + (k * 2 + zb // 2) * 2 + z) * rank, rank)
        if k == 0:
            return tile_at(y1[side], base1 + (2 * bz + z) * rank, rank)
        return tile_at(y2[side], base2 + ((xs - 1) * bz * 2 + (k - 1) * 2 + z) * rank, rank)

    odd = blocks % 2 == 1
    upper = blocks >= 2

    def swap(value):
        return jnp.where(odd, roll(value, width), roll(value, -width))

    for zb in range(3):
        for z in range(2):
            rows = []
            for yb in range(3):
                mid = one_tile(0, zb, z, yb).astype(F32)
                before = one_tile(1, zb, z, yb).astype(F32)
                after = before if xs == 2 else one_tile(2, zb, z, yb).astype(F32)
                rows.append([
                    before,
                    swap(jnp.where(odd, before, mid)),
                    mid,
                    swap(jnp.where(odd, mid, after)),
                    after,
                ])
            for k in range(5):
                low, mid, high = (rows[yb][k] for yb in range(3))
                group = [
                    low,
                    roll(jnp.where(upper, low, mid), 2 * width),
                    mid,
                    roll(jnp.where(upper, mid, high), 2 * width),
                    high,
                ]
                for m in range(5):
                    ones[k, m, 2 * zb + z] = group[m].astype(BF16)

    first = base3 + xs * 12 * rank
    per = 128 // width

    def two_tile(s, t):
        if s == 0:
            return mine_two[t]
        if s == 1 or s == ny - 1:
            return tile_at(y3[1 if s == 1 else 0], first + t * rank, rank)
        return far_two[s - 2][t]

    stacked = []
    for s in range(ny):
        for b in range(nz * nx):
            tile = two_tile(s, b // per).astype(F32)
            stacked.append(jnp.where(blocks == b % per, tile, 0.0).astype(BF16))
    two = dot(coarse[...], jnp.concatenate(stacked, axis=0))
    two = two + roll(two, 2 * width)
    two = (two + roll(two, width)).astype(BF16)

    for e in range(entries):
        ox, oy, oz = far_offset(1, e)
        for z in range(2):
            columns[0, e * rank : (e + 1) * rank, 128 * z : 128 * (z + 1)] = ones[ox, oy, z + oz]
    local_one = dot(coupling[1], columns[0])
    from_two = dot(down_one[...], two)
    ups = []
    for z in range(2):
        total = local_one[:, 128 * z : 128 * (z + 1)]
        for j in range(2):
            for i in range(2):
                child = 4 * i + 2 * j + z
                part = from_two[child * rank : (child + 1) * rank]
                total = total + jnp.where(blocks == 2 * j + i, part, 0.0)
        total = total.astype(BF16).astype(F32)
        half = roll(total, 2 * width)
        for up in (
            jnp.where(blocks == 0, total, jnp.where(blocks == 3, half, roll(total, width))),
            jnp.where(blocks == 0, half, jnp.where(blocks == 3, total, roll(total, -width))),
        ):
            ups.append(
                jnp.concatenate(
                    [jnp.where(odd, 0.0, up).astype(BF16), jnp.where(odd, up, 0.0).astype(BF16)], axis=0
                )
            )
    ups = jnp.concatenate(ups, axis=1)
    for j in range(2):
        for l in range(2):
            part = dot(down_zero[2 * j + l], ups)
            for z in range(2):
                for y in range(2):
                    at = 128 * (2 * z + y)
                    local[2 * z + l, 2 * y + j] = part[:, at : at + 128]

    lane = lax.broadcasted_iota(jnp.int32, (rhs, pts), 1)

    def step(z, carry):
        for half in range(by // 2):
            y = 2 * half
            for e in range(entries):
                ox, oy, oz = far_offset(0, e)
                for k in range(2):
                    columns[half, e * rank : (e + 1) * rank, 128 * k : 128 * (k + 1)] = shifts[ox, z + oz, y + oy + k]
            total = dot(coupling[0], columns[half])
            total = total + jnp.concatenate([local[z, y], local[z, y + 1]], axis=1)
            result = dot(total.astype(BF16), basis[...], ((0,), (0,))) + near[z * (by // 2) + half]
            for k in range(2):
                for x in range(bx):
                    at = (k * bx + x) * rhs
                    value = result[at : at + rhs]
                    if y + k in (0, by - 1) and x in (0, bx - 1):
                        start = pl.multiple_of(z * rhs, rhs)
                        value = value + corners[0 if y + k == 0 else 1, 0 if x == 0 else 1, pl.ds(start, rhs), :]
                    keep = lane < table[counts_at + (x * by + y + k) * bz + z]
                    out[x, y + k, z] = jnp.where(keep, value, 0.0)
        return carry

    lax.fori_loop(0, bz, step, 0)


def body(charges, counts, near_offsets, near_blocks, leaf_basis, transfer, far_offsets, coupling, coarse_coupling):
    bx, by, bz, rhs, pts = charges.shape
    rank = leaf_basis.shape[0]
    entries = far_offsets.shape[1]
    stencil = near_blocks.shape[0]
    nx, ny, nz = (lax.axis_size(a) for a in ("gx", "gy", "gz"))
    assert (bx, by, bz) == (4, 4, 4) and bx * rhs == 128 and pts == 128
    xs = 2 if nx == 2 else 3
    geo = dict(nx=nx, ny=ny, nz=nz, xs=xs, bx=bx, by=by, bz=bz, rhs=rhs, rank=rank)
    geo["extra_x"] = max(nx - 3, 0)
    geo["extra_z"] = max(nz - 3, 0)
    geo["extra_y"] = max(ny - 3, 0)
    per = 128 // rhs
    tiles_x = -(-nx // per)
    tiles_z = -(-nx * nz // per)

    def shape(*dims, dtype=BF16):
        return jax.ShapeDtypeStruct(dims, dtype)

    def part(kernel):
        return functools.partial(kernel, geo)

    table = jnp.concatenate([near_offsets.reshape(-1), far_offsets.reshape(-1), counts.reshape(-1)])

    face = shape(by, bx, rhs, pts)
    message = shape(bz * bx * rhs + (bz * 2 + 2) * rank, 128)
    own, z_high, z_low, mom, y_high, y_low = run(
        first_kernel,
        (shape(bz, by, bx, rhs, pts), face, face, shape(bz * by + 3, rank, 128), message, message),
        (counts, charges, leaf_basis, transfer),
        hbm=(0, 1, 2, 3),
        scratch=[
            pltpu.SMEM(counts.shape, jnp.int32),
            pltpu.VMEM(charges.shape, BF16),
            pltpu.VMEM(leaf_basis.shape, BF16),
            pltpu.VMEM(transfer.shape, BF16),
            pltpu.SemaphoreType.DMA((3 + bx,)),
        ],
        name="first",
    )
    cz_prev = from_shift(z_high, "gz", nz, -1)
    cz_next = from_shift(z_low, "gz", nz, 1)
    if nx == 2:
        sources = [mom, from_shift(mom, "gx", nx, 1)]
    else:
        sources = [mom, from_shift(mom, "gx", nx, -1), from_shift(mom, "gx", nx, 1)]
    extra = [from_shift(mom[bz * by + 2], "gx", nx, s) for s in range(2, nx - 1)]
    y1 = [from_shift(y_high, "gy", ny, -1), from_shift(y_low, "gy", ny, 1)]

    weights = run(
        weight_kernel,
        (
            shape(2, rank, entries * rank),
            shape(rank, nx * ny * nz * rank),
            shape(8 * rank, rank),
            shape(4, rank, 2 * rank),
        ),
        (coupling, coarse_coupling, transfer),
        name="weights",
    )

    charge = shape(bz + 2, by, rhs, pts)
    moment = shape(xs * 2 * by + xs * 2 + tiles_x, rank, 128)
    message = shape(2 * bx * rhs + (xs - 1) * (bz * 2 + 2) * rank, 128)
    x_high, x_low, z_high, z_low, y_high, y_low, two_x = run(
        part(second_kernel),
        (charge, charge, moment, moment, message, message, shape(tiles_x, rank, 128)),
        (own, cz_prev, cz_next, *sources, *extra),
        name="second",
    )
    cx_prev = from_shift(x_high, "gx", nx, -1)
    cx_next = from_shift(x_low, "gx", nx, 1)
    mz_prev = from_shift(z_high, "gz", nz, -1)
    mz_next = from_shift(z_low, "gz", nz, 1)
    extra = [from_shift(two_x, "gz", nz, s) for s in range(2, nz - 1)]
    y2 = [from_shift(y_high, "gy", ny, -1), from_shift(y_low, "gy", ny, 1)]

    message = shape(2 * (bz + 2) * rhs + (xs * 12 + tiles_z) * rank, 128)
    y_high, y_low, two_z = run(
        part(third_kernel),
        (message, message, shape(tiles_z, rank, 128)),
        (cx_prev, cx_next, mz_prev, mz_next, two_x, *extra),
        name="third",
    )
    y3 = [from_shift(y_high, "gy", ny, -1), from_shift(y_low, "gy", ny, 1)]
    extra = [from_shift(two_z, "gy", ny, s) for s in range(2, ny - 1)]

    near = run(
        part(near_kernel),
        shape(bz * by // 2, 2 * bx * rhs, pts, dtype=F32),
        (table, near_blocks, own, cz_prev, cz_next, cx_prev, cx_next, *y1, *y2),
        smem=(0,),
        scratch=[
            pltpu.VMEM((bz + 2, by + 2, (bx + 2) * rhs, pts), BF16),
            pltpu.SMEM((stencil,), jnp.int32),
        ],
        flops=2 * bx * by * bz * rhs * pts * pts * stencil,
        name="near",
    )
    return run(
        part(final_kernel),
        shape(bx, by, bz, rhs, pts, dtype=F32),
        (
            table,
            near,
            near_blocks,
            leaf_basis,
            *weights,
            *sources,
            mz_prev,
            mz_next,
            *y1,
            *y2,
            *y3,
            two_z,
            *extra,
        ),
        smem=(0,),
        scratch=[
            pltpu.VMEM((5, bz + 4, by + 4, rank, 128), BF16),
            pltpu.VMEM((5, 5, 6, rank, 128), BF16),
            pltpu.VMEM((by // 2, entries * rank, 256), BF16),
            pltpu.VMEM((bz, by, rank, 128), F32),
            pltpu.VMEM((2, 2, bz * rhs, pts), F32),
            pltpu.SMEM((stencil,), jnp.int32),
        ],
        name="final",
    )


def solution(mesh):
    in_specs = (
        P("gx", "gy", "gz", None, None),
        P("gx", "gy", "gz"),
        P(),
        P(),
        P(),
        P(),
        P(),
        P(),
        P(),
    )
    out_specs = P("gx", "gy", "gz", None, None)
    return jax.shard_map(body, mesh=mesh, in_specs=in_specs, out_specs=out_specs, check_vma=False)
```

```python
import functools

import jax
import jax.numpy as jnp
from jax import lax
from jax.experimental import pallas as pl
from jax.experimental.pallas import tpu as pltpu
from jax.sharding import PartitionSpec as P


F32 = jnp.float32
BF16 = jnp.bfloat16


def from_shift(value, axis, size, shift):
    return lax.ppermute(value, axis, [(i, (i - shift) % size) for i in range(size)])


def spec_vmem():
    return pl.BlockSpec(memory_space=pltpu.VMEM)


def spec_smem():
    return pl.BlockSpec(memory_space=pltpu.SMEM)


def run(kernel, out_shape, args, smem=(), hbm=(), scratch=(), flops=None, limit=8):
    def spec(i):
        if i in hbm:
            return pl.BlockSpec(memory_space=pltpu.HBM)
        return spec_smem() if i in smem else spec_vmem()

    cost = None
    if flops is not None:
        cost = pl.CostEstimate(flops=flops, transcendentals=0, bytes_accessed=0)
    return pl.pallas_call(
        kernel,
        out_shape=out_shape,
        in_specs=[spec(i) for i in range(len(args))],
        out_specs=jax.tree.map(lambda _: spec_vmem(), out_shape),
        scratch_shapes=scratch,
        compiler_params=pltpu.CompilerParams(vmem_limit_bytes=limit * 1024 * 1024),
        cost_estimate=cost,
    )(*args)


def lane_blocks(rows, width):
    return lax.broadcasted_iota(jnp.int32, (rows, 128), 1) // width


def roll(value, shift):
    shift = shift % 128
    return value if shift == 0 else pltpu.roll(value, shift, 1)


def dot(a, b, dims=((1,), (0,))):
    return lax.dot_general(a, b, (dims, ((), ())), preferred_element_type=F32)


def assemble(sources, width, load):
    per = 128 // width
    out = []
    for start in range(0, len(sources), per):
        total = None
        for d, (key, b) in enumerate(sources[start : start + per]):
            moved = roll(load(key).astype(F32), width * (d - b))
            if total is None:
                total = moved
                blocks = lane_blocks(moved.shape[0], width)
            else:
                total = jnp.where(blocks == d, moved, total)
        out.append(total.astype(BF16))
    return out


def tile_at(ref, start, rank):
    return ref[start : start + rank, :]


def first_kernel(counts_in, charges_in, basis_in, transfer_in, own, z_high, z_low, mom, y_high, y_low, counts, charges, basis, transfer, sems):
    bx, by, bz, rhs, pts = charges.shape
    rank = basis.shape[0]
    width = rhs
    copies = [
        pltpu.make_async_copy(counts_in, counts, sems.at[0]),
        pltpu.make_async_copy(basis_in, basis, sems.at[1]),
        pltpu.make_async_copy(transfer_in, transfer, sems.at[2]),
    ]
    parts = [pltpu.make_async_copy(charges_in.at[x], charges.at[x], sems.at[3 + x]) for x in range(bx)]
    for c in copies[:1] + parts + copies[1:]:
        c.start()
    lane = lax.broadcasted_iota(jnp.int32, (rhs, pts), 1)
    copies[0].wait()
    for x in range(bx):
        parts[x].wait()
        for y in range(by):
            for z in range(bz):
                keep = lane < counts[x, y, z]
                value = jnp.where(keep, charges[x, y, z].astype(F32), 0.0).astype(BF16)
                own[z, y, x] = value
                if z == 0:
                    z_low[y, x] = value
                if z == bz - 1:
                    z_high[y, x] = value
                at = (z * bx + x) * rhs
                if y == 0:
                    y_low[at : at + rhs] = value
                if y == by - 1:
                    y_high[at : at + rhs] = value
    copies[1].wait()
    copies[2].wait()
    base = bz * bx * rhs
    leaf = {}
    for z in range(bz):
        for y in range(0, by, 2):
            rows = own[z, y : y + 2].reshape(2 * bx * rhs, pts)
            value = dot(basis[...], rows, ((1,), (1,))).astype(BF16)
            for k in range(2):
                leaf[z, y + k] = value[:, 128 * k : 128 * (k + 1)]
                mom[z * by + y + k] = leaf[z, y + k]
                at = base + (z * 2 + k) * rank
                (y_low if y == 0 else y_high)[at : at + rank] = leaf[z, y + k]
    sums = [None, None]
    for i in range(2):
        for j in range(2):
            for l in range(2):
                cols = jnp.concatenate([leaf[2 * z + l, 2 * y + j] for z in range(2) for y in range(2)], axis=1)
                part = dot(transfer[4 * i + 2 * j + l], cols)
                sums[i] = part if sums[i] is None else sums[i] + part
    blocks = lane_blocks(rank, width)
    first = bz * by
    one = []
    for z in range(2):
        whole = []
        for y in range(2):
            at = 128 * (z * 2 + y)
            whole.append(sums[0][:, at : at + 128] + roll(sums[1][:, at : at + 128], -width))
        packed = jnp.where(
            blocks == 0,
            whole[0],
            jnp.where(
                blocks == 1,
                roll(whole[0], -width),
                jnp.where(blocks == 2, roll(whole[1], 2 * width), roll(whole[1], width)),
            ),
        ).astype(BF16)
        one.append(packed)
        mom[first + z] = packed
        at = base + (2 * bz + z) * rank
        y_high[at : at + rank] = packed
        y_low[at : at + rank] = packed
    two = None
    for j in range(2):
        for i in range(2):
            part = dot(transfer[4 * i + 2 * j], one[0]) + dot(transfer[4 * i + 2 * j + 1], one[1])
            part = roll(part, -width * (2 * j + i))
            two = part if two is None else two + part
    mom[first + 2] = two.astype(BF16)


def second_kernel(geo, *refs):
    nx, xs, bx, by, bz, rhs, rank = (geo[k] for k in ("nx", "xs", "bx", "by", "bz", "rhs", "rank"))
    it = iter(refs)

    def take(count):
        return [next(it) for _ in range(count)]

    own, prev, nxt = take(3)
    sources = take(xs)
    far = take(geo["extra_x"])
    x_high, x_low, z_high, z_low, y_high, y_low, two = take(7)
    leaf = bz * by
    at = 0
    for s in sources:
        for z in range(2):
            for y in range(by):
                z_high[at] = s[(bz - 2 + z) * by + y]
                z_low[at] = s[z * by + y]
                at += 1
    for s in sources:
        for z in range(2):
            z_high[at] = s[leaf + z]
            z_low[at] = s[leaf + z]
            at += 1

    def load(key):
        if key == 0:
            return sources[0][leaf + 2]
        if key == 1:
            return sources[xs - 1][leaf + 2]
        if key == nx - 1:
            return sources[1][leaf + 2]
        return far[key - 2][...]

    for t, tile in enumerate(assemble([(k, 0) for k in range(nx)], rhs, load)):
        z_high[at + t] = tile
        z_low[at + t] = tile
        two[t] = tile
    for y in range(by):
        for out, x in ((x_high, bx - 1), (x_low, 0)):
            out[0, y] = prev[y, x]
            out[bz + 1, y] = nxt[y, x]
            for z in range(bz):
                out[z + 1, y] = own[z, y, x]
    for out, y in ((y_high, by - 1), (y_low, 0)):
        for k, s in enumerate((prev, nxt)):
            for x in range(bx):
                at = (k * bx + x) * rhs
                out[at : at + rhs] = s[y, x]
    base = 2 * bx * rhs
    for out, start in ((y_high, by - 2), (y_low, 0)):
        for k in range(1, xs):
            for z in range(bz):
                for y in range(2):
                    at = base + (((k - 1) * bz + z) * 2 + y) * rank
                    out[at : at + rank] = sources[k][z * by + start + y]
            for z in range(2):
                at = base + ((xs - 1) * bz * 2 + (k - 1) * 2 + z) * rank
                out[at : at + rank] = sources[k][leaf + z]


def third_kernel(geo, *refs):
    nx, nz, xs, _, by, bz, rhs, rank = (geo[k] for k in ("nx", "nz", "xs", "bx", "by", "bz", "rhs", "rank"))
    it = iter(refs)

    def take(count):
        return [next(it) for _ in range(count)]

    before, after, prev, nxt, mine = take(5)
    far = take(geo["extra_z"])
    y_high, y_low, two = take(3)
    for out, y in ((y_high, by - 1), (y_low, 0)):
        for k, s in enumerate((before, after)):
            for z in range(bz + 2):
                at = (k * (bz + 2) + z) * rhs
                out[at : at + rhs] = s[z, y]
    base = 2 * (bz + 2) * rhs
    for out, start in ((y_high, by - 2), (y_low, 0)):
        for k in range(xs):
            for zh in range(4):
                s = prev if zh < 2 else nxt
                for y in range(2):
                    at = base + ((k * 4 + zh) * 2 + y) * rank
                    out[at : at + rank] = s[(k * 2 + zh % 2) * by + start + y]
            for side, s in enumerate((prev, nxt)):
                for z in range(2):
                    at = base + (xs * 8 + (k * 2 + side) * 2 + z) * rank
                    out[at : at + rank] = s[xs * 2 * by + k * 2 + z]
    first = xs * 2 * by + xs * 2
    per = 128 // rhs
    order = [((s, b // per), b % per) for s in range(nz) for b in range(nx)]

    def load(key):
        s, t = key
        if s == 0:
            return mine[t]
        if s == 1:
            return nxt[first + t]
        if s == nz - 1:
            return prev[first + t]
        return far[s - 2][t]

    for t, tile in enumerate(assemble(order, rhs, load)):
        at = base + (xs * 12 + t) * rank
        y_high[at : at + rank] = tile
        y_low[at : at + rank] = tile
        two[t] = tile


def near_weights(inverse, near_blocks, codes):
    return jnp.concatenate([near_blocks[inverse[c]] for c in codes], axis=1)


def find_inverse(table, inverse, count):
    for s in range(count):
        ox, oy, oz = (table[d, s] + 1 for d in range(3))
        inverse[(ox * 3 + oy) * 3 + oz] = s


def near_kernel(geo, table, near_blocks, own, cz_prev, cz_next, cx_prev, cx_next, *refs):
    bx, by, bz, rhs = (geo[k] for k in ("bx", "by", "bz", "rhs"))
    y1, y2, (out, wide, inverse) = refs[0:2], refs[2:4], refs[4:]
    pts = wide.shape[3]
    stencil = near_blocks.shape[0]
    find_inverse(table, inverse, stencil)
    zero = jnp.zeros((rhs, pts), BF16)
    for z in range(bz + 2):
        for y in (0, by + 1):
            k = 0 if y == 0 else 1
            if z == 0:
                middle = y2[k][0 : bx * rhs]
            elif z == bz + 1:
                middle = y2[k][bx * rhs : 2 * bx * rhs]
            else:
                middle = y1[k][(z - 1) * bx * rhs : z * bx * rhs]
            wide[z, y, 0:rhs] = zero
            wide[z, y, rhs : (bx + 1) * rhs] = middle
            wide[z, y, (bx + 1) * rhs :] = zero
        for y in range(1, by + 1):
            if z == 0:
                middle = cz_prev[y - 1]
            elif z == bz + 1:
                middle = cz_next[y - 1]
            else:
                middle = own[z - 1, y - 1]
            wide[z, y, 0:rhs] = cx_prev[z, y - 1]
            wide[z, y, rhs : (bx + 1) * rhs] = middle.reshape(bx * rhs, pts)
            wide[z, y, (bx + 1) * rhs :] = cx_next[z, y - 1]
    weights = near_weights(inverse, near_blocks, range(stencil))

    def step(number, carry):
        z = number // (by // 2)
        y = number % (by // 2) * 2
        windows = []
        for ox in range(3):
            for oy in range(3):
                for oz in range(3):
                    window = wide[z + oz, pl.ds(y + oy, 2), ox * rhs : (ox + bx) * rhs, :]
                    windows.append(window.reshape(2 * bx * rhs, pts))
        out[number] = dot(jnp.concatenate(windows, axis=1), weights, ((1,), (1,)))
        return carry

    lax.fori_loop(0, bz * by // 2, step, 0)


def weight_kernel(coupling_in, coarse_in, transfer, coupling, coarse, down_one, down_zero):
    entries, rank = coupling_in.shape[1:3]
    for level in range(2):
        coupling[level] = jnp.concatenate([coupling_in[level, e] for e in range(entries)], axis=1)
    nx, ny, nz = coarse_in.shape[:3]
    coarse[...] = jnp.concatenate(
        [coarse_in[x, y, z] for y in range(ny) for z in range(nz) for x in range(nx)], axis=1
    )
    turned = [transfer[c].astype(F32).T.astype(BF16) for c in range(8)]
    for c in range(8):
        down_one[c * rank : (c + 1) * rank] = turned[c]
    for k in range(4):
        down_zero[k] = jnp.concatenate([turned[k], turned[4 + k]], axis=1)


def final_kernel(geo, *refs):
    nx, ny, nz, xs, bx, by, bz, rhs, rank = (
        geo[k] for k in ("nx", "ny", "nz", "xs", "bx", "by", "bz", "rhs", "rank")
    )
    width = rhs
    it = iter(refs)

    def take(count):
        return [next(it) for _ in range(count)]

    counts, near_table, far_table = take(3)
    near, near_blocks, basis, coupling, coarse, down_one, down_zero = take(7)
    sources = take(xs)
    mz_prev, mz_next = take(2)
    y1, y2, y3 = take(2), take(2), take(2)
    (mine_two,) = take(1)
    far_two = take(geo["extra_y"])
    (out,) = take(1)
    shifts, ones, columns, local, corners, inverse = take(6)
    pts = basis.shape[1]
    leaf = bz * by
    blocks = lane_blocks(rank, width)
    stencil = near_blocks.shape[0]
    entries = coupling.shape[2] // rank
    base1 = bz * bx * rhs
    base2 = 2 * bx * rhs
    base3 = 2 * (bz + 2) * rhs

    def far_offset(level, e):
        return [far_table[d, level, e] + 2 for d in range(3)]

    find_inverse(near_table, inverse, stencil)
    for oy, yk in ((0, 0), (2, 1)):
        for ox, xk in ((0, 0), (2, 1)):
            weights = near_weights(inverse, near_blocks, [(ox * 3 + oy) * 3 + oz for oz in range(3)])
            windows = []
            for oz in range(3):
                at = (xk * (bz + 2) + oz) * rhs
                windows.append(y3[yk][at : at + bz * rhs])
            corners[yk, xk] = dot(jnp.concatenate(windows, axis=1), weights, ((1,), (1,)))

    def leaf_tile(k, z, y):
        if 0 <= y < by:
            if z < 0:
                return mz_prev[k * 2 * by + (z + 2) * by + y]
            if z >= bz:
                return mz_next[k * 2 * by + (z - bz) * by + y]
            return sources[k][z * by + y]
        side, yy = (0, y + 2) if y < 0 else (1, y - by)
        if not 0 <= z < bz:
            zh = z + 2 if z < 0 else z - bz + 2
            return tile_at(y3[side], base3 + ((k * 4 + zh) * 2 + yy) * rank, rank)
        if k == 0:
            return tile_at(y1[side], base1 + (z * 2 + yy) * rank, rank)
        return tile_at(y2[side], base2 + (((k - 1) * bz + z) * 2 + yy) * rank, rank)

    for z in range(-2, bz + 2):
        for y in range(-2, by + 2):
            mid = leaf_tile(0, z, y)
            shifts[2, z + 2, y + 2] = mid
            mid = mid.astype(F32)
            before = leaf_tile(1, z, y).astype(F32)
            after = before if xs == 2 else leaf_tile(2, z, y).astype(F32)
            shifts[0, z + 2, y + 2] = roll(jnp.where(blocks >= 2, before, mid), 2 * width).astype(BF16)
            shifts[1, z + 2, y + 2] = roll(jnp.where(blocks >= 3, before, mid), width).astype(BF16)
            shifts[3, z + 2, y + 2] = roll(jnp.where(blocks < 1, after, mid), -width).astype(BF16)
            shifts[4, z + 2, y + 2] = roll(jnp.where(blocks < 2, after, mid), -2 * width).astype(BF16)

    def one_tile(k, zb, z, yb):
        if yb == 1:
            if zb == 1:
                return sources[k][leaf + z]
            return (mz_prev if zb == 0 else mz_next)[xs * 2 * by + k * 2 + z]
        side = yb // 2
        if zb != 1:
            return tile_at(y3[side], base3 + (xs * 8 + (k * 2 + zb // 2) * 2 + z) * rank, rank)
        if k == 0:
            return tile_at(y1[side], base1 + (2 * bz + z) * rank, rank)
        return tile_at(y2[side], base2 + ((xs - 1) * bz * 2 + (k - 1) * 2 + z) * rank, rank)

    odd = blocks % 2 == 1
    upper = blocks >= 2

    def swap(value):
        return jnp.where(odd, roll(value, width), roll(value, -width))

    for zb in range(3):
        for z in range(2):
            rows = []
            for yb in range(3):
                mid = one_tile(0, zb, z, yb).astype(F32)
                before = one_tile(1, zb, z, yb).astype(F32)
                after = before if xs == 2 else one_tile(2, zb, z, yb).astype(F32)
                rows.append([
                    before,
                    swap(jnp.where(odd, before, mid)),
                    mid,
                    swap(jnp.where(odd, mid, after)),
                    after,
                ])
            for k in range(5):
                low, mid, high = (rows[yb][k] for yb in range(3))
                group = [
                    low,
                    roll(jnp.where(upper, low, mid), 2 * width),
                    mid,
                    roll(jnp.where(upper, mid, high), 2 * width),
                    high,
                ]
                for m in range(5):
                    ones[k, m, 2 * zb + z] = group[m].astype(BF16)

    first = base3 + xs * 12 * rank
    per = 128 // width

    def two_tile(s, t):
        if s == 0:
            return mine_two[t]
        if s == 1 or s == ny - 1:
            return tile_at(y3[1 if s == 1 else 0], first + t * rank, rank)
        return far_two[s - 2][t]

    stacked = []
    for s in range(ny):
        for b in range(nz * nx):
            tile = two_tile(s, b // per).astype(F32)
            stacked.append(jnp.where(blocks == b % per, tile, 0.0).astype(BF16))
    two = dot(coarse[...], jnp.concatenate(stacked, axis=0))
    two = two + roll(two, 2 * width)
    two = (two + roll(two, width)).astype(BF16)

    for e in range(entries):
        ox, oy, oz = far_offset(1, e)
        for z in range(2):
            columns[0, e * rank : (e + 1) * rank, 128 * z : 128 * (z + 1)] = ones[ox, oy, z + oz]
    local_one = dot(coupling[1], columns[0])
    from_two = dot(down_one[...], two)
    ups = []
    for z in range(2):
        total = local_one[:, 128 * z : 128 * (z + 1)]
        for j in range(2):
            for i in range(2):
                child = 4 * i + 2 * j + z
                part = from_two[child * rank : (child + 1) * rank]
                total = total + jnp.where(blocks == 2 * j + i, part, 0.0)
        total = total.astype(BF16).astype(F32)
        half = roll(total, 2 * width)
        for up in (
            jnp.where(blocks == 0, total, jnp.where(blocks == 3, half, roll(total, width))),
            jnp.where(blocks == 0, half, jnp.where(blocks == 3, total, roll(total, -width))),
        ):
            ups.append(
                jnp.concatenate(
                    [jnp.where(odd, 0.0, up).astype(BF16), jnp.where(odd, up, 0.0).astype(BF16)], axis=0
                )
            )
    ups = jnp.concatenate(ups, axis=1)
    for j in range(2):
        for l in range(2):
            part = dot(down_zero[2 * j + l], ups)
            for z in range(2):
                for y in range(2):
                    at = 128 * (2 * z + y)
                    local[2 * z + l, 2 * y + j] = part[:, at : at + 128]

    lane = lax.broadcasted_iota(jnp.int32, (rhs, pts), 1)

    def step(z, carry):
        for half in range(by // 2):
            y = 2 * half
            for e in range(entries):
                ox, oy, oz = far_offset(0, e)
                for k in range(2):
                    columns[half, e * rank : (e + 1) * rank, 128 * k : 128 * (k + 1)] = shifts[ox, z + oz, y + oy + k]
            total = dot(coupling[0], columns[half])
            total = total + jnp.concatenate([local[z, y], local[z, y + 1]], axis=1)
            result = dot(total.astype(BF16), basis[...], ((0,), (0,))) + near[z * (by // 2) + half]
            for k in range(2):
                for x in range(bx):
                    at = (k * bx + x) * rhs
                    value = result[at : at + rhs]
                    if y + k in (0, by - 1) and x in (0, bx - 1):
                        start = pl.multiple_of(z * rhs, rhs)
                        value = value + corners[0 if y + k == 0 else 1, 0 if x == 0 else 1, pl.ds(start, rhs), :]
                    keep = lane < counts[x, y + k, z]
                    out[x, y + k, z] = jnp.where(keep, value, 0.0)
        return carry

    lax.fori_loop(0, bz, step, 0)


def body(charges, counts, near_offsets, near_blocks, leaf_basis, transfer, far_offsets, coupling, coarse_coupling):
    bx, by, bz, rhs, pts = charges.shape
    rank = leaf_basis.shape[0]
    entries = far_offsets.shape[1]
    stencil = near_blocks.shape[0]
    nx, ny, nz = (lax.axis_size(a) for a in ("gx", "gy", "gz"))
    assert (bx, by, bz) == (4, 4, 4) and bx * rhs == 128 and pts == 128
    xs = 2 if nx == 2 else 3
    geo = dict(nx=nx, ny=ny, nz=nz, xs=xs, bx=bx, by=by, bz=bz, rhs=rhs, rank=rank)
    geo["extra_x"] = max(nx - 3, 0)
    geo["extra_z"] = max(nz - 3, 0)
    geo["extra_y"] = max(ny - 3, 0)
    per = 128 // rhs
    tiles_x = -(-nx // per)
    tiles_z = -(-nx * nz // per)

    def shape(*dims, dtype=BF16):
        return jax.ShapeDtypeStruct(dims, dtype)

    def part(kernel):
        return functools.partial(kernel, geo)

    near_table = near_offsets.T
    far_table = far_offsets.transpose(2, 0, 1)

    face = shape(by, bx, rhs, pts)
    message = shape(bz * bx * rhs + (bz * 2 + 2) * rank, 128)
    own, z_high, z_low, mom, y_high, y_low = run(
        first_kernel,
        (shape(bz, by, bx, rhs, pts), face, face, shape(bz * by + 3, rank, 128), message, message),
        (counts, charges, leaf_basis, transfer),
        hbm=(0, 1, 2, 3),
        scratch=[
            pltpu.SMEM(counts.shape, jnp.int32),
            pltpu.VMEM(charges.shape, BF16),
            pltpu.VMEM(leaf_basis.shape, BF16),
            pltpu.VMEM(transfer.shape, BF16),
            pltpu.SemaphoreType.DMA((3 + bx,)),
        ],
    )
    cz_prev = from_shift(z_high, "gz", nz, -1)
    cz_next = from_shift(z_low, "gz", nz, 1)
    if nx == 2:
        sources = [mom, from_shift(mom, "gx", nx, 1)]
    else:
        sources = [mom, from_shift(mom, "gx", nx, -1), from_shift(mom, "gx", nx, 1)]
    extra = [from_shift(mom[bz * by + 2], "gx", nx, s) for s in range(2, nx - 1)]
    y1 = [from_shift(y_high, "gy", ny, -1), from_shift(y_low, "gy", ny, 1)]

    weights = run(
        weight_kernel,
        (
            shape(2, rank, entries * rank),
            shape(rank, nx * ny * nz * rank),
            shape(8 * rank, rank),
            shape(4, rank, 2 * rank),
        ),
        (coupling, coarse_coupling, transfer),
    )

    charge = shape(bz + 2, by, rhs, pts)
    moment = shape(xs * 2 * by + xs * 2 + tiles_x, rank, 128)
    message = shape(2 * bx * rhs + (xs - 1) * (bz * 2 + 2) * rank, 128)
    x_high, x_low, z_high, z_low, y_high, y_low, two_x = run(
        part(second_kernel),
        (charge, charge, moment, moment, message, message, shape(tiles_x, rank, 128)),
        (own, cz_prev, cz_next, *sources, *extra),
    )
    cx_prev = from_shift(x_high, "gx", nx, -1)
    cx_next = from_shift(x_low, "gx", nx, 1)
    mz_prev = from_shift(z_high, "gz", nz, -1)
    mz_next = from_shift(z_low, "gz", nz, 1)
    extra = [from_shift(two_x, "gz", nz, s) for s in range(2, nz - 1)]
    y2 = [from_shift(y_high, "gy", ny, -1), from_shift(y_low, "gy", ny, 1)]

    message = shape(2 * (bz + 2) * rhs + (xs * 12 + tiles_z) * rank, 128)
    y_high, y_low, two_z = run(
        part(third_kernel),
        (message, message, shape(tiles_z, rank, 128)),
        (cx_prev, cx_next, mz_prev, mz_next, two_x, *extra),
    )
    y3 = [from_shift(y_high, "gy", ny, -1), from_shift(y_low, "gy", ny, 1)]
    extra = [from_shift(two_z, "gy", ny, s) for s in range(2, ny - 1)]

    near = run(
        part(near_kernel),
        shape(bz * by // 2, 2 * bx * rhs, pts, dtype=F32),
        (near_table, near_blocks, own, cz_prev, cz_next, cx_prev, cx_next, *y1, *y2),
        smem=(0,),
        scratch=[
            pltpu.VMEM((bz + 2, by + 2, (bx + 2) * rhs, pts), BF16),
            pltpu.SMEM((stencil,), jnp.int32),
        ],
        limit=16,
        flops=2 * bx * by * bz * rhs * pts * pts * stencil,
    )
    return run(
        part(final_kernel),
        shape(bx, by, bz, rhs, pts, dtype=F32),
        (
            counts,
            near_table,
            far_table,
            near,
            near_blocks,
            leaf_basis,
            *weights,
            *sources,
            mz_prev,
            mz_next,
            *y1,
            *y2,
            *y3,
            two_z,
            *extra,
        ),
        smem=(0, 1, 2),
        limit=24,
        scratch=[
            pltpu.VMEM((5, bz + 4, by + 4, rank, 128), BF16),
            pltpu.VMEM((5, 5, 6, rank, 128), BF16),
            pltpu.VMEM((by // 2, entries * rank, 256), BF16),
            pltpu.VMEM((bz, by, rank, 128), F32),
            pltpu.VMEM((2, 2, bz * rhs, pts), F32),
            pltpu.SMEM((stencil,), jnp.int32),
        ],
    )


def solution(mesh):
    in_specs = (
        P("gx", "gy", "gz", None, None),
        P("gx", "gy", "gz"),
        P(),
        P(),
        P(),
        P(),
        P(),
        P(),
        P(),
    )
    out_specs = P("gx", "gy", "gz", None, None)

    return jax.shard_map(body, mesh=mesh, in_specs=in_specs, out_specs=out_specs, check_vma=False)
```

```python
import functools

import jax
import jax.numpy as jnp
from jax import lax
from jax.experimental import pallas as pl
from jax.experimental.pallas import tpu as pltpu
from jax.sharding import PartitionSpec as P


F32 = jnp.float32
BF16 = jnp.bfloat16


def from_shift(value, axis, size, shift):
    return lax.ppermute(value, axis, [(i, (i - shift) % size) for i in range(size)])


def spec_vmem():
    return pl.BlockSpec(memory_space=pltpu.VMEM)


def spec_smem():
    return pl.BlockSpec(memory_space=pltpu.SMEM)


def run(kernel, out_shape, args, smem=(), hbm=(), scratch=(), flops=None, limit=8, hbm_out=(), aliases=None):
    def spec(i):
        if i in hbm:
            return pl.BlockSpec(memory_space=pltpu.HBM)
        return spec_smem() if i in smem else spec_vmem()

    cost = None
    if flops is not None:
        cost = pl.CostEstimate(flops=flops, transcendentals=0, bytes_accessed=0)
    count = len(out_shape) if isinstance(out_shape, tuple) else 1
    outs = tuple(pl.BlockSpec(memory_space=pltpu.HBM) if i in hbm_out else spec_vmem() for i in range(count))
    return pl.pallas_call(
        kernel,
        out_shape=out_shape,
        in_specs=[spec(i) for i in range(len(args))],
        out_specs=outs if isinstance(out_shape, tuple) else outs[0],
        input_output_aliases=aliases or {},
        scratch_shapes=scratch,
        compiler_params=pltpu.CompilerParams(vmem_limit_bytes=limit * 1024 * 1024),
        cost_estimate=cost,
    )(*args)


def lane_blocks(rows, width):
    return lax.broadcasted_iota(jnp.int32, (rows, 128), 1) // width


def roll(value, shift):
    shift = shift % 128
    return value if shift == 0 else pltpu.roll(value, shift, 1)


def dot(a, b, dims=((1,), (0,))):
    return lax.dot_general(a, b, (dims, ((), ())), preferred_element_type=F32)


def assemble(sources, width, load):
    per = 128 // width
    out = []
    for start in range(0, len(sources), per):
        total = None
        for d, (key, b) in enumerate(sources[start : start + per]):
            moved = roll(load(key).astype(F32), width * (d - b))
            if total is None:
                total = moved
                blocks = lane_blocks(moved.shape[0], width)
            else:
                total = jnp.where(blocks == d, moved, total)
        out.append(total.astype(BF16))
    return out


def tile_at(ref, start, rank):
    return ref[start : start + rank, :]


def start_kernel(out):
    out[...] = jnp.zeros(out.shape, out.dtype)


def first_kernel(token, counts_in, charges_in, basis_in, transfer_in, own, faces, mom, z_high, z_low, y_high, y_low, two, counts, charges, basis, transfer, sems):
    bx, by, bz, rhs, pts = charges.shape
    rank = basis.shape[0]
    width = rhs
    copies = [
        pltpu.make_async_copy(counts_in, counts, sems.at[0]),
        pltpu.make_async_copy(basis_in, basis, sems.at[1]),
        pltpu.make_async_copy(transfer_in, transfer, sems.at[2]),
    ]
    parts = [pltpu.make_async_copy(charges_in.at[x], charges.at[x], sems.at[3 + x]) for x in range(bx)]
    for c in copies[:1] + parts + copies[1:]:
        c.start()
    lane = lax.broadcasted_iota(jnp.int32, (rhs, pts), 1)
    copies[0].wait()
    for x in range(bx):
        parts[x].wait()
        for y in range(by):
            for z in range(bz):
                keep = lane < counts[x, y, z]
                value = jnp.where(keep, charges[x, y, z].astype(F32), 0.0).astype(BF16)
                own[z, y, x] = value
                if x == 0:
                    faces[0, z, y] = value
                if x == bx - 1:
                    faces[1, z, y] = value
                at = (z * bx + x) * rhs
                if y == 0:
                    y_low[at : at + rhs] = value
                if y == by - 1:
                    y_high[at : at + rhs] = value
    copies[1].wait()
    copies[2].wait()
    base = bz * bx * rhs
    leaf = {}
    for z in range(bz):
        for y in range(0, by, 2):
            rows = own[z, y : y + 2].reshape(2 * bx * rhs, pts)
            value = dot(basis[...], rows, ((1,), (1,))).astype(BF16)
            for k in range(2):
                tile = value[:, 128 * k : 128 * (k + 1)]
                leaf[z, y + k] = tile
                mom[z * by + y + k] = tile
                (z_low if z < 2 else z_high)[z % 2 * by + y + k] = tile
                at = base + (z * 2 + k) * rank
                (y_low if y == 0 else y_high)[at : at + rank] = tile
    sums = [None, None]
    for i in range(2):
        for j in range(2):
            for l in range(2):
                cols = jnp.concatenate([leaf[2 * z + l, 2 * y + j] for z in range(2) for y in range(2)], axis=1)
                part = dot(transfer[4 * i + 2 * j + l], cols)
                sums[i] = part if sums[i] is None else sums[i] + part
    blocks = lane_blocks(rank, width)
    first = bz * by
    one = []
    for z in range(2):
        whole = []
        for y in range(2):
            at = 128 * (z * 2 + y)
            whole.append(sums[0][:, at : at + 128] + roll(sums[1][:, at : at + 128], -width))
        packed = jnp.where(
            blocks == 0,
            whole[0],
            jnp.where(
                blocks == 1,
                roll(whole[0], -width),
                jnp.where(blocks == 2, roll(whole[1], 2 * width), roll(whole[1], width)),
            ),
        ).astype(BF16)
        one.append(packed)
        mom[first + z] = packed
        z_high[2 * by + z] = packed
        z_low[2 * by + z] = packed
        at = base + (2 * bz + z) * rank
        y_high[at : at + rank] = packed
        y_low[at : at + rank] = packed
    total = None
    for j in range(2):
        for i in range(2):
            part = dot(transfer[4 * i + 2 * j], one[0]) + dot(transfer[4 * i + 2 * j + 1], one[1])
            part = roll(part, -width * (2 * j + i))
            total = part if total is None else total + part
    total = total.astype(BF16)
    z_high[2 * by + 2] = total
    z_low[2 * by + 2] = total
    two[0] = total


class Reader:
    def __init__(self, refs):
        self.refs = iter(refs)

    def take(self, count):
        return [next(self.refs) for _ in range(count)]

    def faces(self, geo):
        if geo["nx"] == 2:
            (both,) = self.take(1)
            return both.at[1], both.at[0]
        before, after = self.take(2)
        return before.at[0], after.at[0]


def second_kernel(geo, *refs):
    nz, bx, by, bz, rhs, rank = (geo[k] for k in ("nz", "bx", "by", "bz", "rhs", "rank"))
    read = Reader(refs)
    (own,) = read.take(1)
    before, after = read.faces(geo)
    mom, prev, nxt, mine = read.take(4)
    far = read.take(geo["extra_z"])
    c_high, c_low, wide, y_high, y_low = read.take(5)
    leaf = bz * by
    for z in range(bz + 4):
        for y in range(by):
            if z < 2:
                tile = prev[z * by + y]
            elif z >= bz + 2:
                tile = nxt[(z - bz - 2) * by + y]
            else:
                tile = mom[(z - 2) * by + y]
            wide[z * by + y] = tile
    first = (bz + 4) * by
    for z in range(2):
        wide[first + z] = prev[2 * by + z]
        wide[first + 2 + z] = mom[leaf + z]
        wide[first + 4 + z] = nxt[2 * by + z]

    def load(key):
        if key == 0:
            return mine[0]
        if key == 1:
            return nxt[2 * by + 2]
        if key == nz - 1:
            return prev[2 * by + 2]
        return far[key - 2][0]

    for t, tile in enumerate(assemble([(k, 0) for k in range(nz)], rhs, load)):
        wide[first + 6 + t] = tile
    for out, z in ((c_high, bz - 1), (c_low, 0)):
        for y in range(by):
            out[y, 0] = before[z, y]
            out[y, 1 : bx + 1] = own[z, y]
            out[y, bx + 1] = after[z, y]
    base = 2 * bz * rhs
    for out, y in ((y_high, by - 1), (y_low, 0)):
        for k, s in enumerate((before, after)):
            for z in range(bz):
                at = (k * bz + z) * rhs
                out[at : at + rhs] = s[z, y]
        start = by - 2 if y else 0
        for zh in range(4):
            s = prev if zh < 2 else nxt
            for yy in range(2):
                at = base + (zh * 2 + yy) * rank
                out[at : at + rank] = s[zh % 2 * by + start + yy]
        for side, s in enumerate((prev, nxt)):
            for z in range(2):
                at = base + (8 + side * 2 + z) * rank
                out[at : at + rank] = s[2 * by + z]


def third_kernel(geo, *refs):
    nx, nz, xs, bx, by, bz, rhs, rank = (geo[k] for k in ("nx", "nz", "xs", "bx", "by", "bz", "rhs", "rank"))
    read = Reader(refs)
    prev, nxt = read.take(2)
    sources = read.take(xs)
    far = read.take(geo["extra_x"])
    y_high, y_low, two = read.take(3)
    base = 2 * (bx + 2) * rhs
    first = (bz + 4) * by
    for out, y in ((y_high, by - 1), (y_low, 0)):
        for k, s in enumerate((prev, nxt)):
            at = k * (bx + 2) * rhs
            out[at : at + (bx + 2) * rhs] = s[y].reshape((bx + 2) * rhs, s.shape[3])
        start = by - 2 if y else 0
        for k in range(1, xs):
            for z in range(bz + 4):
                for yy in range(2):
                    at = base + (((k - 1) * (bz + 4) + z) * 2 + yy) * rank
                    out[at : at + rank] = sources[k][z * by + start + yy]
            for z in range(6):
                at = base + ((xs - 1) * (bz + 4) * 2 + (k - 1) * 6 + z) * rank
                out[at : at + rank] = sources[k][first + z]
    per = 128 // rhs
    order = [((s, b // per), b % per) for s in range(nx) for b in range(nz)]

    def load(key):
        s, t = key
        if s == 0:
            return sources[0][first + 6 + t]
        if s == 1:
            return sources[xs - 1][first + 6 + t]
        if s == nx - 1:
            return sources[1][first + 6 + t]
        return far[s - 2][t]

    for t, tile in enumerate(assemble(order, rhs, load)):
        at = base + ((xs - 1) * (2 * (bz + 4) + 6) + t) * rank
        y_high[at : at + rank] = tile
        y_low[at : at + rank] = tile
        two[t] = tile


def near_weights(inverse, near_blocks, codes):
    return jnp.concatenate([near_blocks[inverse[c]] for c in codes], axis=1)


def find_inverse(table, inverse, count):
    for s in range(count):
        ox, oy, oz = (table[d, s] + 1 for d in range(3))
        inverse[(ox * 3 + oy) * 3 + oz] = s


def store_windows(shifts, at, stride, blocks, width, mid, before, after):
    shifts[2 * stride + at] = mid
    mid = mid.astype(F32)
    same = before is after
    before = before.astype(F32)
    after = before if same else after.astype(F32)
    shifts[at] = roll(jnp.where(blocks >= 2, before, mid), 2 * width).astype(BF16)
    shifts[stride + at] = roll(jnp.where(blocks >= 3, before, mid), width).astype(BF16)
    shifts[3 * stride + at] = roll(jnp.where(blocks < 1, after, mid), -width).astype(BF16)
    shifts[4 * stride + at] = roll(jnp.where(blocks < 2, after, mid), -2 * width).astype(BF16)


def near_kernel(geo, *refs):
    xs, bx, by, bz, rhs, rank = (geo[k] for k in ("xs", "bx", "by", "bz", "rhs", "rank"))
    read = Reader(refs)
    table, near_blocks, own = read.take(3)
    before, after = read.faces(geo)
    cz_prev, cz_next = read.take(2)
    y1, y2 = read.take(2), read.take(2)
    sources = read.take(xs)
    out, shifts, wide, inverse = read.take(4)
    pts = wide.shape[3]
    stencil = near_blocks.shape[0]
    find_inverse(table, inverse, stencil)
    rows = (bx + 2) * rhs
    for z in range(bz + 2):
        outer = z in (0, bz + 1)
        for k, y in enumerate((0, by + 1)):
            if outer:
                wide[z, y] = jnp.zeros((rows, pts), BF16)
                continue
            at = (z - 1) * rhs
            wide[z, y, 0:rhs] = y2[k][at : at + rhs]
            wide[z, y, rhs : rows - rhs] = y1[k][bx * at : bx * (at + rhs)]
            wide[z, y, rows - rhs :] = y2[k][bz * rhs + at : bz * rhs + at + rhs]
        for y in range(1, by + 1):
            if outer:
                wide[z, y] = (cz_prev if z == 0 else cz_next)[y - 1].reshape(rows, pts)
                continue
            wide[z, y, 0:rhs] = before[z - 1, y - 1]
            wide[z, y, rhs : rows - rhs] = own[z - 1, y - 1].reshape(bx * rhs, pts)
            wide[z, y, rows - rhs :] = after[z - 1, y - 1]
    weights = near_weights(inverse, near_blocks, range(stencil))

    def step(number, carry):
        z = number // (by // 2)
        y = number % (by // 2) * 2
        windows = []
        for ox in range(3):
            for oy in range(3):
                for oz in range(3):
                    window = wide[z + oz, pl.ds(y + oy, 2), ox * rhs : (ox + bx) * rhs, :]
                    windows.append(window.reshape(2 * bx * rhs, pts))
        out[number] = dot(jnp.concatenate(windows, axis=1), weights, ((1,), (1,)))
        return carry

    lax.fori_loop(0, bz * by // 2, step, 0)
    blocks = lane_blocks(rank, rhs)
    for z in range(bz + 4):
        for y in range(by):
            tiles = [s[z * by + y] for s in sources]
            store_windows(
                shifts, z * (by + 4) + y + 2, (bz + 4) * (by + 4), blocks, rhs, tiles[0], tiles[1], tiles[-1]
            )


def weight_kernel(coupling_in, coarse_in, transfer, coupling, coarse, down_one, down_zero):
    entries, rank = coupling_in.shape[1:3]
    for level in range(2):
        coupling[level] = jnp.concatenate([coupling_in[level, e] for e in range(entries)], axis=1)
    nx, ny, nz = coarse_in.shape[:3]
    coarse[...] = jnp.concatenate(
        [coarse_in[x, y, z] for y in range(ny) for x in range(nx) for z in range(nz)], axis=1
    )
    turned = [transfer[c].astype(F32).T.astype(BF16) for c in range(8)]
    for c in range(8):
        down_one[c * rank : (c + 1) * rank] = turned[c]
    for k in range(4):
        down_zero[k] = jnp.concatenate([turned[k], turned[4 + k]], axis=1)


def final_kernel(geo, *refs):
    nx, ny, nz, xs, bx, by, bz, rhs, rank = (
        geo[k] for k in ("nx", "ny", "nz", "xs", "bx", "by", "bz", "rhs", "rank")
    )
    width = rhs
    read = Reader(refs)
    counts, near_table, far_table = read.take(3)
    near, near_blocks, basis, coupling, coarse, down_one, down_zero, _ = read.take(8)
    sources = read.take(xs)
    y1, y2, y3 = read.take(2), read.take(2), read.take(2)
    (mine_two,) = read.take(1)
    far_two = read.take(geo["extra_y"])
    out, shifts = read.take(2)
    ones, corners, planes, inverse, sems = read.take(5)
    pts = basis.shape[1]
    blocks = lane_blocks(rank, width)
    stencil = near_blocks.shape[0]
    entries = coupling.shape[2] // rank
    base1 = bz * bx * rhs
    base2 = 2 * bz * rhs
    base3 = 2 * (bx + 2) * rhs
    first = (bz + 4) * by

    def leaf_tile(k, z, side, yy):
        if k > 0:
            return tile_at(y3[side], base3 + (((k - 1) * (bz + 4) + z + 2) * 2 + yy) * rank, rank)
        if 0 <= z < bz:
            return tile_at(y1[side], base1 + (z * 2 + yy) * rank, rank)
        zh = z + 2 if z < 0 else z - bz + 2
        return tile_at(y2[side], base2 + (zh * 2 + yy) * rank, rank)

    for z in range(-2, bz + 2):
        for side in range(2):
            for yy in range(2):
                tiles = [leaf_tile(k, z, side, yy) for k in range(xs)]
                at = (z + 2) * (by + 4) + yy + side * (by + 2)
                store_windows(shifts, at, (bz + 4) * (by + 4), blocks, width, tiles[0], tiles[1], tiles[-1])

    def one_tile(k, zb, z, yb):
        if yb == 1:
            return sources[k][first + zb * 2 + z]
        side = yb // 2
        if k > 0:
            return tile_at(y3[side], base3 + ((xs - 1) * (bz + 4) * 2 + (k - 1) * 6 + zb * 2 + z) * rank, rank)
        if zb == 1:
            return tile_at(y1[side], base1 + (2 * bz + z) * rank, rank)
        return tile_at(y2[side], base2 + (8 + (zb // 2) * 2 + z) * rank, rank)

    odd = blocks % 2 == 1
    upper = blocks >= 2

    def swap(value):
        return jnp.where(odd, roll(value, width), roll(value, -width))

    for zb in range(3):
        for z in range(2):
            rows = []
            for yb in range(3):
                mid = one_tile(0, zb, z, yb).astype(F32)
                before = one_tile(1, zb, z, yb).astype(F32)
                after = before if xs == 2 else one_tile(2, zb, z, yb).astype(F32)
                rows.append([
                    before,
                    swap(jnp.where(odd, before, mid)),
                    mid,
                    swap(jnp.where(odd, mid, after)),
                    after,
                ])
            for k in range(5):
                low, mid, high = (rows[yb][k] for yb in range(3))
                group = [
                    low,
                    roll(jnp.where(upper, low, mid), 2 * width),
                    mid,
                    roll(jnp.where(upper, mid, high), 2 * width),
                    high,
                ]
                for m in range(5):
                    ones[(k * 5 + m) * 6 + 2 * zb + z] = group[m].astype(BF16)

    start_two = base3 + (xs - 1) * (2 * (bz + 4) + 6) * rank
    per = 128 // width

    def two_tile(s, t):
        if s == 0:
            return mine_two[t]
        if s == 1 or s == ny - 1:
            return tile_at(y3[1 if s == 1 else 0], start_two + t * rank, rank)
        return far_two[s - 2][t]

    stacked = []
    for s in range(ny):
        for b in range(nz * nx):
            tile = two_tile(s, b // per).astype(F32)
            stacked.append(jnp.where(blocks == b % per, tile, 0.0).astype(BF16))
    two = dot(coarse[...], jnp.concatenate(stacked, axis=0))
    two = two + roll(two, 2 * width)
    two = (two + roll(two, width)).astype(BF16)

    starts = []
    for e in range(entries):
        ox, oy, oz = (far_table[d, 1, e] + 2 for d in range(3))
        starts.append((ox * 5 + oy) * 6 + oz)
    columns = [jnp.concatenate([ones[s + z] for s in starts], axis=0) for z in range(2)]
    local_one = dot(coupling[1], jnp.concatenate(columns, axis=1))
    from_two = dot(down_one[...], two)
    ups = []
    for z in range(2):
        total = local_one[:, 128 * z : 128 * (z + 1)]
        for j in range(2):
            for i in range(2):
                child = 4 * i + 2 * j + z
                part = from_two[child * rank : (child + 1) * rank]
                total = total + jnp.where(blocks == 2 * j + i, part, 0.0)
        total = total.astype(BF16).astype(F32)
        half = roll(total, 2 * width)
        for up in (
            jnp.where(blocks == 0, total, jnp.where(blocks == 3, half, roll(total, width))),
            jnp.where(blocks == 0, half, jnp.where(blocks == 3, total, roll(total, -width))),
        ):
            ups.append(
                jnp.concatenate(
                    [jnp.where(odd, 0.0, up).astype(BF16), jnp.where(odd, up, 0.0).astype(BF16)], axis=0
                )
            )
    ups = jnp.concatenate(ups, axis=1)
    local = {}
    for j in range(2):
        for l in range(2):
            part = dot(down_zero[2 * j + l], ups)
            for z in range(2):
                for y in range(2):
                    at = 128 * (2 * z + y)
                    local[2 * z + l, 2 * y + j] = part[:, at : at + 128]

    find_inverse(near_table, inverse, stencil)
    for oy, yk in ((0, 0), (2, 1)):
        for oz, zk in ((0, 0), (2, 1)):
            weights = near_weights(inverse, near_blocks, [(ox * 3 + oy) * 3 + oz for ox in range(3)])
            windows = []
            for ox in range(3):
                at = (zk * (bx + 2) + ox) * rhs
                windows.append(y3[yk][at : at + bx * rhs])
            corners[yk, zk] = dot(jnp.concatenate(windows, axis=1), weights, ((1,), (1,)))

    lane = lax.broadcasted_iota(jnp.int32, (rhs, pts), 1)
    starts = []
    for e in range(entries):
        ox, oy, oz = (far_table[d, 0, e] + 2 for d in range(3))
        starts.append((ox * (bz + 4) + oz) * (by + 4) + oy)
    copies = []
    for z in range(bz):
        for half in range(by // 2):
            y = 2 * half
            columns = [
                jnp.concatenate([shifts[s + z * (by + 4) + y + k] for s in starts], axis=0) for k in range(2)
            ]
            total = dot(coupling[0], jnp.concatenate(columns, axis=1))
            total = total + jnp.concatenate([local[z, y], local[z, y + 1]], axis=1)
            result = dot(total.astype(BF16), basis[...], ((0,), (0,))) + near[z * (by // 2) + half]
            for k in range(2):
                block = result[k * bx * rhs : (k + 1) * bx * rhs]
                if y + k in (0, by - 1) and z in (0, bz - 1):
                    block = block + corners[0 if y + k == 0 else 1, 0 if z == 0 else 1]
                for x in range(bx):
                    keep = lane < counts[x, y + k, z]
                    planes[z, x, y + k] = jnp.where(keep, block[x * rhs : (x + 1) * rhs], 0.0)
        copies.append(pltpu.make_async_copy(planes.at[z], out.at[:, :, z], sems.at[z]))
        copies[-1].start()
    for c in copies:
        c.wait()


def body(charges, counts, near_offsets, near_blocks, leaf_basis, transfer, far_offsets, coupling, coarse_coupling):
    bx, by, bz, rhs, pts = charges.shape
    rank = leaf_basis.shape[0]
    entries = far_offsets.shape[1]
    stencil = near_blocks.shape[0]
    nx, ny, nz = (lax.axis_size(a) for a in ("gx", "gy", "gz"))
    assert (bx, by, bz) == (4, 4, 4) and bx * rhs == 128 and pts == 128
    xs = 2 if nx == 2 else 3
    geo = dict(nx=nx, ny=ny, nz=nz, xs=xs, bx=bx, by=by, bz=bz, rhs=rhs, rank=rank)
    geo["extra_x"] = max(nx - 3, 0)
    geo["extra_z"] = max(nz - 3, 0)
    geo["extra_y"] = max(ny - 3, 0)
    per = 128 // rhs
    tiles_z = -(-nz // per)
    tiles_x = -(-nx * nz // per)

    def shape(*dims, dtype=BF16):
        return jax.ShapeDtypeStruct(dims, dtype)

    def part(kernel):
        return functools.partial(kernel, geo)

    near_table = near_offsets.T
    far_table = far_offsets.transpose(2, 0, 1)

    token = run(start_kernel, shape(8, 128, dtype=jnp.int32), (), flops=10**10)
    side = shape(2 * by + 3, rank, 128)
    message = shape(bz * bx * rhs + (bz * 2 + 2) * rank, 128)
    own, faces, mom, z_high, z_low, y_high, y_low, two = run(
        first_kernel,
        (
            shape(bz, by, bx, rhs, pts),
            shape(2, bz, by, rhs, pts),
            shape(bz * by + 2, rank, 128),
            side,
            side,
            message,
            message,
            shape(1, rank, 128),
        ),
        (token, counts, charges, leaf_basis, transfer),
        hbm=(1, 2, 3, 4),
        scratch=[
            pltpu.SMEM(counts.shape, jnp.int32),
            pltpu.VMEM(charges.shape, BF16),
            pltpu.VMEM(leaf_basis.shape, BF16),
            pltpu.VMEM(transfer.shape, BF16),
            pltpu.SemaphoreType.DMA((3 + bx,)),
        ],
    )
    mz_prev = from_shift(z_high, "gz", nz, -1)
    mz_next = from_shift(z_low, "gz", nz, 1)
    if nx == 2:
        faces = [from_shift(faces, "gx", nx, 1)]
    else:
        faces = [from_shift(faces[1:], "gx", nx, -1), from_shift(faces[:1], "gx", nx, 1)]
    extra = [from_shift(two, "gz", nz, s) for s in range(2, nz - 1)]
    y1 = [from_shift(y_high, "gy", ny, -1), from_shift(y_low, "gy", ny, 1)]

    weights = run(
        weight_kernel,
        (
            shape(2, rank, entries * rank),
            shape(rank, nx * ny * nz * rank),
            shape(8 * rank, rank),
            shape(4, rank, 2 * rank),
        ),
        (coupling, coarse_coupling, transfer),
    )

    charge = shape(by, bx + 2, rhs, pts)
    message = shape(2 * bz * rhs + 12 * rank, 128)
    c_high, c_low, wide, y_high, y_low = run(
        part(second_kernel),
        (charge, charge, shape((bz + 4) * by + 6 + tiles_z, rank, 128), message, message),
        (own, *faces, mom, mz_prev, mz_next, two, *extra),
    )
    if nx == 2:
        sources = [wide, from_shift(wide, "gx", nx, 1)]
    else:
        sources = [wide, from_shift(wide, "gx", nx, -1), from_shift(wide, "gx", nx, 1)]
    cz_prev = from_shift(c_high, "gz", nz, -1)
    cz_next = from_shift(c_low, "gz", nz, 1)
    y2 = [from_shift(y_high, "gy", ny, -1), from_shift(y_low, "gy", ny, 1)]
    extra = [from_shift(wide[-tiles_z:], "gx", nx, s) for s in range(2, nx - 1)]

    message = shape(2 * (bx + 2) * rhs + ((xs - 1) * (2 * (bz + 4) + 6) + tiles_x) * rank, 128)
    y_high, y_low, two = run(
        part(third_kernel), (message, message, shape(tiles_x, rank, 128)), (cz_prev, cz_next, *sources, *extra)
    )
    y3 = [from_shift(y_high, "gy", ny, -1), from_shift(y_low, "gy", ny, 1)]
    extra = [from_shift(two, "gy", ny, s) for s in range(2, ny - 1)]

    windows = shape(5 * (bz + 4) * (by + 4), rank, 128)
    near, shifts = run(
        part(near_kernel),
        (shape(bz * by // 2, 2 * bx * rhs, pts, dtype=F32), windows),
        (near_table, near_blocks, own, *faces, cz_prev, cz_next, *y1, *y2, *sources),
        smem=(0,),
        scratch=[
            pltpu.VMEM((bz + 2, by + 2, (bx + 2) * rhs, pts), BF16),
            pltpu.SMEM((stencil,), jnp.int32),
        ],
        limit=16,
        flops=2 * bx * by * bz * rhs * pts * pts * stencil,
    )
    args = (
        counts,
        near_table,
        far_table,
        near,
        near_blocks,
        leaf_basis,
        *weights,
        shifts,
        *sources,
        *y1,
        *y2,
        *y3,
        two,
        *extra,
    )
    potentials, _ = run(
        part(final_kernel),
        (shape(bx, by, bz, rhs, pts, dtype=F32), windows),
        args,
        smem=(0, 1, 2),
        hbm_out=(0,),
        aliases={10: 1},
        limit=24,
        scratch=[
            pltpu.VMEM((5 * 5 * 6, rank, 128), BF16),
            pltpu.VMEM((2, 2, bx * rhs, pts), F32),
            pltpu.VMEM((bz, bx, by, rhs, pts), F32),
            pltpu.SMEM((stencil,), jnp.int32),
            pltpu.SemaphoreType.DMA((bz,)),
        ],
    )
    return potentials


def solution(mesh):
    in_specs = (
        P("gx", "gy", "gz", None, None),
        P("gx", "gy", "gz"),
        P(),
        P(),
        P(),
        P(),
        P(),
        P(),
        P(),
    )
    out_specs = P("gx", "gy", "gz", None, None)

    return jax.shard_map(body, mesh=mesh, in_specs=in_specs, out_specs=out_specs, check_vma=False)
```

```python
import functools

import jax
import jax.numpy as jnp
from jax import lax
from jax.experimental import pallas as pl
from jax.experimental.pallas import tpu as pltpu
from jax.sharding import PartitionSpec as P


F32 = jnp.float32
BF16 = jnp.bfloat16


def from_shift(value, axis, size, shift):
    return lax.ppermute(value, axis, [(i, (i - shift) % size) for i in range(size)])


def spec_vmem():
    return pl.BlockSpec(memory_space=pltpu.VMEM)


def spec_smem():
    return pl.BlockSpec(memory_space=pltpu.SMEM)


def run(kernel, out_shape, args, smem=(), anywhere=(), scratch=(), flops=None, limit=8, hbm_out=(), aliases=None):
    def spec(i):
        if i in anywhere:
            return pl.BlockSpec(memory_space=pl.ANY)
        return spec_smem() if i in smem else spec_vmem()

    cost = None
    if flops is not None:
        cost = pl.CostEstimate(flops=flops, transcendentals=0, bytes_accessed=0)
    count = len(out_shape) if isinstance(out_shape, tuple) else 1
    outs = tuple(pl.BlockSpec(memory_space=pltpu.HBM) if i in hbm_out else spec_vmem() for i in range(count))
    return pl.pallas_call(
        kernel,
        out_shape=out_shape,
        in_specs=[spec(i) for i in range(len(args))],
        out_specs=outs if isinstance(out_shape, tuple) else outs[0],
        input_output_aliases=aliases or {},
        scratch_shapes=scratch,
        compiler_params=pltpu.CompilerParams(vmem_limit_bytes=limit * 1024 * 1024),
        cost_estimate=cost,
    )(*args)


def lane_blocks(rows, width):
    return lax.broadcasted_iota(jnp.int32, (rows, 128), 1) // width


def roll(value, shift):
    shift = shift % 128
    return value if shift == 0 else pltpu.roll(value, shift, 1)


def dot(a, b, dims=((1,), (0,))):
    return lax.dot_general(a, b, (dims, ((), ())), preferred_element_type=F32)


def assemble(sources, width, load):
    per = 128 // width
    out = []
    for start in range(0, len(sources), per):
        total = None
        for d, (key, b) in enumerate(sources[start : start + per]):
            moved = roll(load(key).astype(F32), width * (d - b))
            if total is None:
                total = moved
                blocks = lane_blocks(moved.shape[0], width)
            else:
                total = jnp.where(blocks == d, moved, total)
        out.append(total.astype(BF16))
    return out


def tile_at(ref, start, rank):
    return ref[start : start + rank, :]


def start_kernel(out):
    out[...] = jnp.zeros(out.shape, out.dtype)


def first_kernel(token, live, charges, basis, transfer, own, faces, mom, z_high, z_low, y_high, y_low, two):
    bx, by, bz, rhs, pts = charges.shape
    rank = basis.shape[0]
    width = rhs
    for x in range(bx):
        for y in range(by):
            for z in range(bz):
                value = (charges[x, y, z].astype(F32) * live[x, y, z : z + 1]).astype(BF16)
                own[z, y, x] = value
                if x == 0:
                    faces[0, z, y] = value
                if x == bx - 1:
                    faces[1, z, y] = value
                at = (z * bx + x) * rhs
                if y == 0:
                    y_low[at : at + rhs] = value
                if y == by - 1:
                    y_high[at : at + rhs] = value
    base = bz * bx * rhs
    leaf = {}
    for z in range(bz):
        for y in range(0, by, 2):
            rows = own[z, y : y + 2].reshape(2 * bx * rhs, pts)
            value = dot(basis[...], rows, ((1,), (1,))).astype(BF16)
            for k in range(2):
                tile = value[:, 128 * k : 128 * (k + 1)]
                leaf[z, y + k] = tile
                mom[z * by + y + k] = tile
                (z_low if z < 2 else z_high)[z % 2 * by + y + k] = tile
                at = base + (z * 2 + k) * rank
                (y_low if y == 0 else y_high)[at : at + rank] = tile
    sums = [None, None]
    for i in range(2):
        for j in range(2):
            for l in range(2):
                cols = jnp.concatenate([leaf[2 * z + l, 2 * y + j] for z in range(2) for y in range(2)], axis=1)
                part = dot(transfer[4 * i + 2 * j + l], cols)
                sums[i] = part if sums[i] is None else sums[i] + part
    blocks = lane_blocks(rank, width)
    first = bz * by
    one = []
    for z in range(2):
        whole = []
        for y in range(2):
            at = 128 * (z * 2 + y)
            whole.append(sums[0][:, at : at + 128] + roll(sums[1][:, at : at + 128], -width))
        packed = jnp.where(
            blocks == 0,
            whole[0],
            jnp.where(
                blocks == 1,
                roll(whole[0], -width),
                jnp.where(blocks == 2, roll(whole[1], 2 * width), roll(whole[1], width)),
            ),
        ).astype(BF16)
        one.append(packed)
        mom[first + z] = packed
        z_high[2 * by + z] = packed
        z_low[2 * by + z] = packed
        at = base + (2 * bz + z) * rank
        y_high[at : at + rank] = packed
        y_low[at : at + rank] = packed
    total = None
    for j in range(2):
        for i in range(2):
            part = dot(transfer[4 * i + 2 * j], one[0]) + dot(transfer[4 * i + 2 * j + 1], one[1])
            part = roll(part, -width * (2 * j + i))
            total = part if total is None else total + part
    total = total.astype(BF16)
    z_high[2 * by + 2] = total
    z_low[2 * by + 2] = total
    two[0] = total


class Reader:
    def __init__(self, refs):
        self.refs = iter(refs)

    def take(self, count):
        return [next(self.refs) for _ in range(count)]

    def faces(self, geo):
        if geo["nx"] == 2:
            (both,) = self.take(1)
            return both.at[1], both.at[0]
        before, after = self.take(2)
        return before.at[0], after.at[0]


def second_kernel(geo, *refs):
    nz, bx, by, bz, rhs, rank = (geo[k] for k in ("nz", "bx", "by", "bz", "rhs", "rank"))
    read = Reader(refs)
    (own,) = read.take(1)
    before, after = read.faces(geo)
    mom, prev, nxt, mine = read.take(4)
    far = read.take(geo["extra_z"])
    c_high, c_low, wide, y_high, y_low = read.take(5)
    for z in range(bz + 4):
        for y in range(by):
            if z < 2:
                tile = prev[z * by + y]
            elif z >= bz + 2:
                tile = nxt[(z - bz - 2) * by + y]
            else:
                tile = mom[(z - 2) * by + y]
            wide[z * by + y] = tile
    first = (bz + 4) * by

    def load(key):
        if key == 0:
            return mine[0]
        if key == 1:
            return nxt[2 * by + 2]
        if key == nz - 1:
            return prev[2 * by + 2]
        return far[key - 2][0]

    for t, tile in enumerate(assemble([(k, 0) for k in range(nz)], rhs, load)):
        wide[first + t] = tile
    for out, z in ((c_high, bz - 1), (c_low, 0)):
        for y in range(by):
            out[y, 0] = before[z, y]
            out[y, 1 : bx + 1] = own[z, y]
            out[y, bx + 1] = after[z, y]
    base = 2 * bz * rhs
    for out, y in ((y_high, by - 1), (y_low, 0)):
        for k, s in enumerate((before, after)):
            for z in range(bz):
                at = (k * bz + z) * rhs
                out[at : at + rhs] = s[z, y]
        start = by - 2 if y else 0
        for zh in range(4):
            s = prev if zh < 2 else nxt
            for yy in range(2):
                at = base + (zh * 2 + yy) * rank
                out[at : at + rank] = s[zh % 2 * by + start + yy]
        for side, s in enumerate((prev, nxt)):
            for z in range(2):
                at = base + (8 + side * 2 + z) * rank
                out[at : at + rank] = s[2 * by + z]


def third_kernel(geo, *refs):
    nx, nz, xs, bx, by, bz, rhs, rank = (geo[k] for k in ("nx", "nz", "xs", "bx", "by", "bz", "rhs", "rank"))
    read = Reader(refs)
    prev, nxt = read.take(2)
    sources = read.take(xs)
    mom, mz_prev, mz_next = read.take(3)
    y1, y2 = read.take(2), read.take(2)
    far = read.take(geo["extra_x"])
    y_high, y_low, one, two = read.take(4)
    base1 = bz * bx * rhs
    base2 = 2 * bz * rhs
    for yb in range(3):
        for zb in range(3):
            for z in range(2):
                if yb == 1:
                    tile = mom[bz * by + z] if zb == 1 else (mz_prev if zb == 0 else mz_next)[2 * by + z]
                elif zb == 1:
                    tile = tile_at(y1[yb // 2], base1 + (2 * bz + z) * rank, rank)
                else:
                    tile = tile_at(y2[yb // 2], base2 + (8 + (zb // 2) * 2 + z) * rank, rank)
                one[(yb * 3 + zb) * 2 + z] = tile
    base = 2 * (bx + 2) * rhs
    first = (bz + 4) * by
    for out, y in ((y_high, by - 1), (y_low, 0)):
        for k, s in enumerate((prev, nxt)):
            at = k * (bx + 2) * rhs
            out[at : at + (bx + 2) * rhs] = s[y].reshape((bx + 2) * rhs, s.shape[3])
        start = by - 2 if y else 0
        for k in range(1, xs):
            for z in range(bz + 4):
                for yy in range(2):
                    at = base + (((k - 1) * (bz + 4) + z) * 2 + yy) * rank
                    out[at : at + rank] = sources[k][z * by + start + yy]
    per = 128 // rhs
    order = [((s, b // per), b % per) for s in range(nx) for b in range(nz)]

    def load(key):
        s, t = key
        if s == 0:
            return sources[0][first + t]
        if s == 1:
            return sources[xs - 1][first + t]
        if s == nx - 1:
            return sources[1][first + t]
        return far[s - 2][t]

    for t, tile in enumerate(assemble(order, rhs, load)):
        at = base + ((xs - 1) * 2 * (bz + 4) + t) * rank
        y_high[at : at + rank] = tile
        y_low[at : at + rank] = tile
        two[t] = tile


def near_weights(inverse, near_blocks, codes):
    return jnp.concatenate([near_blocks[inverse[c]] for c in codes], axis=1)


def find_inverse(table, inverse, count):
    for s in range(count):
        ox, oy, oz = (table[d, s] + 1 for d in range(3))
        inverse[(ox * 3 + oy) * 3 + oz] = s


def store_windows(shifts, at, stride, blocks, width, mid, before, after):
    shifts[2 * stride + at] = mid
    mid = mid.astype(F32)
    same = before is after
    before = before.astype(F32)
    after = before if same else after.astype(F32)
    shifts[at] = roll(jnp.where(blocks >= 2, before, mid), 2 * width).astype(BF16)
    shifts[stride + at] = roll(jnp.where(blocks >= 3, before, mid), width).astype(BF16)
    shifts[3 * stride + at] = roll(jnp.where(blocks < 1, after, mid), -width).astype(BF16)
    shifts[4 * stride + at] = roll(jnp.where(blocks < 2, after, mid), -2 * width).astype(BF16)


def windows_y(blocks, width, tiles):
    low, mid, high = (t.astype(F32) for t in tiles)
    upper = blocks >= 2
    return [
        low,
        roll(jnp.where(upper, low, mid), 2 * width),
        mid,
        roll(jnp.where(upper, mid, high), 2 * width),
        high,
    ]


def near_kernel(geo, *refs):
    xs, bx, by, bz, rhs, rank = (geo[k] for k in ("xs", "bx", "by", "bz", "rhs", "rank"))
    read = Reader(refs)
    table, near_blocks, own = read.take(3)
    before, after = read.faces(geo)
    cz_prev, cz_next = read.take(2)
    y1, y2 = read.take(2), read.take(2)
    sources = read.take(xs)
    (one,) = read.take(1)
    out, shifts, ones, corner_weights, wide, inverse = read.take(6)
    pts = wide.shape[3]
    stencil = near_blocks.shape[0]
    find_inverse(table, inverse, stencil)
    rows = (bx + 2) * rhs
    for z in range(bz + 2):
        outer = z in (0, bz + 1)
        for k, y in enumerate((0, by + 1)):
            if outer:
                wide[z, y] = jnp.zeros((rows, pts), BF16)
                continue
            at = (z - 1) * rhs
            wide[z, y, 0:rhs] = y2[k][at : at + rhs]
            wide[z, y, rhs : rows - rhs] = y1[k][bx * at : bx * (at + rhs)]
            wide[z, y, rows - rhs :] = y2[k][bz * rhs + at : bz * rhs + at + rhs]
        for y in range(1, by + 1):
            if outer:
                wide[z, y] = (cz_prev if z == 0 else cz_next)[y - 1].reshape(rows, pts)
                continue
            wide[z, y, 0:rhs] = before[z - 1, y - 1]
            wide[z, y, rhs : rows - rhs] = own[z - 1, y - 1].reshape(bx * rhs, pts)
            wide[z, y, rows - rhs :] = after[z - 1, y - 1]
    weights = near_weights(inverse, near_blocks, range(stencil))

    def step(number, carry):
        z = number // (by // 2)
        y = number % (by // 2) * 2
        windows = []
        for ox in range(3):
            for oy in range(3):
                for oz in range(3):
                    window = wide[z + oz, pl.ds(y + oy, 2), ox * rhs : (ox + bx) * rhs, :]
                    windows.append(window.reshape(2 * bx * rhs, pts))
        out[number] = dot(jnp.concatenate(windows, axis=1), weights, ((1,), (1,)))
        return carry

    lax.fori_loop(0, bz * by // 2, step, 0)
    blocks = lane_blocks(rank, rhs)
    for z in range(bz + 4):
        for y in range(by):
            tiles = [s[z * by + y] for s in sources]
            store_windows(
                shifts, z * (by + 4) + y + 2, (bz + 4) * (by + 4), blocks, rhs, tiles[0], tiles[1], tiles[-1]
            )
    for z in range(6):
        for m, mid in enumerate(windows_y(blocks, rhs, [one[yb * 6 + z] for yb in range(3)])):
            ones[(10 + m) * 6 + z] = mid.astype(BF16)
            ones[(5 + m) * 6 + z] = roll(mid, rhs).astype(BF16)
            ones[(15 + m) * 6 + z] = roll(mid, -rhs).astype(BF16)
    for yk in range(2):
        for zk in range(2):
            codes = [(ox * 3 + 2 * yk) * 3 + 2 * zk for ox in range(3)]
            corner_weights[yk, zk] = near_weights(inverse, near_blocks, codes)


def weight_kernel(coupling_in, coarse_in, transfer, coupling, coarse, down_one, down_zero):
    entries, rank = coupling_in.shape[1:3]
    for level in range(2):
        coupling[level] = jnp.concatenate([coupling_in[level, e] for e in range(entries)], axis=1)
    nx, ny, nz = coarse_in.shape[:3]
    coarse[...] = jnp.concatenate(
        [coarse_in[x, y, z] for y in range(ny) for x in range(nx) for z in range(nz)], axis=1
    )
    turned = [transfer[c].astype(F32).T.astype(BF16) for c in range(8)]
    for c in range(8):
        down_one[c * rank : (c + 1) * rank] = turned[c]
    for k in range(4):
        down_zero[k] = jnp.concatenate([turned[k], turned[4 + k]], axis=1)


def final_kernel(geo, *refs):
    nx, ny, nz, xs, bx, by, bz, rhs, rank = (
        geo[k] for k in ("nx", "ny", "nz", "xs", "bx", "by", "bz", "rhs", "rank")
    )
    width = rhs
    read = Reader(refs)
    far_in, live, near, corner_weights, basis, coupling, coarse, down_one, down_zero = read.take(9)
    read.take(2)
    beside = read.take(xs - 1)
    y1, y2, y3 = read.take(2), read.take(2), read.take(2)
    (mine_two,) = read.take(1)
    far_two = read.take(geo["extra_y"])
    out, shifts, ones = read.take(3)
    corners, planes, far_table, sems = read.take(4)
    table_copy = pltpu.make_async_copy(far_in, far_table, sems.at[bz])
    table_copy.start()
    blocks = lane_blocks(rank, width)
    entries = coupling.shape[2] // rank
    base1 = bz * bx * rhs
    base2 = 2 * bz * rhs
    base3 = 2 * (bx + 2) * rhs

    def leaf_tile(k, z, side, yy):
        if k > 0:
            return tile_at(y3[side], base3 + (((k - 1) * (bz + 4) + z + 2) * 2 + yy) * rank, rank)
        if 0 <= z < bz:
            return tile_at(y1[side], base1 + (z * 2 + yy) * rank, rank)
        zh = z + 2 if z < 0 else z - bz + 2
        return tile_at(y2[side], base2 + (zh * 2 + yy) * rank, rank)

    for z in range(-2, bz + 2):
        for side in range(2):
            for yy in range(2):
                tiles = [leaf_tile(k, z, side, yy) for k in range(xs)]
                at = (z + 2) * (by + 4) + yy + side * (by + 2)
                store_windows(shifts, at, (bz + 4) * (by + 4), blocks, width, tiles[0], tiles[1], tiles[-1])

    odd = blocks % 2 == 1
    for z in range(6):
        sides = [windows_y(blocks, width, [s[yb * 6 + z] for yb in range(3)]) for s in beside]
        for m in range(5):
            before, after = sides[0][m], sides[-1][m]
            ones[m * 6 + z] = before.astype(BF16)
            ones[(20 + m) * 6 + z] = after.astype(BF16)
            at = (5 + m) * 6 + z
            ones[at] = jnp.where(odd, ones[at].astype(F32), roll(before, -width)).astype(BF16)
            at = (15 + m) * 6 + z
            ones[at] = jnp.where(odd, roll(after, width), ones[at].astype(F32)).astype(BF16)

    start_two = base3 + (xs - 1) * 2 * (bz + 4) * rank
    per = 128 // width

    def two_tile(s, t):
        if s == 0:
            return mine_two[t]
        if s == 1 or s == ny - 1:
            return tile_at(y3[1 if s == 1 else 0], start_two + t * rank, rank)
        return far_two[s - 2][t]

    stacked = []
    for s in range(ny):
        for b in range(nz * nx):
            tile = two_tile(s, b // per).astype(F32)
            stacked.append(jnp.where(blocks == b % per, tile, 0.0).astype(BF16))
    two = dot(coarse[...], jnp.concatenate(stacked, axis=0))
    two = two + roll(two, 2 * width)
    two = (two + roll(two, width)).astype(BF16)

    table_copy.wait()
    starts = []
    for e in range(entries):
        ox, oy, oz = (far_table[d, 1, e] + 2 for d in range(3))
        starts.append((ox * 5 + oy) * 6 + oz)
    columns = [jnp.concatenate([ones[s + z] for s in starts], axis=0) for z in range(2)]
    local_one = dot(coupling[1], jnp.concatenate(columns, axis=1))
    from_two = dot(down_one[...], two)
    ups = []
    for z in range(2):
        total = local_one[:, 128 * z : 128 * (z + 1)]
        for j in range(2):
            for i in range(2):
                child = 4 * i + 2 * j + z
                part = from_two[child * rank : (child + 1) * rank]
                total = total + jnp.where(blocks == 2 * j + i, part, 0.0)
        total = total.astype(BF16).astype(F32)
        half = roll(total, 2 * width)
        for up in (
            jnp.where(blocks == 0, total, jnp.where(blocks == 3, half, roll(total, width))),
            jnp.where(blocks == 0, half, jnp.where(blocks == 3, total, roll(total, -width))),
        ):
            ups.append(
                jnp.concatenate(
                    [jnp.where(odd, 0.0, up).astype(BF16), jnp.where(odd, up, 0.0).astype(BF16)], axis=0
                )
            )
    ups = jnp.concatenate(ups, axis=1)
    local = {}
    for j in range(2):
        for l in range(2):
            part = dot(down_zero[2 * j + l], ups)
            for z in range(2):
                for y in range(2):
                    at = 128 * (2 * z + y)
                    local[2 * z + l, 2 * y + j] = part[:, at : at + 128]

    for yk in range(2):
        for zk in range(2):
            windows = []
            for ox in range(3):
                at = (zk * (bx + 2) + ox) * rhs
                windows.append(y3[yk][at : at + bx * rhs])
            corners[yk, zk] = dot(jnp.concatenate(windows, axis=1), corner_weights[yk, zk], ((1,), (1,)))

    starts = []
    for e in range(entries):
        ox, oy, oz = (far_table[d, 0, e] + 2 for d in range(3))
        starts.append((ox * (bz + 4) + oz) * (by + 4) + oy)
    copies = []
    for z in range(bz):
        for half in range(by // 2):
            y = 2 * half
            columns = [
                jnp.concatenate([shifts[s + z * (by + 4) + y + k] for s in starts], axis=0) for k in range(2)
            ]
            total = dot(coupling[0], jnp.concatenate(columns, axis=1))
            total = total + jnp.concatenate([local[z, y], local[z, y + 1]], axis=1)
            result = dot(total.astype(BF16), basis[...], ((0,), (0,))) + near[z * (by // 2) + half]
            for k in range(2):
                block = result[k * bx * rhs : (k + 1) * bx * rhs]
                if y + k in (0, by - 1) and z in (0, bz - 1):
                    block = block + corners[0 if y + k == 0 else 1, 0 if z == 0 else 1]
                for x in range(bx):
                    planes[z, x, y + k] = block[x * rhs : (x + 1) * rhs] * live[x, y + k, z : z + 1]
        copies.append(pltpu.make_async_copy(planes.at[z], out.at[:, :, z], sems.at[z]))
        copies[-1].start()
    for c in copies:
        c.wait()


def body(charges, counts, near_offsets, near_blocks, leaf_basis, transfer, far_offsets, coupling, coarse_coupling):
    bx, by, bz, rhs, pts = charges.shape
    rank = leaf_basis.shape[0]
    entries = far_offsets.shape[1]
    stencil = near_blocks.shape[0]
    nx, ny, nz = (lax.axis_size(a) for a in ("gx", "gy", "gz"))
    assert (bx, by, bz) == (4, 4, 4) and bx * rhs == 128 and pts == 128
    xs = 2 if nx == 2 else 3
    geo = dict(nx=nx, ny=ny, nz=nz, xs=xs, bx=bx, by=by, bz=bz, rhs=rhs, rank=rank)
    geo["extra_x"] = max(nx - 3, 0)
    geo["extra_z"] = max(nz - 3, 0)
    geo["extra_y"] = max(ny - 3, 0)
    per = 128 // rhs
    tiles_z = -(-nz // per)
    tiles_x = -(-nx * nz // per)

    def shape(*dims, dtype=BF16):
        return jax.ShapeDtypeStruct(dims, dtype)

    def part(kernel):
        return functools.partial(kernel, geo)

    live = (jnp.arange(pts, dtype=jnp.int32) < counts[..., None]).astype(F32)
    near_table = near_offsets.T
    far_table = far_offsets.transpose(2, 0, 1)

    token = run(start_kernel, shape(8, 128, dtype=jnp.int32), (), flops=10**10)
    side = shape(2 * by + 3, rank, 128)
    message = shape(bz * bx * rhs + (bz * 2 + 2) * rank, 128)
    own, faces, mom, z_high, z_low, y_high, y_low, two = run(
        first_kernel,
        (
            shape(bz, by, bx, rhs, pts),
            shape(2, bz, by, rhs, pts),
            shape(bz * by + 2, rank, 128),
            side,
            side,
            message,
            message,
            shape(1, rank, 128),
        ),
        (token, live, charges, leaf_basis, transfer),
    )
    mz_prev = from_shift(z_high, "gz", nz, -1)
    mz_next = from_shift(z_low, "gz", nz, 1)
    if nx == 2:
        faces = [from_shift(faces, "gx", nx, 1)]
    else:
        faces = [from_shift(faces[1:], "gx", nx, -1), from_shift(faces[:1], "gx", nx, 1)]
    extra = [from_shift(two, "gz", nz, s) for s in range(2, nz - 1)]
    y1 = [from_shift(y_high, "gy", ny, -1), from_shift(y_low, "gy", ny, 1)]

    weights = run(
        weight_kernel,
        (
            shape(2, rank, entries * rank),
            shape(rank, nx * ny * nz * rank),
            shape(8 * rank, rank),
            shape(4, rank, 2 * rank),
        ),
        (coupling, coarse_coupling, transfer),
    )

    charge = shape(by, bx + 2, rhs, pts)
    message = shape(2 * bz * rhs + 12 * rank, 128)
    c_high, c_low, wide, y_high, y_low = run(
        part(second_kernel),
        (charge, charge, shape((bz + 4) * by + tiles_z, rank, 128), message, message),
        (own, *faces, mom, mz_prev, mz_next, two, *extra),
    )
    if nx == 2:
        sources = [wide, from_shift(wide, "gx", nx, 1)]
    else:
        sources = [wide, from_shift(wide, "gx", nx, -1), from_shift(wide, "gx", nx, 1)]
    cz_prev = from_shift(c_high, "gz", nz, -1)
    cz_next = from_shift(c_low, "gz", nz, 1)
    y2 = [from_shift(y_high, "gy", ny, -1), from_shift(y_low, "gy", ny, 1)]
    extra = [from_shift(wide[-tiles_z:], "gx", nx, s) for s in range(2, nx - 1)]

    message = shape(2 * (bx + 2) * rhs + ((xs - 1) * 2 * (bz + 4) + tiles_x) * rank, 128)
    y_high, y_low, one, two = run(
        part(third_kernel),
        (message, message, shape(18, rank, 128), shape(tiles_x, rank, 128)),
        (cz_prev, cz_next, *sources, mom, mz_prev, mz_next, *y1, *y2, *extra),
    )
    if nx == 2:
        beside = [from_shift(one, "gx", nx, 1)]
    else:
        beside = [from_shift(one, "gx", nx, -1), from_shift(one, "gx", nx, 1)]
    y3 = [from_shift(y_high, "gy", ny, -1), from_shift(y_low, "gy", ny, 1)]
    extra = [from_shift(two, "gy", ny, s) for s in range(2, ny - 1)]

    windows = shape(5 * (bz + 4) * (by + 4), rank, 128)
    columns = shape(5 * 5 * 6, rank, 128)
    near, shifts, ones, corner_weights = run(
        part(near_kernel),
        (
            shape(bz * by // 2, 2 * bx * rhs, pts, dtype=F32),
            windows,
            columns,
            shape(2, 2, pts, 3 * pts),
        ),
        (near_table, near_blocks, own, *faces, cz_prev, cz_next, *y1, *y2, *sources, one),
        smem=(0,),
        scratch=[
            pltpu.VMEM((bz + 2, by + 2, (bx + 2) * rhs, pts), BF16),
            pltpu.SMEM((stencil,), jnp.int32),
        ],
        limit=16,
        flops=2 * bx * by * bz * rhs * pts * pts * stencil,
    )
    args = (
        far_table,
        live,
        near,
        corner_weights,
        leaf_basis,
        *weights,
        shifts,
        ones,
        *beside,
        *y1,
        *y2,
        *y3,
        two,
        *extra,
    )
    potentials, _, _ = run(
        part(final_kernel),
        (shape(bx, by, bz, rhs, pts, dtype=F32), windows, columns),
        args,
        anywhere=(0,),
        hbm_out=(0,),
        aliases={9: 1, 10: 2},
        limit=24,
        scratch=[
            pltpu.VMEM((2, 2, bx * rhs, pts), F32),
            pltpu.VMEM((bz, bx, by, rhs, pts), F32),
            pltpu.SMEM(far_table.shape, jnp.int32),
            pltpu.SemaphoreType.DMA((bz + 1,)),
        ],
    )
    return potentials


def solution(mesh):
    in_specs = (
        P("gx", "gy", "gz", None, None),
        P("gx", "gy", "gz"),
        P(),
        P(),
        P(),
        P(),
        P(),
        P(),
        P(),
    )
    out_specs = P("gx", "gy", "gz", None, None)

    return jax.shard_map(body, mesh=mesh, in_specs=in_specs, out_specs=out_specs, check_vma=False)
```

```python
import functools

import jax
import jax.numpy as jnp
from jax import lax
from jax.experimental import pallas as pl
from jax.experimental.pallas import tpu as pltpu
from jax.sharding import PartitionSpec as P


F32 = jnp.float32
BF16 = jnp.bfloat16


def from_shift(value, axis, size, shift):
    return lax.ppermute(value, axis, [(i, (i - shift) % size) for i in range(size)])


def spec_vmem():
    return pl.BlockSpec(memory_space=pltpu.VMEM)


def spec_smem():
    return pl.BlockSpec(memory_space=pltpu.SMEM)


def run(kernel, out_shape, args, smem=(), anywhere=(), scratch=(), flops=None, limit=8, hbm_out=(), aliases=None):
    def spec(i):
        if i in anywhere:
            return pl.BlockSpec(memory_space=pl.ANY)
        return spec_smem() if i in smem else spec_vmem()

    cost = None
    if flops is not None:
        cost = pl.CostEstimate(flops=flops, transcendentals=0, bytes_accessed=0)
    count = len(out_shape) if isinstance(out_shape, tuple) else 1
    outs = tuple(pl.BlockSpec(memory_space=pltpu.HBM) if i in hbm_out else spec_vmem() for i in range(count))
    return pl.pallas_call(
        kernel,
        out_shape=out_shape,
        in_specs=[spec(i) for i in range(len(args))],
        out_specs=outs if isinstance(out_shape, tuple) else outs[0],
        input_output_aliases=aliases or {},
        scratch_shapes=scratch,
        compiler_params=pltpu.CompilerParams(vmem_limit_bytes=limit * 1024 * 1024),
        cost_estimate=cost,
    )(*args)


def lane_blocks(rows, width):
    return lax.broadcasted_iota(jnp.int32, (rows, 128), 1) // width


class Masks:
    def __init__(self, rank, width):
        lanes = lax.broadcasted_iota(jnp.int16, (rank, 128), 1)
        bound = [jnp.int16(width * k) for k in range(4)]
        self.first = lanes < bound[1]
        self.lower = lanes < bound[2]
        self.last = lanes >= bound[3]
        self.odd = ((lanes >= bound[1]) & self.lower) | self.last


def roll(value, shift):
    shift = shift % 128
    return value if shift == 0 else pltpu.roll(value, shift, 1)


def dot(a, b, dims=((1,), (0,))):
    return lax.dot_general(a, b, (dims, ((), ())), preferred_element_type=F32)


def assemble(sources, width, load):
    per = 128 // width
    out = []
    for start in range(0, len(sources), per):
        total = None
        for d, (key, b) in enumerate(sources[start : start + per]):
            moved = roll(load(key).astype(F32), width * (d - b))
            if total is None:
                total = moved
                blocks = lane_blocks(moved.shape[0], width)
            else:
                total = jnp.where(blocks == d, moved, total)
        out.append(total.astype(BF16))
    return out


def tile_at(ref, start, rank):
    return ref[start : start + rank, :]


def start_kernel(out):
    out[...] = jnp.zeros(out.shape, out.dtype)


def first_kernel(token, live, charges, basis, transfer, own, faces, mom, z_high, z_low, y_high, y_low, two):
    bx, by, bz, rhs, pts = charges.shape
    rank = basis.shape[0]
    width = rhs
    for x in range(bx):
        for y in range(by):
            for z in range(bz):
                value = (charges[x, y, z].astype(F32) * live[x, y, z : z + 1]).astype(BF16)
                own[z, y, x] = value
                if x == 0:
                    faces[0, z, y] = value
                if x == bx - 1:
                    faces[1, z, y] = value
                at = (z * bx + x) * rhs
                if y == 0:
                    y_low[at : at + rhs] = value
                if y == by - 1:
                    y_high[at : at + rhs] = value
    base = bz * bx * rhs
    leaf = {}
    for z in range(bz):
        for y in range(0, by, 2):
            rows = own[z, y : y + 2].reshape(2 * bx * rhs, pts)
            value = dot(basis[...], rows, ((1,), (1,))).astype(BF16)
            for k in range(2):
                tile = value[:, 128 * k : 128 * (k + 1)]
                leaf[z, y + k] = tile
                mom[z * by + y + k] = tile
                (z_low if z < 2 else z_high)[z % 2 * by + y + k] = tile
                at = base + (z * 2 + k) * rank
                (y_low if y == 0 else y_high)[at : at + rank] = tile
    sums = [None, None]
    for i in range(2):
        for j in range(2):
            for l in range(2):
                cols = jnp.concatenate([leaf[2 * z + l, 2 * y + j] for z in range(2) for y in range(2)], axis=1)
                part = dot(transfer[4 * i + 2 * j + l], cols)
                sums[i] = part if sums[i] is None else sums[i] + part
    blocks = lane_blocks(rank, width)
    first = bz * by
    one = []
    for z in range(2):
        whole = []
        for y in range(2):
            at = 128 * (z * 2 + y)
            whole.append(sums[0][:, at : at + 128] + roll(sums[1][:, at : at + 128], -width))
        packed = jnp.where(
            blocks == 0,
            whole[0],
            jnp.where(
                blocks == 1,
                roll(whole[0], -width),
                jnp.where(blocks == 2, roll(whole[1], 2 * width), roll(whole[1], width)),
            ),
        ).astype(BF16)
        one.append(packed)
        mom[first + z] = packed
        z_high[2 * by + z] = packed
        z_low[2 * by + z] = packed
        at = base + (2 * bz + z) * rank
        y_high[at : at + rank] = packed
        y_low[at : at + rank] = packed
    total = None
    for j in range(2):
        for i in range(2):
            part = dot(transfer[4 * i + 2 * j], one[0]) + dot(transfer[4 * i + 2 * j + 1], one[1])
            part = roll(part, -width * (2 * j + i))
            total = part if total is None else total + part
    total = total.astype(BF16)
    z_high[2 * by + 2] = total
    z_low[2 * by + 2] = total
    two[0] = total


class Reader:
    def __init__(self, refs):
        self.refs = iter(refs)

    def take(self, count):
        return [next(self.refs) for _ in range(count)]

    def faces(self, geo):
        if geo["nx"] == 2:
            (both,) = self.take(1)
            return both.at[1], both.at[0]
        before, after = self.take(2)
        return before.at[0], after.at[0]


def second_kernel(geo, *refs):
    nz, bx, by, bz, rhs, rank = (geo[k] for k in ("nz", "bx", "by", "bz", "rhs", "rank"))
    read = Reader(refs)
    (own,) = read.take(1)
    before, after = read.faces(geo)
    mom, prev, nxt, mine = read.take(4)
    far = read.take(geo["extra_z"])
    c_high, c_low, wide, y_high, y_low = read.take(5)
    for z in range(bz + 4):
        for y in range(by):
            if z < 2:
                tile = prev[z * by + y]
            elif z >= bz + 2:
                tile = nxt[(z - bz - 2) * by + y]
            else:
                tile = mom[(z - 2) * by + y]
            wide[z * by + y] = tile
    first = (bz + 4) * by

    def load(key):
        if key == 0:
            return mine[0]
        if key == 1:
            return nxt[2 * by + 2]
        if key == nz - 1:
            return prev[2 * by + 2]
        return far[key - 2][0]

    for t, tile in enumerate(assemble([(k, 0) for k in range(nz)], rhs, load)):
        wide[first + t] = tile
    for out, z in ((c_high, bz - 1), (c_low, 0)):
        for y in range(by):
            out[y, 0] = before[z, y]
            out[y, 1 : bx + 1] = own[z, y]
            out[y, bx + 1] = after[z, y]
    base = 2 * bz * rhs
    for out, y in ((y_high, by - 1), (y_low, 0)):
        for k, s in enumerate((before, after)):
            for z in range(bz):
                at = (k * bz + z) * rhs
                out[at : at + rhs] = s[z, y]
        start = by - 2 if y else 0
        for zh in range(4):
            s = prev if zh < 2 else nxt
            for yy in range(2):
                at = base + (zh * 2 + yy) * rank
                out[at : at + rank] = s[zh % 2 * by + start + yy]
        for side, s in enumerate((prev, nxt)):
            for z in range(2):
                at = base + (8 + side * 2 + z) * rank
                out[at : at + rank] = s[2 * by + z]


def third_kernel(geo, *refs):
    nx, nz, xs, bx, by, bz, rhs, rank = (geo[k] for k in ("nx", "nz", "xs", "bx", "by", "bz", "rhs", "rank"))
    read = Reader(refs)
    prev, nxt = read.take(2)
    sources = read.take(xs)
    mom, mz_prev, mz_next = read.take(3)
    y1, y2 = read.take(2), read.take(2)
    far = read.take(geo["extra_x"])
    y_high, y_low, one, two = read.take(4)
    base1 = bz * bx * rhs
    base2 = 2 * bz * rhs
    for yb in range(3):
        for zb in range(3):
            for z in range(2):
                if yb == 1:
                    tile = mom[bz * by + z] if zb == 1 else (mz_prev if zb == 0 else mz_next)[2 * by + z]
                elif zb == 1:
                    tile = tile_at(y1[yb // 2], base1 + (2 * bz + z) * rank, rank)
                else:
                    tile = tile_at(y2[yb // 2], base2 + (8 + (zb // 2) * 2 + z) * rank, rank)
                one[(yb * 3 + zb) * 2 + z] = tile
    base = 2 * (bx + 2) * rhs
    first = (bz + 4) * by
    for out, y in ((y_high, by - 1), (y_low, 0)):
        for k, s in enumerate((prev, nxt)):
            at = k * (bx + 2) * rhs
            out[at : at + (bx + 2) * rhs] = s[y].reshape((bx + 2) * rhs, s.shape[3])
        start = by - 2 if y else 0
        for k in range(1, xs):
            for z in range(bz + 4):
                for yy in range(2):
                    at = base + (((k - 1) * (bz + 4) + z) * 2 + yy) * rank
                    out[at : at + rank] = sources[k][z * by + start + yy]
    per = 128 // rhs
    order = [((s, b // per), b % per) for s in range(nx) for b in range(nz)]

    def load(key):
        s, t = key
        if s == 0:
            return sources[0][first + t]
        if s == 1:
            return sources[xs - 1][first + t]
        if s == nx - 1:
            return sources[1][first + t]
        return far[s - 2][t]

    for t, tile in enumerate(assemble(order, rhs, load)):
        at = base + ((xs - 1) * 2 * (bz + 4) + t) * rank
        y_high[at : at + rank] = tile
        y_low[at : at + rank] = tile
        two[t] = tile


def near_weights(inverse, near_blocks, codes):
    return jnp.concatenate([near_blocks[inverse[c]] for c in codes], axis=1)


def find_inverse(table, inverse, count):
    for s in range(count):
        ox, oy, oz = (table[d, s] + 1 for d in range(3))
        inverse[(ox * 3 + oy) * 3 + oz] = s


def store_windows(shifts, at, stride, masks, width, mid, before, after):
    shifts[at] = roll(jnp.where(masks.lower, mid, before), 2 * width)
    shifts[stride + at] = roll(jnp.where(masks.last, before, mid), width)
    shifts[2 * stride + at] = mid
    shifts[3 * stride + at] = roll(jnp.where(masks.first, after, mid), -width)
    shifts[4 * stride + at] = roll(jnp.where(masks.lower, after, mid), 2 * width)


def windows_y(masks, width, tiles):
    low, mid, high = tiles
    return [
        low,
        roll(jnp.where(masks.lower, mid, low), 2 * width),
        mid,
        roll(jnp.where(masks.lower, high, mid), 2 * width),
        high,
    ]


def near_product(geo, weights, window, out, first, planes):
    bx, by, rhs = (geo[k] for k in ("bx", "by", "rhs"))
    rows, blocks = [], ([], [])
    for plane in planes:
        for ox in range(3):
            for oy in range(3):
                rows.append(window(first + plane, oy, ox))
                for k in range(2):
                    blocks[k].append(weights(ox, oy, plane + 1 - k))
    right = jnp.concatenate([jnp.concatenate(b, axis=1) for b in blocks], axis=0)
    value = dot(jnp.concatenate(rows, axis=1), right, ((1,), (1,)))
    for k in range(2):
        out[first + k] = value[:, 128 * k : 128 * (k + 1)]


def inner_kernel(geo, *refs):
    bx, by, bz, rhs = (geo[k] for k in ("bx", "by", "bz", "rhs"))
    read = Reader(refs)
    table, near_blocks, own = read.take(3)
    before, after = read.faces(geo)
    y1 = read.take(2)
    out, wide, inverse = read.take(3)
    pts = wide.shape[3]
    find_inverse(table, inverse, near_blocks.shape[0])
    rows = (bx + 2) * rhs
    none = jnp.zeros((rhs, pts), BF16)
    for z in range(bz):
        for k, y in enumerate((0, by + 1)):
            wide[z, y, 0:rhs] = none
            wide[z, y, rhs : rows - rhs] = y1[k][z * bx * rhs : (z + 1) * bx * rhs]
            wide[z, y, rows - rhs :] = none
        for y in range(1, by + 1):
            wide[z, y, 0:rhs] = before[z, y - 1]
            wide[z, y, rhs : rows - rhs] = own[z, y - 1].reshape(bx * rhs, pts)
            wide[z, y, rows - rhs :] = after[z, y - 1]
    empty = jnp.zeros((pts, pts), BF16)

    def weights(ox, oy, oz):
        return near_blocks[inverse[(ox * 3 + oy) * 3 + oz]] if 0 <= oz < 3 else empty

    def window(z, oy, ox):
        return wide[z, oy : oy + by, ox * rhs : (ox + bx) * rhs, :].reshape(by * bx * rhs, pts)

    for first in range(0, bz, 2):
        planes = [p for p in range(-1, 3) if 0 <= first + p < bz]
        near_product(geo, weights, window, out, first, planes)


def near_kernel(geo, *refs):
    xs, bx, by, bz, rhs, rank = (geo[k] for k in ("xs", "bx", "by", "bz", "rhs", "rank"))
    read = Reader(refs)
    table, near_blocks = read.take(2)
    read.take(1)
    cz_prev, cz_next = read.take(2)
    y2 = read.take(2)
    sources = read.take(xs)
    (one,) = read.take(1)
    out, shifts, ones, corner_weights, wide, inverse = read.take(6)
    pts = wide.shape[3]
    find_inverse(table, inverse, near_blocks.shape[0])
    rows = (bx + 2) * rhs
    for k, s in enumerate((cz_prev, cz_next)):
        for y in (0, by + 1):
            wide[k, y] = jnp.zeros((rows, pts), BF16)
        for y in range(by):
            wide[k, y + 1] = s[y].reshape(rows, pts)
    for k, z in enumerate((0, bz - 1)):
        codes = [(ox * 3 + oy) * 3 + 2 * k for ox in range(3) for oy in range(3)]
        left = [
            wide[k, oy : oy + by, ox * rhs : (ox + bx) * rhs, :].reshape(by * bx * rhs, pts)
            for ox in range(3)
            for oy in range(3)
        ]
        right = near_weights(inverse, near_blocks, codes)
        out[z] = out[z] + dot(jnp.concatenate(left, axis=1), right, ((1,), (1,)))
    none = jnp.zeros((rhs, pts), BF16)
    for yk, y in enumerate((0, by - 1)):
        for xk, x in enumerate((0, bx - 1)):
            at = xk * bz * rhs
            column = y2[yk][at : at + bz * rhs]
            column = jnp.concatenate([none, column, none], axis=0)
            left = jnp.concatenate([column[oz * rhs : (oz + bz) * rhs] for oz in range(3)], axis=1)
            right = near_weights(inverse, near_blocks, [(6 * xk + 2 * yk) * 3 + oz for oz in range(3)])
            value = dot(left, right, ((1,), (1,)))
            at = (y * bx + x) * rhs
            for z in range(bz):
                out[z, at : at + rhs] = out[z, at : at + rhs] + value[z * rhs : (z + 1) * rhs]
    masks = Masks(rank, rhs)
    for z in range(bz + 4):
        for y in range(by):
            tiles = [s[z * by + y] for s in sources]
            at = z * (by + 4) + y + 2
            store_windows(shifts, at, (bz + 4) * (by + 4), masks, rhs, tiles[0], tiles[1], tiles[-1])
    for z in range(6):
        for m, mid in enumerate(windows_y(masks, rhs, [one[yb * 6 + z] for yb in range(3)])):
            ones[(10 + m) * 6 + z] = mid
            ones[(5 + m) * 6 + z] = roll(mid, rhs)
            ones[(15 + m) * 6 + z] = roll(mid, -rhs)
    for yk in range(2):
        for zk in range(2):
            codes = [(ox * 3 + 2 * yk) * 3 + 2 * zk for ox in range(3)]
            corner_weights[yk, zk] = near_weights(inverse, near_blocks, codes)


def weight_kernel(coupling_in, coarse_in, transfer, coupling, coarse, down_one, down_zero):
    entries, rank = coupling_in.shape[1:3]
    for level in range(2):
        coupling[level] = jnp.concatenate([coupling_in[level, e] for e in range(entries)], axis=1)
    nx, ny, nz = coarse_in.shape[:3]
    coarse[...] = jnp.concatenate(
        [coarse_in[x, y, z] for y in range(ny) for x in range(nx) for z in range(nz)], axis=1
    )
    turned = [transfer[c].astype(F32).T.astype(BF16) for c in range(8)]
    for c in range(8):
        down_one[c * rank : (c + 1) * rank] = turned[c]
    for k in range(4):
        down_zero[k] = jnp.concatenate([turned[k], turned[4 + k]], axis=1)


def final_kernel(geo, *refs):
    nx, ny, nz, xs, bx, by, bz, rhs, rank = (
        geo[k] for k in ("nx", "ny", "nz", "xs", "bx", "by", "bz", "rhs", "rank")
    )
    width = rhs
    read = Reader(refs)
    far_in, live, near, corner_weights, basis, coupling, coarse, down_one, down_zero = read.take(9)
    read.take(2)
    beside = read.take(xs - 1)
    y1, y2, y3 = read.take(2), read.take(2), read.take(2)
    (mine_two,) = read.take(1)
    far_two = read.take(geo["extra_y"])
    out, shifts, ones = read.take(3)
    corners, planes, far_table, sems = read.take(4)
    table_copy = pltpu.make_async_copy(far_in, far_table, sems.at[bz])
    table_copy.start()
    blocks = lane_blocks(rank, width)
    masks = Masks(rank, width)
    entries = coupling.shape[2] // rank
    base1 = bz * bx * rhs
    base2 = 2 * bz * rhs
    base3 = 2 * (bx + 2) * rhs

    def leaf_tile(k, z, side, yy):
        if k > 0:
            return tile_at(y3[side], base3 + (((k - 1) * (bz + 4) + z + 2) * 2 + yy) * rank, rank)
        if 0 <= z < bz:
            return tile_at(y1[side], base1 + (z * 2 + yy) * rank, rank)
        zh = z + 2 if z < 0 else z - bz + 2
        return tile_at(y2[side], base2 + (zh * 2 + yy) * rank, rank)

    for z in range(-2, bz + 2):
        for side in range(2):
            for yy in range(2):
                tiles = [leaf_tile(k, z, side, yy) for k in range(xs)]
                at = (z + 2) * (by + 4) + yy + side * (by + 2)
                store_windows(shifts, at, (bz + 4) * (by + 4), masks, width, tiles[0], tiles[1], tiles[-1])

    for z in range(6):
        sides = [windows_y(masks, width, [s[yb * 6 + z] for yb in range(3)]) for s in beside]
        for m in range(5):
            before, after = sides[0][m], sides[-1][m]
            ones[m * 6 + z] = before
            ones[(20 + m) * 6 + z] = after
            at = (5 + m) * 6 + z
            ones[at] = jnp.where(masks.odd, ones[at], roll(before, -width))
            at = (15 + m) * 6 + z
            ones[at] = jnp.where(masks.odd, roll(after, width), ones[at])

    start_two = base3 + (xs - 1) * 2 * (bz + 4) * rank
    per = 128 // width

    def two_tile(s, t):
        if s == 0:
            return mine_two[t]
        if s == 1 or s == ny - 1:
            return tile_at(y3[1 if s == 1 else 0], start_two + t * rank, rank)
        return far_two[s - 2][t]

    lanes = lax.broadcasted_iota(jnp.int16, (rank, 128), 1)
    quarter = [(lanes >= jnp.int16(width * b)) & (lanes < jnp.int16(width * (b + 1))) for b in range(per)]
    stacked = []
    for s in range(ny):
        for b in range(nz * nx):
            tile = two_tile(s, b // per)
            stacked.append(jnp.where(quarter[b % per], tile, jnp.zeros_like(tile)))
    two = dot(coarse[...], jnp.concatenate(stacked, axis=0))
    two = two + roll(two, 2 * width)
    two = (two + roll(two, width)).astype(BF16)

    table_copy.wait()
    starts = []
    for e in range(entries):
        ox, oy, oz = (far_table[d, 1, e] + 2 for d in range(3))
        starts.append((ox * 5 + oy) * 6 + oz)
    columns = [jnp.concatenate([ones[s + z] for s in starts], axis=0) for z in range(2)]
    local_one = dot(coupling[1], jnp.concatenate(columns, axis=1))
    from_two = dot(down_one[...], two)
    ups = []
    for z in range(2):
        total = local_one[:, 128 * z : 128 * (z + 1)]
        for j in range(2):
            for i in range(2):
                child = 4 * i + 2 * j + z
                part = from_two[child * rank : (child + 1) * rank]
                total = total + jnp.where(blocks == 2 * j + i, part, 0.0)
        total = total.astype(BF16)
        half = roll(total, 2 * width)
        none = jnp.zeros_like(total)
        for up in (
            jnp.where(masks.first, total, jnp.where(masks.last, half, roll(total, width))),
            jnp.where(masks.first, half, jnp.where(masks.last, total, roll(total, -width))),
        ):
            ups.append(jnp.concatenate([jnp.where(masks.odd, none, up), jnp.where(masks.odd, up, none)], axis=0))
    ups = jnp.concatenate(ups, axis=1)
    local = {}
    for j in range(2):
        for l in range(2):
            part = dot(down_zero[2 * j + l], ups)
            for z in range(2):
                for y in range(2):
                    at = 128 * (2 * z + y)
                    local[2 * z + l, 2 * y + j] = part[:, at : at + 128]

    for yk in range(2):
        for zk in range(2):
            windows = []
            for ox in range(3):
                at = (zk * (bx + 2) + ox) * rhs
                windows.append(y3[yk][at : at + bx * rhs])
            corners[yk, zk] = dot(jnp.concatenate(windows, axis=1), corner_weights[yk, zk], ((1,), (1,)))

    starts = []
    for e in range(entries):
        ox, oy, oz = (far_table[d, 0, e] + 2 for d in range(3))
        starts.append((ox * (bz + 4) + oz) * (by + 4) + oy)
    totals = []
    for z in range(bz):
        for y in range(0, by, 2):
            columns = [
                jnp.concatenate([shifts[s + z * (by + 4) + y + k] for s in starts], axis=0) for k in range(2)
            ]
            total = dot(coupling[0], jnp.concatenate(columns, axis=1))
            totals.append((total + jnp.concatenate([local[z, y], local[z, y + 1]], axis=1)).astype(BF16))
    copies = []
    for z in range(bz):
        for half in range(by // 2):
            y = 2 * half
            number = z * (by // 2) + half
            result = dot(totals[number], basis[...], ((0,), (0,)))
            result = result + near[z, half * 2 * bx * rhs : (half + 1) * 2 * bx * rhs]
            for k in range(2):
                block = result[k * bx * rhs : (k + 1) * bx * rhs]
                if y + k in (0, by - 1) and z in (0, bz - 1):
                    block = block + corners[0 if y + k == 0 else 1, 0 if z == 0 else 1]
                for x in range(bx):
                    planes[z, x, y + k] = block[x * rhs : (x + 1) * rhs] * live[x, y + k, z : z + 1]
        copies.append(pltpu.make_async_copy(planes.at[z], out.at[:, :, z], sems.at[z]))
        copies[-1].start()
    for c in copies:
        c.wait()


def body(charges, counts, near_offsets, near_blocks, leaf_basis, transfer, far_offsets, coupling, coarse_coupling):
    bx, by, bz, rhs, pts = charges.shape
    rank = leaf_basis.shape[0]
    entries = far_offsets.shape[1]
    stencil = near_blocks.shape[0]
    nx, ny, nz = (lax.axis_size(a) for a in ("gx", "gy", "gz"))
    assert (bx, by, bz) == (4, 4, 4) and bx * rhs == 128 and pts == 128
    xs = 2 if nx == 2 else 3
    geo = dict(nx=nx, ny=ny, nz=nz, xs=xs, bx=bx, by=by, bz=bz, rhs=rhs, rank=rank)
    geo["extra_x"] = max(nx - 3, 0)
    geo["extra_z"] = max(nz - 3, 0)
    geo["extra_y"] = max(ny - 3, 0)
    per = 128 // rhs
    tiles_z = -(-nz // per)
    tiles_x = -(-nx * nz // per)

    def shape(*dims, dtype=BF16):
        return jax.ShapeDtypeStruct(dims, dtype)

    def part(kernel):
        return functools.partial(kernel, geo)

    live = (jnp.arange(pts, dtype=jnp.int32) < counts[..., None]).astype(F32)
    near_table = near_offsets.T
    far_table = far_offsets.transpose(2, 0, 1)

    token = run(start_kernel, shape(8, 128, dtype=jnp.int32), (), flops=10**10)
    side = shape(2 * by + 3, rank, 128)
    message = shape(bz * bx * rhs + (bz * 2 + 2) * rank, 128)
    own, faces, mom, z_high, z_low, y_high, y_low, two = run(
        first_kernel,
        (
            shape(bz, by, bx, rhs, pts),
            shape(2, bz, by, rhs, pts),
            shape(bz * by + 2, rank, 128),
            side,
            side,
            message,
            message,
            shape(1, rank, 128),
        ),
        (token, live, charges, leaf_basis, transfer),
    )
    mz_prev = from_shift(z_high, "gz", nz, -1)
    mz_next = from_shift(z_low, "gz", nz, 1)
    if nx == 2:
        faces = [from_shift(faces, "gx", nx, 1)]
    else:
        faces = [from_shift(faces[1:], "gx", nx, -1), from_shift(faces[:1], "gx", nx, 1)]
    extra = [from_shift(two, "gz", nz, s) for s in range(2, nz - 1)]
    y1 = [from_shift(y_high, "gy", ny, -1), from_shift(y_low, "gy", ny, 1)]

    weights = run(
        weight_kernel,
        (
            shape(2, rank, entries * rank),
            shape(rank, nx * ny * nz * rank),
            shape(8 * rank, rank),
            shape(4, rank, 2 * rank),
        ),
        (coupling, coarse_coupling, transfer),
    )

    charge = shape(by, bx + 2, rhs, pts)
    message = shape(2 * bz * rhs + 12 * rank, 128)
    c_high, c_low, wide, y_high, y_low = run(
        part(second_kernel),
        (charge, charge, shape((bz + 4) * by + tiles_z, rank, 128), message, message),
        (own, *faces, mom, mz_prev, mz_next, two, *extra),
    )
    if nx == 2:
        sources = [wide, from_shift(wide, "gx", nx, 1)]
    else:
        sources = [wide, from_shift(wide, "gx", nx, -1), from_shift(wide, "gx", nx, 1)]
    cz_prev = from_shift(c_high, "gz", nz, -1)
    cz_next = from_shift(c_low, "gz", nz, 1)
    y2 = [from_shift(y_high, "gy", ny, -1), from_shift(y_low, "gy", ny, 1)]
    extra = [from_shift(wide[-tiles_z:], "gx", nx, s) for s in range(2, nx - 1)]

    field = shape(bz, by * bx * rhs, pts, dtype=F32)
    near = run(
        part(inner_kernel),
        field,
        (near_table, near_blocks, own, *faces, *y1),
        smem=(0,),
        scratch=[
            pltpu.VMEM((bz, by + 2, (bx + 2) * rhs, pts), BF16),
            pltpu.SMEM((stencil,), jnp.int32),
        ],
        limit=16,
        flops=2 * bx * by * bz * rhs * pts * pts * stencil,
    )

    message = shape(2 * (bx + 2) * rhs + ((xs - 1) * 2 * (bz + 4) + tiles_x) * rank, 128)
    y_high, y_low, one, two = run(
        part(third_kernel),
        (message, message, shape(18, rank, 128), shape(tiles_x, rank, 128)),
        (cz_prev, cz_next, *sources, mom, mz_prev, mz_next, *y1, *y2, *extra),
    )
    if nx == 2:
        beside = [from_shift(one, "gx", nx, 1)]
    else:
        beside = [from_shift(one, "gx", nx, -1), from_shift(one, "gx", nx, 1)]
    y3 = [from_shift(y_high, "gy", ny, -1), from_shift(y_low, "gy", ny, 1)]
    extra = [from_shift(two, "gy", ny, s) for s in range(2, ny - 1)]

    windows = shape(5 * (bz + 4) * (by + 4), rank, 128)
    columns = shape(5 * 5 * 6, rank, 128)
    near, shifts, ones, corner_weights = run(
        part(near_kernel),
        (field, windows, columns, shape(2, 2, pts, 3 * pts)),
        (near_table, near_blocks, near, cz_prev, cz_next, *y2, *sources, one),
        smem=(0,),
        aliases={2: 0},
        scratch=[
            pltpu.VMEM((2, by + 2, (bx + 2) * rhs, pts), BF16),
            pltpu.SMEM((stencil,), jnp.int32),
        ],
        limit=16,
        flops=2 * bx * by * bz * rhs * pts * pts * 9,
    )
    args = (
        far_table,
        live,
        near,
        corner_weights,
        leaf_basis,
        *weights,
        shifts,
        ones,
        *beside,
        *y1,
        *y2,
        *y3,
        two,
        *extra,
    )
    potentials, _, _ = run(
        part(final_kernel),
        (shape(bx, by, bz, rhs, pts, dtype=F32), windows, columns),
        args,
        anywhere=(0,),
        hbm_out=(0,),
        aliases={9: 1, 10: 2},
        limit=24,
        scratch=[
            pltpu.VMEM((2, 2, bx * rhs, pts), F32),
            pltpu.VMEM((bz, bx, by, rhs, pts), F32),
            pltpu.SMEM(far_table.shape, jnp.int32),
            pltpu.SemaphoreType.DMA((bz + 1,)),
        ],
    )
    return potentials


def solution(mesh):
    in_specs = (
        P("gx", "gy", "gz", None, None),
        P("gx", "gy", "gz"),
        P(),
        P(),
        P(),
        P(),
        P(),
        P(),
        P(),
    )
    out_specs = P("gx", "gy", "gz", None, None)

    return jax.shard_map(body, mesh=mesh, in_specs=in_specs, out_specs=out_specs, check_vma=False)
```

```python
import functools

import jax
import jax.numpy as jnp
from jax import lax
from jax.experimental import pallas as pl
from jax.experimental.pallas import tpu as pltpu
from jax.sharding import PartitionSpec as P


F32 = jnp.float32
BF16 = jnp.bfloat16


def from_shift(value, axis, size, shift):
    return lax.ppermute(value, axis, [(i, (i - shift) % size) for i in range(size)])


def spec_vmem():
    return pl.BlockSpec(memory_space=pltpu.VMEM)


def spec_smem():
    return pl.BlockSpec(memory_space=pltpu.SMEM)


def run(kernel, out_shape, args, smem=(), anywhere=(), scratch=(), flops=None, limit=8, hbm_out=(), aliases=None):
    def spec(i):
        if i in anywhere:
            return pl.BlockSpec(memory_space=pl.ANY)
        return spec_smem() if i in smem else spec_vmem()

    cost = None
    if flops is not None:
        cost = pl.CostEstimate(flops=flops, transcendentals=0, bytes_accessed=0)
    count = len(out_shape) if isinstance(out_shape, tuple) else 1
    outs = tuple(pl.BlockSpec(memory_space=pltpu.HBM) if i in hbm_out else spec_vmem() for i in range(count))
    return pl.pallas_call(
        kernel,
        out_shape=out_shape,
        in_specs=[spec(i) for i in range(len(args))],
        out_specs=outs if isinstance(out_shape, tuple) else outs[0],
        input_output_aliases=aliases or {},
        scratch_shapes=scratch,
        compiler_params=pltpu.CompilerParams(vmem_limit_bytes=limit * 1024 * 1024),
        cost_estimate=cost,
    )(*args)


def lane_blocks(rows, width):
    return lax.broadcasted_iota(jnp.int32, (rows, 128), 1) // width


class Masks:
    def __init__(self, rank, width):
        lanes = lax.broadcasted_iota(jnp.int16, (rank, 128), 1)
        bound = [jnp.int16(width * k) for k in range(4)]
        self.first = lanes < bound[1]
        self.lower = lanes < bound[2]
        self.last = lanes >= bound[3]
        self.odd = ((lanes >= bound[1]) & self.lower) | self.last


def roll(value, shift):
    shift = shift % 128
    return value if shift == 0 else pltpu.roll(value, shift, 1)


def dot(a, b, dims=((1,), (0,))):
    return lax.dot_general(a, b, (dims, ((), ())), preferred_element_type=F32)


def assemble(sources, width, load):
    per = 128 // width
    out = []
    for start in range(0, len(sources), per):
        total = None
        for d, (key, b) in enumerate(sources[start : start + per]):
            moved = roll(load(key).astype(F32), width * (d - b))
            if total is None:
                total = moved
                blocks = lane_blocks(moved.shape[0], width)
            else:
                total = jnp.where(blocks == d, moved, total)
        out.append(total.astype(BF16))
    return out


def tile_at(ref, start, rank):
    return ref[start : start + rank, :]


def start_kernel(out):
    out[...] = jnp.zeros(out.shape, out.dtype)


def first_kernel(token, live, charges, basis, transfer, own, faces, mom, z_high, z_low, y_high, y_low, two):
    bx, by, bz, rhs, pts = charges.shape
    rank = basis.shape[0]
    width = rhs
    for x in range(bx):
        for y in range(by):
            for z in range(bz):
                value = (charges[x, y, z].astype(F32) * live[x, y, z : z + 1]).astype(BF16)
                own[z, y, x] = value
                if x == 0:
                    faces[0, z, y] = value
                if x == bx - 1:
                    faces[1, z, y] = value
                at = (z * bx + x) * rhs
                if y == 0:
                    y_low[at : at + rhs] = value
                if y == by - 1:
                    y_high[at : at + rhs] = value
    base = bz * bx * rhs
    leaf = {}
    for z in range(bz):
        for y in range(0, by, 2):
            rows = own[z, y : y + 2].reshape(2 * bx * rhs, pts)
            value = dot(basis[...], rows, ((1,), (1,))).astype(BF16)
            for k in range(2):
                tile = value[:, 128 * k : 128 * (k + 1)]
                leaf[z, y + k] = tile
                mom[z * by + y + k] = tile
                (z_low if z < 2 else z_high)[z % 2 * by + y + k] = tile
                at = base + (z * 2 + k) * rank
                (y_low if y == 0 else y_high)[at : at + rank] = tile
    sums = [None, None]
    for i in range(2):
        for j in range(2):
            for l in range(2):
                cols = jnp.concatenate([leaf[2 * z + l, 2 * y + j] for z in range(2) for y in range(2)], axis=1)
                part = dot(transfer[4 * i + 2 * j + l], cols)
                sums[i] = part if sums[i] is None else sums[i] + part
    blocks = lane_blocks(rank, width)
    first = bz * by
    one = []
    for z in range(2):
        whole = []
        for y in range(2):
            at = 128 * (z * 2 + y)
            whole.append(sums[0][:, at : at + 128] + roll(sums[1][:, at : at + 128], -width))
        packed = jnp.where(
            blocks == 0,
            whole[0],
            jnp.where(
                blocks == 1,
                roll(whole[0], -width),
                jnp.where(blocks == 2, roll(whole[1], 2 * width), roll(whole[1], width)),
            ),
        ).astype(BF16)
        one.append(packed)
        mom[first + z] = packed
        z_high[2 * by + z] = packed
        z_low[2 * by + z] = packed
        at = base + (2 * bz + z) * rank
        y_high[at : at + rank] = packed
        y_low[at : at + rank] = packed
    total = None
    for j in range(2):
        for i in range(2):
            part = dot(transfer[4 * i + 2 * j], one[0]) + dot(transfer[4 * i + 2 * j + 1], one[1])
            part = roll(part, -width * (2 * j + i))
            total = part if total is None else total + part
    total = total.astype(BF16)
    z_high[2 * by + 2] = total
    z_low[2 * by + 2] = total
    two[0] = total


class Reader:
    def __init__(self, refs):
        self.refs = iter(refs)

    def take(self, count):
        return [next(self.refs) for _ in range(count)]

    def faces(self, geo):
        if geo["nx"] == 2:
            (both,) = self.take(1)
            return both.at[1], both.at[0]
        before, after = self.take(2)
        return before.at[0], after.at[0]


def second_kernel(geo, *refs):
    nz, bx, by, bz, rhs, rank = (geo[k] for k in ("nz", "bx", "by", "bz", "rhs", "rank"))
    read = Reader(refs)
    (own,) = read.take(1)
    before, after = read.faces(geo)
    mom, prev, nxt, mine = read.take(4)
    far = read.take(geo["extra_z"])
    c_high, c_low, wide, y_high, y_low, line = read.take(6)
    for z in range(bz + 4):
        for y in range(by):
            if z < 2:
                tile = prev[z * by + y]
            elif z >= bz + 2:
                tile = nxt[(z - bz - 2) * by + y]
            else:
                tile = mom[(z - 2) * by + y]
            wide[z * by + y] = tile

    def load(key):
        if key == 0:
            return mine[0]
        if key == 1:
            return nxt[2 * by + 2]
        if key == nz - 1:
            return prev[2 * by + 2]
        return far[key - 2][0]

    for t, tile in enumerate(assemble([(k, 0) for k in range(nz)], rhs, load)):
        line[t] = tile
        at = 2 * bz * rhs + (12 + t) * rank
        y_high[at : at + rank] = tile
        y_low[at : at + rank] = tile
    for out, z in ((c_high, bz - 1), (c_low, 0)):
        for y in range(by):
            out[y, 0] = before[z, y]
            out[y, 1 : bx + 1] = own[z, y]
            out[y, bx + 1] = after[z, y]
    base = 2 * bz * rhs
    for out, y in ((y_high, by - 1), (y_low, 0)):
        for k, s in enumerate((before, after)):
            for z in range(bz):
                at = (k * bz + z) * rhs
                out[at : at + rhs] = s[z, y]
        start = by - 2 if y else 0
        for zh in range(4):
            s = prev if zh < 2 else nxt
            for yy in range(2):
                at = base + (zh * 2 + yy) * rank
                out[at : at + rank] = s[zh % 2 * by + start + yy]
        for side, s in enumerate((prev, nxt)):
            for z in range(2):
                at = base + (8 + side * 2 + z) * rank
                out[at : at + rank] = s[2 * by + z]


def third_kernel(geo, *refs):
    xs, bx, by, bz, rhs, rank = (geo[k] for k in ("xs", "bx", "by", "bz", "rhs", "rank"))
    read = Reader(refs)
    prev, nxt = read.take(2)
    sources = [None] + read.take(xs - 1)
    y_high, y_low = read.take(2)
    base = 2 * (bx + 2) * rhs
    for out, y in ((y_high, by - 1), (y_low, 0)):
        for k, s in enumerate((prev, nxt)):
            at = k * (bx + 2) * rhs
            out[at : at + (bx + 2) * rhs] = s[y].reshape((bx + 2) * rhs, s.shape[3])
        start = by - 2 if y else 0
        for k in range(1, xs):
            for z in range(bz + 4):
                for yy in range(2):
                    at = base + (((k - 1) * (bz + 4) + z) * 2 + yy) * rank
                    out[at : at + rank] = sources[k][z * by + start + yy]


def column_kernel(geo, *refs):
    ny, bx, by, bz, rhs, rank = (geo[k] for k in ("ny", "bx", "by", "bz", "rhs", "rank"))
    read = Reader(refs)
    mom, mz_prev, mz_next = read.take(3)
    y1, y2 = read.take(2), read.take(2)
    (line,) = read.take(1)
    far = read.take(geo["extra_y"])
    (one,) = read.take(1)
    base1 = bz * bx * rhs
    base2 = 2 * bz * rhs
    for yb in range(3):
        for zb in range(3):
            for z in range(2):
                if yb == 1:
                    tile = mom[bz * by + z] if zb == 1 else (mz_prev if zb == 0 else mz_next)[2 * by + z]
                elif zb == 1:
                    tile = tile_at(y1[yb // 2], base1 + (2 * bz + z) * rank, rank)
                else:
                    tile = tile_at(y2[yb // 2], base2 + (8 + (zb // 2) * 2 + z) * rank, rank)
                one[(yb * 3 + zb) * 2 + z] = tile
    tiles = line.shape[0]
    for s in range(ny):
        for t in range(tiles):
            if s == 0:
                tile = line[t]
            elif s == 1 or s == ny - 1:
                tile = tile_at(y2[1 if s == 1 else 0], base2 + (12 + t) * rank, rank)
            else:
                tile = far[s - 2][t]
            one[18 + s * tiles + t] = tile


def near_weights(inverse, near_blocks, codes):
    return jnp.concatenate([near_blocks[inverse[c]] for c in codes], axis=1)


def find_inverse(table, inverse, count):
    for s in range(count):
        ox, oy, oz = (table[d, s] + 1 for d in range(3))
        inverse[(ox * 3 + oy) * 3 + oz] = s


def store_windows(shifts, at, stride, masks, width, mid, before, after):
    shifts[at] = roll(jnp.where(masks.lower, mid, before), 2 * width)
    shifts[stride + at] = roll(jnp.where(masks.last, before, mid), width)
    shifts[2 * stride + at] = mid
    shifts[3 * stride + at] = roll(jnp.where(masks.first, after, mid), -width)
    shifts[4 * stride + at] = roll(jnp.where(masks.lower, after, mid), 2 * width)


def windows_y(masks, width, tiles):
    low, mid, high = tiles
    return [
        low,
        roll(jnp.where(masks.lower, mid, low), 2 * width),
        mid,
        roll(jnp.where(masks.lower, high, mid), 2 * width),
        high,
    ]


def near_product(geo, weights, window, out, first, planes):
    bx, by, rhs = (geo[k] for k in ("bx", "by", "rhs"))
    rows, blocks = [], ([], [])
    for plane in planes:
        for ox in range(3):
            for oy in range(3):
                rows.append(window(first + plane, oy, ox))
                for k in range(2):
                    blocks[k].append(weights(ox, oy, plane + 1 - k))
    right = jnp.concatenate([jnp.concatenate(b, axis=1) for b in blocks], axis=0)
    value = dot(jnp.concatenate(rows, axis=1), right, ((1,), (1,)))
    for k in range(2):
        out[first + k] = value[:, 128 * k : 128 * (k + 1)]


def inner_kernel(geo, *refs):
    bx, by, bz, rhs = (geo[k] for k in ("bx", "by", "bz", "rhs"))
    read = Reader(refs)
    table, near_blocks, own = read.take(3)
    before, after = read.faces(geo)
    y1 = read.take(2)
    out, wide, inverse = read.take(3)
    pts = wide.shape[3]
    find_inverse(table, inverse, near_blocks.shape[0])
    rows = (bx + 2) * rhs
    none = jnp.zeros((rhs, pts), BF16)
    for z in range(bz):
        for k, y in enumerate((0, by + 1)):
            wide[z, y, 0:rhs] = none
            wide[z, y, rhs : rows - rhs] = y1[k][z * bx * rhs : (z + 1) * bx * rhs]
            wide[z, y, rows - rhs :] = none
        for y in range(1, by + 1):
            wide[z, y, 0:rhs] = before[z, y - 1]
            wide[z, y, rhs : rows - rhs] = own[z, y - 1].reshape(bx * rhs, pts)
            wide[z, y, rows - rhs :] = after[z, y - 1]
    empty = jnp.zeros((pts, pts), BF16)

    def weights(ox, oy, oz):
        return near_blocks[inverse[(ox * 3 + oy) * 3 + oz]] if 0 <= oz < 3 else empty

    def window(z, oy, ox):
        return wide[z, oy : oy + by, ox * rhs : (ox + bx) * rhs, :].reshape(by * bx * rhs, pts)

    for first in range(0, bz, 2):
        planes = [p for p in range(-1, 3) if 0 <= first + p < bz]
        near_product(geo, weights, window, out, first, planes)


def near_kernel(geo, *refs):
    xs, bx, by, bz, rhs, rank = (geo[k] for k in ("xs", "bx", "by", "bz", "rhs", "rank"))
    read = Reader(refs)
    table, near_blocks = read.take(2)
    read.take(1)
    cz_prev, cz_next = read.take(2)
    y2 = read.take(2)
    sources = read.take(xs)
    (one,) = read.take(1)
    out, shifts, ones, corner_weights, wide, inverse = read.take(6)
    pts = wide.shape[3]
    find_inverse(table, inverse, near_blocks.shape[0])
    rows = (bx + 2) * rhs
    for k, s in enumerate((cz_prev, cz_next)):
        for y in (0, by + 1):
            wide[k, y] = jnp.zeros((rows, pts), BF16)
        for y in range(by):
            wide[k, y + 1] = s[y].reshape(rows, pts)
    for k, z in enumerate((0, bz - 1)):
        codes = [(ox * 3 + oy) * 3 + 2 * k for ox in range(3) for oy in range(3)]
        left = [
            wide[k, oy : oy + by, ox * rhs : (ox + bx) * rhs, :].reshape(by * bx * rhs, pts)
            for ox in range(3)
            for oy in range(3)
        ]
        right = near_weights(inverse, near_blocks, codes)
        out[z] = out[z] + dot(jnp.concatenate(left, axis=1), right, ((1,), (1,)))
    none = jnp.zeros((rhs, pts), BF16)
    for yk, y in enumerate((0, by - 1)):
        for xk, x in enumerate((0, bx - 1)):
            at = xk * bz * rhs
            column = y2[yk][at : at + bz * rhs]
            column = jnp.concatenate([none, column, none], axis=0)
            left = jnp.concatenate([column[oz * rhs : (oz + bz) * rhs] for oz in range(3)], axis=1)
            right = near_weights(inverse, near_blocks, [(6 * xk + 2 * yk) * 3 + oz for oz in range(3)])
            value = dot(left, right, ((1,), (1,)))
            at = (y * bx + x) * rhs
            for z in range(bz):
                out[z, at : at + rhs] = out[z, at : at + rhs] + value[z * rhs : (z + 1) * rhs]
    masks = Masks(rank, rhs)
    for z in range(bz + 4):
        for y in range(by):
            tiles = [s[z * by + y] for s in sources]
            at = z * (by + 4) + y + 2
            store_windows(shifts, at, (bz + 4) * (by + 4), masks, rhs, tiles[0], tiles[1], tiles[-1])
    for z in range(6):
        for m, mid in enumerate(windows_y(masks, rhs, [one[yb * 6 + z] for yb in range(3)])):
            ones[(10 + m) * 6 + z] = mid
            ones[(5 + m) * 6 + z] = roll(mid, rhs)
            ones[(15 + m) * 6 + z] = roll(mid, -rhs)
    for yk in range(2):
        for zk in range(2):
            codes = [(ox * 3 + 2 * yk) * 3 + 2 * zk for ox in range(3)]
            corner_weights[yk, zk] = near_weights(inverse, near_blocks, codes)


def weight_kernel(coupling_in, coarse_in, transfer, coupling, coarse, down_one, down_zero):
    entries, rank = coupling_in.shape[1:3]
    for level in range(2):
        coupling[level] = jnp.concatenate([coupling_in[level, e] for e in range(entries)], axis=1)
    nx, ny, nz = coarse_in.shape[:3]
    coarse[...] = jnp.concatenate(
        [coarse_in[x, y, z] for x in range(nx) for y in range(ny) for z in range(nz)], axis=1
    )
    turned = [transfer[c].astype(F32).T.astype(BF16) for c in range(8)]
    for c in range(8):
        down_one[c * rank : (c + 1) * rank] = turned[c]
    for k in range(4):
        down_zero[k] = jnp.concatenate([turned[k], turned[4 + k]], axis=1)


def final_kernel(geo, *refs):
    nx, ny, nz, xs, bx, by, bz, rhs, rank = (
        geo[k] for k in ("nx", "ny", "nz", "xs", "bx", "by", "bz", "rhs", "rank")
    )
    width = rhs
    read = Reader(refs)
    far_in, live, near, corner_weights, basis, coupling, coarse, down_one, down_zero = read.take(9)
    read.take(2)
    beside = read.take(xs - 1)
    y1, y2, y3 = read.take(2), read.take(2), read.take(2)
    (one,) = read.take(1)
    far_two = read.take(geo["extra_x"])
    out, shifts, ones = read.take(3)
    corners, planes, far_table, sems = read.take(4)
    table_copy = pltpu.make_async_copy(far_in, far_table, sems.at[bz])
    table_copy.start()
    blocks = lane_blocks(rank, width)
    masks = Masks(rank, width)
    entries = coupling.shape[2] // rank
    base1 = bz * bx * rhs
    base2 = 2 * bz * rhs
    base3 = 2 * (bx + 2) * rhs

    def leaf_tile(k, z, side, yy):
        if k > 0:
            return tile_at(y3[side], base3 + (((k - 1) * (bz + 4) + z + 2) * 2 + yy) * rank, rank)
        if 0 <= z < bz:
            return tile_at(y1[side], base1 + (z * 2 + yy) * rank, rank)
        zh = z + 2 if z < 0 else z - bz + 2
        return tile_at(y2[side], base2 + (zh * 2 + yy) * rank, rank)

    for z in range(-2, bz + 2):
        for side in range(2):
            for yy in range(2):
                tiles = [leaf_tile(k, z, side, yy) for k in range(xs)]
                at = (z + 2) * (by + 4) + yy + side * (by + 2)
                store_windows(shifts, at, (bz + 4) * (by + 4), masks, width, tiles[0], tiles[1], tiles[-1])

    for z in range(6):
        sides = [windows_y(masks, width, [s[yb * 6 + z] for yb in range(3)]) for s in beside]
        for m in range(5):
            before, after = sides[0][m], sides[-1][m]
            ones[m * 6 + z] = before
            ones[(20 + m) * 6 + z] = after
            at = (5 + m) * 6 + z
            ones[at] = jnp.where(masks.odd, ones[at], roll(before, -width))
            at = (15 + m) * 6 + z
            ones[at] = jnp.where(masks.odd, roll(after, width), ones[at])

    per = 128 // width
    tiles = -(-nz // per)

    def two_tile(s, t):
        if s == 0:
            return one[18 + t]
        if s == 1:
            return beside[-1][18 + t]
        if s == nx - 1:
            return beside[0][18 + t]
        return far_two[s - 2][t]

    lanes = lax.broadcasted_iota(jnp.int16, (rank, 128), 1)
    quarter = [(lanes >= jnp.int16(width * b)) & (lanes < jnp.int16(width * (b + 1))) for b in range(per)]
    stacked = []
    for s in range(nx):
        for y in range(ny):
            for b in range(nz):
                tile = two_tile(s, y * tiles + b // per)
                stacked.append(jnp.where(quarter[b % per], tile, jnp.zeros_like(tile)))
    two = dot(coarse[...], jnp.concatenate(stacked, axis=0))
    two = two + roll(two, 2 * width)
    two = (two + roll(two, width)).astype(BF16)

    table_copy.wait()
    starts = []
    for e in range(entries):
        ox, oy, oz = (far_table[d, 1, e] + 2 for d in range(3))
        starts.append((ox * 5 + oy) * 6 + oz)
    columns = [jnp.concatenate([ones[s + z] for s in starts], axis=0) for z in range(2)]
    local_one = dot(coupling[1], jnp.concatenate(columns, axis=1))
    from_two = dot(down_one[...], two)
    ups = []
    for z in range(2):
        total = local_one[:, 128 * z : 128 * (z + 1)]
        for j in range(2):
            for i in range(2):
                child = 4 * i + 2 * j + z
                part = from_two[child * rank : (child + 1) * rank]
                total = total + jnp.where(blocks == 2 * j + i, part, 0.0)
        total = total.astype(BF16)
        half = roll(total, 2 * width)
        none = jnp.zeros_like(total)
        for up in (
            jnp.where(masks.first, total, jnp.where(masks.last, half, roll(total, width))),
            jnp.where(masks.first, half, jnp.where(masks.last, total, roll(total, -width))),
        ):
            ups.append(jnp.concatenate([jnp.where(masks.odd, none, up), jnp.where(masks.odd, up, none)], axis=0))
    ups = jnp.concatenate(ups, axis=1)
    local = {}
    for j in range(2):
        for l in range(2):
            part = dot(down_zero[2 * j + l], ups)
            for z in range(2):
                for y in range(2):
                    at = 128 * (2 * z + y)
                    local[2 * z + l, 2 * y + j] = part[:, at : at + 128]

    for yk in range(2):
        for zk in range(2):
            windows = []
            for ox in range(3):
                at = (zk * (bx + 2) + ox) * rhs
                windows.append(y3[yk][at : at + bx * rhs])
            corners[yk, zk] = dot(jnp.concatenate(windows, axis=1), corner_weights[yk, zk], ((1,), (1,)))

    starts = []
    for e in range(entries):
        ox, oy, oz = (far_table[d, 0, e] + 2 for d in range(3))
        starts.append((ox * (bz + 4) + oz) * (by + 4) + oy)
    totals = []
    for z in range(bz):
        for y in range(0, by, 2):
            columns = [
                jnp.concatenate([shifts[s + z * (by + 4) + y + k] for s in starts], axis=0) for k in range(2)
            ]
            total = dot(coupling[0], jnp.concatenate(columns, axis=1))
            totals.append((total + jnp.concatenate([local[z, y], local[z, y + 1]], axis=1)).astype(BF16))
    copies = []
    for z in range(bz):
        for half in range(by // 2):
            y = 2 * half
            number = z * (by // 2) + half
            result = dot(totals[number], basis[...], ((0,), (0,)))
            result = result + near[z, half * 2 * bx * rhs : (half + 1) * 2 * bx * rhs]
            for k in range(2):
                block = result[k * bx * rhs : (k + 1) * bx * rhs]
                if y + k in (0, by - 1) and z in (0, bz - 1):
                    block = block + corners[0 if y + k == 0 else 1, 0 if z == 0 else 1]
                for x in range(bx):
                    planes[z, x, y + k] = block[x * rhs : (x + 1) * rhs] * live[x, y + k, z : z + 1]
        copies.append(pltpu.make_async_copy(planes.at[z], out.at[:, :, z], sems.at[z]))
        copies[-1].start()
    for c in copies:
        c.wait()


def body(charges, counts, near_offsets, near_blocks, leaf_basis, transfer, far_offsets, coupling, coarse_coupling):
    bx, by, bz, rhs, pts = charges.shape
    rank = leaf_basis.shape[0]
    entries = far_offsets.shape[1]
    stencil = near_blocks.shape[0]
    nx, ny, nz = (lax.axis_size(a) for a in ("gx", "gy", "gz"))
    assert (bx, by, bz) == (4, 4, 4) and bx * rhs == 128 and pts == 128
    xs = 2 if nx == 2 else 3
    geo = dict(nx=nx, ny=ny, nz=nz, xs=xs, bx=bx, by=by, bz=bz, rhs=rhs, rank=rank)
    geo["extra_x"] = max(nx - 3, 0)
    geo["extra_z"] = max(nz - 3, 0)
    geo["extra_y"] = max(ny - 3, 0)
    per = 128 // rhs
    tiles_z = -(-nz // per)

    def shape(*dims, dtype=BF16):
        return jax.ShapeDtypeStruct(dims, dtype)

    def part(kernel):
        return functools.partial(kernel, geo)

    live = (jnp.arange(pts, dtype=jnp.int32) < counts[..., None]).astype(F32)
    near_table = near_offsets.T
    far_table = far_offsets.transpose(2, 0, 1)

    token = run(start_kernel, shape(8, 128, dtype=jnp.int32), (), flops=10**10)
    side = shape(2 * by + 3, rank, 128)
    message = shape(bz * bx * rhs + (bz * 2 + 2) * rank, 128)
    own, faces, mom, z_high, z_low, y_high, y_low, two = run(
        first_kernel,
        (
            shape(bz, by, bx, rhs, pts),
            shape(2, bz, by, rhs, pts),
            shape(bz * by + 2, rank, 128),
            side,
            side,
            message,
            message,
            shape(1, rank, 128),
        ),
        (token, live, charges, leaf_basis, transfer),
    )
    mz_prev = from_shift(z_high, "gz", nz, -1)
    mz_next = from_shift(z_low, "gz", nz, 1)
    if nx == 2:
        faces = [from_shift(faces, "gx", nx, 1)]
    else:
        faces = [from_shift(faces[1:], "gx", nx, -1), from_shift(faces[:1], "gx", nx, 1)]
    extra = [from_shift(two, "gz", nz, s) for s in range(2, nz - 1)]
    y1 = [from_shift(y_high, "gy", ny, -1), from_shift(y_low, "gy", ny, 1)]

    weights = run(
        weight_kernel,
        (
            shape(2, rank, entries * rank),
            shape(rank, nx * ny * nz * rank),
            shape(8 * rank, rank),
            shape(4, rank, 2 * rank),
        ),
        (coupling, coarse_coupling, transfer),
    )

    charge = shape(by, bx + 2, rhs, pts)
    message = shape(2 * bz * rhs + (12 + tiles_z) * rank, 128)
    c_high, c_low, wide, y_high, y_low, line = run(
        part(second_kernel),
        (charge, charge, shape((bz + 4) * by, rank, 128), message, message, shape(tiles_z, rank, 128)),
        (own, *faces, mom, mz_prev, mz_next, two, *extra),
    )
    if nx == 2:
        sources = [wide, from_shift(wide, "gx", nx, 1)]
    else:
        sources = [wide, from_shift(wide, "gx", nx, -1), from_shift(wide, "gx", nx, 1)]
    cz_prev = from_shift(c_high, "gz", nz, -1)
    cz_next = from_shift(c_low, "gz", nz, 1)
    y2 = [from_shift(y_high, "gy", ny, -1), from_shift(y_low, "gy", ny, 1)]
    extra = [from_shift(line, "gy", ny, s) for s in range(2, ny - 1)]

    field = shape(bz, by * bx * rhs, pts, dtype=F32)
    near = run(
        part(inner_kernel),
        field,
        (near_table, near_blocks, own, *faces, *y1),
        smem=(0,),
        scratch=[
            pltpu.VMEM((bz, by + 2, (bx + 2) * rhs, pts), BF16),
            pltpu.SMEM((stencil,), jnp.int32),
        ],
        limit=16,
        flops=2 * bx * by * bz * rhs * pts * pts * stencil,
    )

    message = shape(2 * (bx + 2) * rhs + (xs - 1) * 2 * (bz + 4) * rank, 128)
    y_high, y_low = run(part(third_kernel), (message, message), (cz_prev, cz_next, *sources[1:]))
    one = run(part(column_kernel), shape(18 + ny * tiles_z, rank, 128), (mom, mz_prev, mz_next, *y1, *y2, line, *extra))
    if nx == 2:
        beside = [from_shift(one, "gx", nx, 1)]
    else:
        beside = [from_shift(one, "gx", nx, -1), from_shift(one, "gx", nx, 1)]
    y3 = [from_shift(y_high, "gy", ny, -1), from_shift(y_low, "gy", ny, 1)]
    extra = [from_shift(one[18:], "gx", nx, s) for s in range(2, nx - 1)]

    windows = shape(5 * (bz + 4) * (by + 4), rank, 128)
    columns = shape(5 * 5 * 6, rank, 128)
    near, shifts, ones, corner_weights = run(
        part(near_kernel),
        (field, windows, columns, shape(2, 2, pts, 3 * pts)),
        (near_table, near_blocks, near, cz_prev, cz_next, *y2, *sources, one),
        smem=(0,),
        aliases={2: 0},
        scratch=[
            pltpu.VMEM((2, by + 2, (bx + 2) * rhs, pts), BF16),
            pltpu.SMEM((stencil,), jnp.int32),
        ],
        limit=16,
        flops=2 * bx * by * bz * rhs * pts * pts * 9,
    )
    args = (
        far_table,
        live,
        near,
        corner_weights,
        leaf_basis,
        *weights,
        shifts,
        ones,
        *beside,
        *y1,
        *y2,
        *y3,
        one,
        *extra,
    )
    potentials, _, _ = run(
        part(final_kernel),
        (shape(bx, by, bz, rhs, pts, dtype=F32), windows, columns),
        args,
        anywhere=(0,),
        hbm_out=(0,),
        aliases={9: 1, 10: 2},
        limit=24,
        scratch=[
            pltpu.VMEM((2, 2, bx * rhs, pts), F32),
            pltpu.VMEM((bz, bx, by, rhs, pts), F32),
            pltpu.SMEM(far_table.shape, jnp.int32),
            pltpu.SemaphoreType.DMA((bz + 1,)),
        ],
    )
    return potentials


def solution(mesh):
    in_specs = (
        P("gx", "gy", "gz", None, None),
        P("gx", "gy", "gz"),
        P(),
        P(),
        P(),
        P(),
        P(),
        P(),
        P(),
    )
    out_specs = P("gx", "gy", "gz", None, None)

    return jax.shard_map(body, mesh=mesh, in_specs=in_specs, out_specs=out_specs, check_vma=False)
```

```python
import functools

import jax
import jax.numpy as jnp
from jax import lax
from jax.experimental import pallas as pl
from jax.experimental.pallas import tpu as pltpu
from jax.sharding import PartitionSpec as P


F32 = jnp.float32
BF16 = jnp.bfloat16


def from_shift(value, axis, size, shift):
    return lax.ppermute(value, axis, [(i, (i - shift) % size) for i in range(size)])


def spec_vmem():
    return pl.BlockSpec(memory_space=pltpu.VMEM)


def spec_smem():
    return pl.BlockSpec(memory_space=pltpu.SMEM)


def run(kernel, out_shape, args, smem=(), anywhere=(), scratch=(), flops=None, limit=8, hbm_out=(), aliases=None):
    def spec(i):
        if i in anywhere:
            return pl.BlockSpec(memory_space=pl.ANY)
        return spec_smem() if i in smem else spec_vmem()

    cost = None
    if flops is not None:
        cost = pl.CostEstimate(flops=flops, transcendentals=0, bytes_accessed=0)
    count = len(out_shape) if isinstance(out_shape, tuple) else 1
    outs = tuple(pl.BlockSpec(memory_space=pltpu.HBM) if i in hbm_out else spec_vmem() for i in range(count))
    return pl.pallas_call(
        kernel,
        out_shape=out_shape,
        in_specs=[spec(i) for i in range(len(args))],
        out_specs=outs if isinstance(out_shape, tuple) else outs[0],
        input_output_aliases=aliases or {},
        scratch_shapes=scratch,
        compiler_params=pltpu.CompilerParams(vmem_limit_bytes=limit * 1024 * 1024),
        cost_estimate=cost,
    )(*args)


def lane_blocks(rows, width):
    return lax.broadcasted_iota(jnp.int32, (rows, 128), 1) // width


class Masks:
    def __init__(self, rank, width):
        lanes = lax.broadcasted_iota(jnp.int16, (rank, 128), 1)
        bound = [jnp.int16(width * k) for k in range(4)]
        self.first = lanes < bound[1]
        self.lower = lanes < bound[2]
        self.last = lanes >= bound[3]
        self.odd = ((lanes >= bound[1]) & self.lower) | self.last


def roll(value, shift):
    shift = shift % 128
    return value if shift == 0 else pltpu.roll(value, shift, 1)


def dot(a, b, dims=((1,), (0,))):
    return lax.dot_general(a, b, (dims, ((), ())), preferred_element_type=F32)


def assemble(sources, width, load):
    per = 128 // width
    out = []
    for start in range(0, len(sources), per):
        total = None
        for d, (key, b) in enumerate(sources[start : start + per]):
            moved = roll(load(key).astype(F32), width * (d - b))
            if total is None:
                total = moved
                blocks = lane_blocks(moved.shape[0], width)
            else:
                total = jnp.where(blocks == d, moved, total)
        out.append(total.astype(BF16))
    return out


def tile_at(ref, start, rank):
    return ref[start : start + rank, :]


def start_kernel(out):
    out[...] = jnp.zeros(out.shape, out.dtype)


def lift(transfer, groups, width):
    sums = [None, None]
    for i in range(2):
        for j in range(2):
            for l in range(2):
                cols = jnp.concatenate([g[l][2 * y + j] for g in groups for y in range(2)], axis=1)
                part = dot(transfer[4 * i + 2 * j + l], cols)
                sums[i] = part if sums[i] is None else sums[i] + part
    blocks = lane_blocks(sums[0].shape[0], width)
    tiles = []
    for z in range(len(groups)):
        whole = []
        for y in range(2):
            at = 128 * (z * 2 + y)
            whole.append(sums[0][:, at : at + 128] + roll(sums[1][:, at : at + 128], -width))
        packed = jnp.where(
            blocks == 0,
            whole[0],
            jnp.where(
                blocks == 1,
                roll(whole[0], -width),
                jnp.where(blocks == 2, roll(whole[1], 2 * width), roll(whole[1], width)),
            ),
        )
        tiles.append(packed.astype(BF16))
    return tiles


def fold(tile, width):
    masks = Masks(16, width)
    rows = [tile[16 * k : 16 * (k + 1)] for k in range(3)]
    return jnp.where(masks.first, rows[0], jnp.where(masks.lower, roll(rows[1], width), roll(rows[2], 2 * width)))


def unfold(rows, width):
    return jnp.concatenate([rows, roll(rows, -width), roll(rows, -2 * width)], axis=0)


def first_kernel(token, live, charges, basis, transfer, own, faces, mom, z_high, z_low, y_high, y_low, two):
    bx, by, bz, rhs, pts = charges.shape
    rank = basis.shape[0]
    width = rhs
    for x in range(bx):
        for y in range(by):
            for z in range(bz):
                value = (charges[x, y, z].astype(F32) * live[x, y, z : z + 1]).astype(BF16)
                own[z, y, x] = value
                if x == 0:
                    faces[0, z, y] = value
                if x == bx - 1:
                    faces[1, z, y] = value
                at = (z * bx + x) * rhs
                if y == 0:
                    y_low[at : at + rhs] = value
                if y == by - 1:
                    y_high[at : at + rhs] = value
    base = bz * bx * rhs
    leaf = {}
    for z in range(bz):
        for y in range(0, by, 2):
            rows = own[z, y : y + 2].reshape(2 * bx * rhs, pts)
            value = dot(basis[...], rows, ((1,), (1,))).astype(BF16)
            for k in range(2):
                tile = value[:, 128 * k : 128 * (k + 1)]
                leaf[z, y + k] = tile
                mom[z * by + y + k] = tile
                at = (z % 2 * by + y + k) * rank
                (z_low if z < 2 else z_high)[at : at + rank] = tile
                at = base + (z * 2 + k) * rank
                (y_low if y == 0 else y_high)[at : at + rank] = tile
    one = lift(transfer, [[[leaf[2 * z + l, y] for y in range(by)] for l in range(2)] for z in range(2)], width)
    for z in range(2):
        mom[bz * by + z] = one[z]
        (z_low if z else z_high)[2 * by * rank : (2 * by + 1) * rank] = one[z]
        at = base + (2 * bz + z) * rank
        y_high[at : at + rank] = one[z]
        y_low[at : at + rank] = one[z]
    total = None
    for j in range(2):
        for i in range(2):
            part = dot(transfer[4 * i + 2 * j], one[0]) + dot(transfer[4 * i + 2 * j + 1], one[1])
            part = roll(part, -width * (2 * j + i))
            total = part if total is None else total + part
    total = fold(total.astype(BF16), width)
    z_high[(2 * by + 1) * rank :] = total
    z_low[(2 * by + 1) * rank :] = total
    two[...] = total


class Reader:
    def __init__(self, refs):
        self.refs = iter(refs)

    def take(self, count):
        return [next(self.refs) for _ in range(count)]

    def faces(self, geo):
        if geo["nx"] == 2:
            (both,) = self.take(1)
            return both.at[1], both.at[0]
        before, after = self.take(2)
        return before.at[0], after.at[0]


def second_kernel(geo, *refs):
    bx, by, bz, rank = (geo[k] for k in ("bx", "by", "bz", "rank"))
    read = Reader(refs)
    (own,) = read.take(1)
    before, after = read.faces(geo)
    mom, prev, nxt = read.take(3)
    c_high, c_low, wide = read.take(3)
    for z in range(bz + 4):
        for y in range(by):
            if z < 2:
                tile = tile_at(prev, (z * by + y) * rank, rank)
            elif z >= bz + 2:
                tile = tile_at(nxt, ((z - bz - 2) * by + y) * rank, rank)
            else:
                tile = mom[(z - 2) * by + y]
            wide[z * by + y] = tile
    for out, z in ((c_high, bz - 1), (c_low, 0)):
        for y in range(by):
            out[y, 0] = before[z, y]
            out[y, 1 : bx + 1] = own[z, y]
            out[y, bx + 1] = after[z, y]


def sides_kernel(geo, *refs):
    nz, _, by, bz, rhs, rank = (geo[k] for k in ("nz", "bx", "by", "bz", "rhs", "rank"))
    read = Reader(refs)
    before, after = read.faces(geo)
    transfer, prev, nxt, mine = read.take(4)
    far = read.take(geo["extra_z"])
    y_high, y_low, line, halo = read.take(4)

    def leaf(s, z, y):
        return tile_at(s, (z * by + y) * rank, rank)

    near = lift(transfer, [[[leaf(s, l, y) for y in range(by)] for l in range(2)] for s in (prev, nxt)], rhs)
    sent = [tile_at(s, 2 * by * rank, rank) for s in (prev, nxt)]
    level = [sent[0], near[0], near[1], sent[1]]
    base = 2 * bz * rhs
    for z in range(4):
        halo[z] = level[z]
        at = base + (8 + z) * rank
        y_high[at : at + rank] = level[z]
        y_low[at : at + rank] = level[z]
    for out, y in ((y_high, by - 1), (y_low, 0)):
        for k, s in enumerate((before, after)):
            for z in range(bz):
                at = (k * bz + z) * rhs
                out[at : at + rhs] = s[z, y]
        start = by - 2 if y else 0
        for zh in range(4):
            for yy in range(2):
                at = base + (zh * 2 + yy) * rank
                out[at : at + rank] = leaf(prev if zh < 2 else nxt, zh % 2, start + yy)

    def load(key):
        if key == 0:
            return unfold(mine[...], rhs)
        if key == 1:
            return unfold(nxt[(2 * by + 1) * rank :, :], rhs)
        if key == nz - 1:
            return unfold(prev[(2 * by + 1) * rank :, :], rhs)
        return unfold(far[key - 2][...], rhs)

    for t, tile in enumerate(assemble([(k, 0) for k in range(nz)], rhs, load)):
        line[t] = tile
        at = base + (12 + t) * rank
        y_high[at : at + rank] = tile
        y_low[at : at + rank] = tile


def third_kernel(geo, *refs):
    xs, bx, by, bz, rhs, rank = (geo[k] for k in ("xs", "bx", "by", "bz", "rhs", "rank"))
    read = Reader(refs)
    prev, nxt = read.take(2)
    sources = [None] + read.take(xs - 1)
    y_high, y_low = read.take(2)
    base = 2 * (bx + 2) * rhs
    for out, y in ((y_high, by - 1), (y_low, 0)):
        for k, s in enumerate((prev, nxt)):
            at = k * (bx + 2) * rhs
            out[at : at + (bx + 2) * rhs] = s[y].reshape((bx + 2) * rhs, s.shape[3])
        start = by - 2 if y else 0
        for k in range(1, xs):
            for z in range(bz + 4):
                for yy in range(2):
                    at = base + (((k - 1) * (bz + 4) + z) * 2 + yy) * rank
                    out[at : at + rank] = sources[k][z * by + start + yy]


def sent_index(yb, z):
    left_out = [(1, k) for k in range(1, 5)]
    order = [(b, k) for b in range(3) for k in range(6) if (b, k) not in left_out]
    return order.index((yb, z)) if (yb, z) in order else None


def column_kernel(geo, *refs):
    ny, bx, by, bz, rhs, rank = (geo[k] for k in ("ny", "bx", "by", "bz", "rhs", "rank"))
    read = Reader(refs)
    mom, halo = read.take(2)
    y1, y2 = read.take(2), read.take(2)
    (line,) = read.take(1)
    far = read.take(geo["extra_y"])
    one, send = read.take(2)
    base1 = bz * bx * rhs
    base2 = 2 * bz * rhs
    for yb in range(3):
        for z in range(6):
            inside = z in (2, 3)
            if yb == 1:
                tile = mom[bz * by + z - 2] if inside else halo[z if z < 2 else z - 2]
            elif inside:
                tile = tile_at(y1[yb // 2], base1 + (2 * bz + z - 2) * rank, rank)
            else:
                tile = tile_at(y2[yb // 2], base2 + (8 + (z if z < 2 else z - 2)) * rank, rank)
            one[yb * 6 + z] = tile
            at = sent_index(yb, z)
            if at is not None:
                send[at] = tile
    tiles = line.shape[0]
    for s in range(ny):
        for t in range(tiles):
            if s == 0:
                tile = line[t]
            elif s == 1 or s == ny - 1:
                tile = tile_at(y2[1 if s == 1 else 0], base2 + (12 + t) * rank, rank)
            else:
                tile = far[s - 2][t]
            send[14 + s * tiles + t] = tile


def near_weights(inverse, near_blocks, codes):
    return jnp.concatenate([near_blocks[inverse[c]] for c in codes], axis=1)


def find_inverse(table, inverse, count):
    for s in range(count):
        ox, oy, oz = (table[d, s] + 1 for d in range(3))
        inverse[(ox * 3 + oy) * 3 + oz] = s


def store_windows(shifts, at, stride, masks, width, mid, before, after):
    shifts[at] = roll(jnp.where(masks.lower, mid, before), 2 * width)
    shifts[stride + at] = roll(jnp.where(masks.last, before, mid), width)
    shifts[2 * stride + at] = mid
    shifts[3 * stride + at] = roll(jnp.where(masks.first, after, mid), -width)
    shifts[4 * stride + at] = roll(jnp.where(masks.lower, after, mid), 2 * width)


def windows_y(masks, width, tiles):
    low, mid, high = tiles
    return [
        low,
        roll(jnp.where(masks.lower, mid, low), 2 * width),
        mid,
        roll(jnp.where(masks.lower, high, mid), 2 * width),
        high,
    ]


def near_product(geo, weights, window, out, first, planes):
    bx, by, rhs = (geo[k] for k in ("bx", "by", "rhs"))
    rows, blocks = [], ([], [])
    for plane in planes:
        for ox in range(3):
            for oy in range(3):
                rows.append(window(first + plane, oy, ox))
                for k in range(2):
                    blocks[k].append(weights(ox, oy, plane + 1 - k))
    right = jnp.concatenate([jnp.concatenate(b, axis=1) for b in blocks], axis=0)
    value = dot(jnp.concatenate(rows, axis=1), right, ((1,), (1,)))
    for k in range(2):
        out[first + k] = value[:, 128 * k : 128 * (k + 1)]


def inner_kernel(geo, *refs):
    bx, by, bz, rhs = (geo[k] for k in ("bx", "by", "bz", "rhs"))
    read = Reader(refs)
    table, near_blocks, own = read.take(3)
    before, after = read.faces(geo)
    y1 = read.take(2)
    out, wide, inverse = read.take(3)
    pts = wide.shape[3]
    find_inverse(table, inverse, near_blocks.shape[0])
    rows = (bx + 2) * rhs
    none = jnp.zeros((rhs, pts), BF16)
    for z in range(bz):
        for k, y in enumerate((0, by + 1)):
            wide[z, y, 0:rhs] = none
            wide[z, y, rhs : rows - rhs] = y1[k][z * bx * rhs : (z + 1) * bx * rhs]
            wide[z, y, rows - rhs :] = none
        for y in range(1, by + 1):
            wide[z, y, 0:rhs] = before[z, y - 1]
            wide[z, y, rhs : rows - rhs] = own[z, y - 1].reshape(bx * rhs, pts)
            wide[z, y, rows - rhs :] = after[z, y - 1]
    empty = jnp.zeros((pts, pts), BF16)

    def weights(ox, oy, oz):
        return near_blocks[inverse[(ox * 3 + oy) * 3 + oz]] if 0 <= oz < 3 else empty

    def window(z, oy, ox):
        return wide[z, oy : oy + by, ox * rhs : (ox + bx) * rhs, :].reshape(by * bx * rhs, pts)

    for first in range(0, bz, 2):
        planes = [p for p in range(-1, 3) if 0 <= first + p < bz]
        near_product(geo, weights, window, out, first, planes)


def near_kernel(geo, *refs):
    xs, bx, by, bz, rhs, rank = (geo[k] for k in ("xs", "bx", "by", "bz", "rhs", "rank"))
    read = Reader(refs)
    table, near_blocks = read.take(2)
    read.take(1)
    (transfer,) = read.take(1)
    cz_prev, cz_next = read.take(2)
    y2 = read.take(2)
    sources = read.take(xs)
    (one,) = read.take(1)
    out, shifts, ones, corner_weights, lifted, wide, inverse = read.take(7)
    pts = wide.shape[3]
    find_inverse(table, inverse, near_blocks.shape[0])
    rows = (bx + 2) * rhs
    for k, s in enumerate((cz_prev, cz_next)):
        for y in (0, by + 1):
            wide[k, y] = jnp.zeros((rows, pts), BF16)
        for y in range(by):
            wide[k, y + 1] = s[y].reshape(rows, pts)
    for k, z in enumerate((0, bz - 1)):
        codes = [(ox * 3 + oy) * 3 + 2 * k for ox in range(3) for oy in range(3)]
        left = [
            wide[k, oy : oy + by, ox * rhs : (ox + bx) * rhs, :].reshape(by * bx * rhs, pts)
            for ox in range(3)
            for oy in range(3)
        ]
        right = near_weights(inverse, near_blocks, codes)
        out[z] = out[z] + dot(jnp.concatenate(left, axis=1), right, ((1,), (1,)))
    none = jnp.zeros((rhs, pts), BF16)
    for yk, y in enumerate((0, by - 1)):
        for xk, x in enumerate((0, bx - 1)):
            at = xk * bz * rhs
            column = y2[yk][at : at + bz * rhs]
            column = jnp.concatenate([none, column, none], axis=0)
            left = jnp.concatenate([column[oz * rhs : (oz + bz) * rhs] for oz in range(3)], axis=1)
            right = near_weights(inverse, near_blocks, [(6 * xk + 2 * yk) * 3 + oz for oz in range(3)])
            value = dot(left, right, ((1,), (1,)))
            at = (y * bx + x) * rhs
            for z in range(bz):
                out[z, at : at + rhs] = out[z, at : at + rhs] + value[z * rhs : (z + 1) * rhs]
    masks = Masks(rank, rhs)
    for z in range(bz + 4):
        for y in range(by):
            tiles = [s[z * by + y] for s in sources]
            at = z * (by + 4) + y + 2
            store_windows(shifts, at, (bz + 4) * (by + 4), masks, rhs, tiles[0], tiles[1], tiles[-1])
    for k in range(1, xs):
        groups = [
            [[sources[k][(2 * z + l) * by + y] for y in range(by)] for l in range(2)] for z in range(bz // 2 + 2)
        ]
        for z, tile in enumerate(lift(transfer, groups, rhs)):
            lifted[(k - 1) * 4 + z] = tile
    for z in range(6):
        for m, mid in enumerate(windows_y(masks, rhs, [one[yb * 6 + z] for yb in range(3)])):
            ones[(10 + m) * 6 + z] = mid
            ones[(5 + m) * 6 + z] = roll(mid, rhs)
            ones[(15 + m) * 6 + z] = roll(mid, -rhs)
    for yk in range(2):
        for zk in range(2):
            codes = [(ox * 3 + 2 * yk) * 3 + 2 * zk for ox in range(3)]
            corner_weights[yk, zk] = near_weights(inverse, near_blocks, codes)


def weight_kernel(coupling_in, coarse_in, transfer, coupling, coarse, down_one, down_zero):
    entries, rank = coupling_in.shape[1:3]
    for level in range(2):
        coupling[level] = jnp.concatenate([coupling_in[level, e] for e in range(entries)], axis=1)
    nx, ny, nz = coarse_in.shape[:3]
    coarse[...] = jnp.concatenate(
        [coarse_in[x, y, z] for x in range(nx) for y in range(ny) for z in range(nz)], axis=1
    )
    turned = [transfer[c].astype(F32).T.astype(BF16) for c in range(8)]
    for c in range(8):
        down_one[c * rank : (c + 1) * rank] = turned[c]
    for k in range(4):
        down_zero[k] = jnp.concatenate([turned[k], turned[4 + k]], axis=1)


def final_kernel(geo, *refs):
    nx, ny, nz, xs, bx, by, bz, rhs, rank = (
        geo[k] for k in ("nx", "ny", "nz", "xs", "bx", "by", "bz", "rhs", "rank")
    )
    width = rhs
    read = Reader(refs)
    far_in, live, near, corner_weights, basis, coupling, coarse, down_one, down_zero = read.take(9)
    read.take(2)
    beside = read.take(xs - 1)
    y1, y2, y3 = read.take(2), read.take(2), read.take(2)
    lifted, send = read.take(2)
    far_two = read.take(geo["extra_x"])
    out, shifts, ones = read.take(3)
    corners, planes, far_table, sems = read.take(4)
    table_copy = pltpu.make_async_copy(far_in, far_table, sems.at[bz])
    table_copy.start()
    blocks = lane_blocks(rank, width)
    masks = Masks(rank, width)
    entries = coupling.shape[2] // rank
    base1 = bz * bx * rhs
    base2 = 2 * bz * rhs
    base3 = 2 * (bx + 2) * rhs

    def leaf_tile(k, z, side, yy):
        if k > 0:
            return tile_at(y3[side], base3 + (((k - 1) * (bz + 4) + z + 2) * 2 + yy) * rank, rank)
        if 0 <= z < bz:
            return tile_at(y1[side], base1 + (z * 2 + yy) * rank, rank)
        zh = z + 2 if z < 0 else z - bz + 2
        return tile_at(y2[side], base2 + (zh * 2 + yy) * rank, rank)

    for z in range(-2, bz + 2):
        for side in range(2):
            for yy in range(2):
                tiles = [leaf_tile(k, z, side, yy) for k in range(xs)]
                at = (z + 2) * (by + 4) + yy + side * (by + 2)
                store_windows(shifts, at, (bz + 4) * (by + 4), masks, width, tiles[0], tiles[1], tiles[-1])

    def one_tile(k, yb, z):
        at = sent_index(yb, z)
        return lifted[k * 4 + z - 1] if at is None else beside[k][at]

    for z in range(6):
        sides = [windows_y(masks, width, [one_tile(k, yb, z) for yb in range(3)]) for k in range(xs - 1)]
        for m in range(5):
            before, after = sides[0][m], sides[-1][m]
            ones[m * 6 + z] = before
            ones[(20 + m) * 6 + z] = after
            at = (5 + m) * 6 + z
            ones[at] = jnp.where(masks.odd, ones[at], roll(before, -width))
            at = (15 + m) * 6 + z
            ones[at] = jnp.where(masks.odd, roll(after, width), ones[at])

    per = 128 // width
    tiles = -(-nz // per)

    def two_tile(s, t):
        if s == 0:
            return send[14 + t]
        if s == 1:
            return beside[-1][14 + t]
        if s == nx - 1:
            return beside[0][14 + t]
        return far_two[s - 2][t]

    lanes = lax.broadcasted_iota(jnp.int16, (rank, 128), 1)
    quarter = [(lanes >= jnp.int16(width * b)) & (lanes < jnp.int16(width * (b + 1))) for b in range(per)]
    stacked = []
    for s in range(nx):
        for y in range(ny):
            for b in range(nz):
                tile = two_tile(s, y * tiles + b // per)
                stacked.append(jnp.where(quarter[b % per], tile, jnp.zeros_like(tile)))
    two = dot(coarse[...], jnp.concatenate(stacked, axis=0))
    two = two + roll(two, 2 * width)
    two = (two + roll(two, width)).astype(BF16)

    table_copy.wait()
    starts = []
    for e in range(entries):
        ox, oy, oz = (far_table[d, 1, e] + 2 for d in range(3))
        starts.append((ox * 5 + oy) * 6 + oz)
    columns = [jnp.concatenate([ones[s + z] for s in starts], axis=0) for z in range(2)]
    local_one = dot(coupling[1], jnp.concatenate(columns, axis=1))
    from_two = dot(down_one[...], two)
    ups = []
    for z in range(2):
        total = local_one[:, 128 * z : 128 * (z + 1)]
        for j in range(2):
            for i in range(2):
                child = 4 * i + 2 * j + z
                part = from_two[child * rank : (child + 1) * rank]
                total = total + jnp.where(blocks == 2 * j + i, part, 0.0)
        total = total.astype(BF16)
        half = roll(total, 2 * width)
        none = jnp.zeros_like(total)
        for up in (
            jnp.where(masks.first, total, jnp.where(masks.last, half, roll(total, width))),
            jnp.where(masks.first, half, jnp.where(masks.last, total, roll(total, -width))),
        ):
            ups.append(jnp.concatenate([jnp.where(masks.odd, none, up), jnp.where(masks.odd, up, none)], axis=0))
    ups = jnp.concatenate(ups, axis=1)
    local = {}
    for j in range(2):
        for l in range(2):
            part = dot(down_zero[2 * j + l], ups)
            for z in range(2):
                for y in range(2):
                    at = 128 * (2 * z + y)
                    local[2 * z + l, 2 * y + j] = part[:, at : at + 128]

    for yk in range(2):
        for zk in range(2):
            windows = []
            for ox in range(3):
                at = (zk * (bx + 2) + ox) * rhs
                windows.append(y3[yk][at : at + bx * rhs])
            corners[yk, zk] = dot(jnp.concatenate(windows, axis=1), corner_weights[yk, zk], ((1,), (1,)))

    starts = []
    for e in range(entries):
        ox, oy, oz = (far_table[d, 0, e] + 2 for d in range(3))
        starts.append((ox * (bz + 4) + oz) * (by + 4) + oy)
    totals = []
    for z in range(bz):
        for y in range(0, by, 2):
            columns = [
                jnp.concatenate([shifts[s + z * (by + 4) + y + k] for s in starts], axis=0) for k in range(2)
            ]
            total = dot(coupling[0], jnp.concatenate(columns, axis=1))
            totals.append((total + jnp.concatenate([local[z, y], local[z, y + 1]], axis=1)).astype(BF16))
    copies = []
    for z in range(bz):
        for half in range(by // 2):
            y = 2 * half
            number = z * (by // 2) + half
            result = dot(totals[number], basis[...], ((0,), (0,)))
            result = result + near[z, half * 2 * bx * rhs : (half + 1) * 2 * bx * rhs]
            for k in range(2):
                block = result[k * bx * rhs : (k + 1) * bx * rhs]
                if y + k in (0, by - 1) and z in (0, bz - 1):
                    block = block + corners[0 if y + k == 0 else 1, 0 if z == 0 else 1]
                for x in range(bx):
                    planes[z, x, y + k] = block[x * rhs : (x + 1) * rhs] * live[x, y + k, z : z + 1]
        copies.append(pltpu.make_async_copy(planes.at[z], out.at[:, :, z], sems.at[z]))
        copies[-1].start()
    for c in copies:
        c.wait()


def body(charges, counts, near_offsets, near_blocks, leaf_basis, transfer, far_offsets, coupling, coarse_coupling):
    bx, by, bz, rhs, pts = charges.shape
    rank = leaf_basis.shape[0]
    entries = far_offsets.shape[1]
    stencil = near_blocks.shape[0]
    nx, ny, nz = (lax.axis_size(a) for a in ("gx", "gy", "gz"))
    assert (bx, by, bz) == (4, 4, 4) and bx * rhs == 128 and pts == 128
    xs = 2 if nx == 2 else 3
    geo = dict(nx=nx, ny=ny, nz=nz, xs=xs, bx=bx, by=by, bz=bz, rhs=rhs, rank=rank)
    geo["extra_x"] = max(nx - 3, 0)
    geo["extra_z"] = max(nz - 3, 0)
    geo["extra_y"] = max(ny - 3, 0)
    per = 128 // rhs
    tiles_z = -(-nz // per)

    def shape(*dims, dtype=BF16):
        return jax.ShapeDtypeStruct(dims, dtype)

    def part(kernel):
        return functools.partial(kernel, geo)

    live = (jnp.arange(pts, dtype=jnp.int32) < counts[..., None]).astype(F32)
    near_table = near_offsets.T
    far_table = far_offsets.transpose(2, 0, 1)

    token = run(start_kernel, shape(8, 128, dtype=jnp.int32), (), flops=10**10)
    assert rank == 48
    side = shape((2 * by + 1) * rank + 16, 128)
    message = shape(bz * bx * rhs + (bz * 2 + 2) * rank, 128)
    own, faces, mom, z_high, z_low, y_high, y_low, two = run(
        first_kernel,
        (
            shape(bz, by, bx, rhs, pts),
            shape(2, bz, by, rhs, pts),
            shape(bz * by + 2, rank, 128),
            side,
            side,
            message,
            message,
            shape(16, 128),
        ),
        (token, live, charges, leaf_basis, transfer),
    )
    mz_prev = from_shift(z_high, "gz", nz, -1)
    mz_next = from_shift(z_low, "gz", nz, 1)
    if nx == 2:
        faces = [from_shift(faces, "gx", nx, 1)]
    else:
        faces = [from_shift(faces[1:], "gx", nx, -1), from_shift(faces[:1], "gx", nx, 1)]
    extra = [from_shift(two, "gz", nz, s) for s in range(2, nz - 1)]
    y1 = [from_shift(y_high, "gy", ny, -1), from_shift(y_low, "gy", ny, 1)]

    weights = run(
        weight_kernel,
        (
            shape(2, rank, entries * rank),
            shape(rank, nx * ny * nz * rank),
            shape(8 * rank, rank),
            shape(4, rank, 2 * rank),
        ),
        (coupling, coarse_coupling, transfer),
    )

    charge = shape(by, bx + 2, rhs, pts)
    c_high, c_low, wide = run(
        part(second_kernel), (charge, charge, shape((bz + 4) * by, rank, 128)), (own, *faces, mom, mz_prev, mz_next)
    )
    message = shape(2 * bz * rhs + (12 + tiles_z) * rank, 128)
    y_high, y_low, line, halo = run(
        part(sides_kernel),
        (message, message, shape(tiles_z, rank, 128), shape(4, rank, 128)),
        (*faces, transfer, mz_prev, mz_next, two, *extra),
    )
    if nx == 2:
        sources = [wide, from_shift(wide, "gx", nx, 1)]
    else:
        sources = [wide, from_shift(wide, "gx", nx, -1), from_shift(wide, "gx", nx, 1)]
    cz_prev = from_shift(c_high, "gz", nz, -1)
    cz_next = from_shift(c_low, "gz", nz, 1)
    y2 = [from_shift(y_high, "gy", ny, -1), from_shift(y_low, "gy", ny, 1)]
    extra = [from_shift(line, "gy", ny, s) for s in range(2, ny - 1)]

    field = shape(bz, by * bx * rhs, pts, dtype=F32)
    near = run(
        part(inner_kernel),
        field,
        (near_table, near_blocks, own, *faces, *y1),
        smem=(0,),
        scratch=[
            pltpu.VMEM((bz, by + 2, (bx + 2) * rhs, pts), BF16),
            pltpu.SMEM((stencil,), jnp.int32),
        ],
        limit=16,
        flops=2 * bx * by * bz * rhs * pts * pts * stencil,
    )

    message = shape(2 * (bx + 2) * rhs + (xs - 1) * 2 * (bz + 4) * rank, 128)
    y_high, y_low = run(part(third_kernel), (message, message), (cz_prev, cz_next, *sources[1:]))
    one, send = run(
        part(column_kernel),
        (shape(18, rank, 128), shape(14 + ny * tiles_z, rank, 128)),
        (mom, halo, *y1, *y2, line, *extra),
    )
    if nx == 2:
        beside = [from_shift(send, "gx", nx, 1)]
    else:
        beside = [from_shift(send, "gx", nx, -1), from_shift(send, "gx", nx, 1)]
    y3 = [from_shift(y_high, "gy", ny, -1), from_shift(y_low, "gy", ny, 1)]
    extra = [from_shift(send[14:], "gx", nx, s) for s in range(2, nx - 1)]

    windows = shape(5 * (bz + 4) * (by + 4), rank, 128)
    columns = shape(5 * 5 * 6, rank, 128)
    near, shifts, ones, corner_weights, lifted = run(
        part(near_kernel),
        (field, windows, columns, shape(2, 2, pts, 3 * pts), shape((xs - 1) * 4, rank, 128)),
        (near_table, near_blocks, near, transfer, cz_prev, cz_next, *y2, *sources, one),
        smem=(0,),
        aliases={2: 0},
        scratch=[
            pltpu.VMEM((2, by + 2, (bx + 2) * rhs, pts), BF16),
            pltpu.SMEM((stencil,), jnp.int32),
        ],
        limit=16,
        flops=2 * bx * by * bz * rhs * pts * pts * 9,
    )
    args = (
        far_table,
        live,
        near,
        corner_weights,
        leaf_basis,
        *weights,
        shifts,
        ones,
        *beside,
        *y1,
        *y2,
        *y3,
        lifted,
        send,
        *extra,
    )
    potentials, _, _ = run(
        part(final_kernel),
        (shape(bx, by, bz, rhs, pts, dtype=F32), windows, columns),
        args,
        anywhere=(0,),
        hbm_out=(0,),
        aliases={9: 1, 10: 2},
        limit=24,
        scratch=[
            pltpu.VMEM((2, 2, bx * rhs, pts), F32),
            pltpu.VMEM((bz, bx, by, rhs, pts), F32),
            pltpu.SMEM(far_table.shape, jnp.int32),
            pltpu.SemaphoreType.DMA((bz + 1,)),
        ],
    )
    return potentials


def solution(mesh):
    in_specs = (
        P("gx", "gy", "gz", None, None),
        P("gx", "gy", "gz"),
        P(),
        P(),
        P(),
        P(),
        P(),
        P(),
        P(),
    )
    out_specs = P("gx", "gy", "gz", None, None)

    return jax.shard_map(body, mesh=mesh, in_specs=in_specs, out_specs=out_specs, check_vma=False)
```

```python
import functools

import jax
import jax.numpy as jnp
from jax import lax
from jax.experimental import pallas as pl
from jax.experimental.pallas import tpu as pltpu
from jax.sharding import PartitionSpec as P


F32 = jnp.float32
BF16 = jnp.bfloat16


def from_shift(value, axis, size, shift):
    return lax.ppermute(value, axis, [(i, (i - shift) % size) for i in range(size)])


def spec_vmem():
    return pl.BlockSpec(memory_space=pltpu.VMEM)


def spec_smem():
    return pl.BlockSpec(memory_space=pltpu.SMEM)


def run(kernel, out_shape, args, smem=(), anywhere=(), scratch=(), flops=None, limit=8, hbm_out=(), aliases=None):
    def spec(i):
        if i in anywhere:
            return pl.BlockSpec(memory_space=pl.ANY)
        return spec_smem() if i in smem else spec_vmem()

    cost = None
    if flops is not None:
        cost = pl.CostEstimate(flops=flops, transcendentals=0, bytes_accessed=0)
    count = len(out_shape) if isinstance(out_shape, tuple) else 1
    outs = tuple(pl.BlockSpec(memory_space=pltpu.HBM) if i in hbm_out else spec_vmem() for i in range(count))
    return pl.pallas_call(
        kernel,
        out_shape=out_shape,
        in_specs=[spec(i) for i in range(len(args))],
        out_specs=outs if isinstance(out_shape, tuple) else outs[0],
        input_output_aliases=aliases or {},
        scratch_shapes=scratch,
        compiler_params=pltpu.CompilerParams(vmem_limit_bytes=limit * 1024 * 1024),
        cost_estimate=cost,
    )(*args)


def lane_blocks(rows, width):
    return lax.broadcasted_iota(jnp.int32, (rows, 128), 1) // width


class Masks:
    def __init__(self, rank, width):
        lanes = lax.broadcasted_iota(jnp.int16, (rank, 128), 1)
        bound = [jnp.int16(width * k) for k in range(4)]
        self.first = lanes < bound[1]
        self.lower = lanes < bound[2]
        self.last = lanes >= bound[3]
        self.odd = ((lanes >= bound[1]) & self.lower) | self.last


def roll(value, shift):
    shift = shift % 128
    return value if shift == 0 else pltpu.roll(value, shift, 1)


def dot(a, b, dims=((1,), (0,))):
    return lax.dot_general(a, b, (dims, ((), ())), preferred_element_type=F32)


def assemble(sources, width, load):
    per = 128 // width
    out = []
    for start in range(0, len(sources), per):
        total = None
        for d, (key, b) in enumerate(sources[start : start + per]):
            moved = roll(load(key).astype(F32), width * (d - b))
            if total is None:
                total = moved
                blocks = lane_blocks(moved.shape[0], width)
            else:
                total = jnp.where(blocks == d, moved, total)
        out.append(total.astype(BF16))
    return out


def tile_at(ref, start, rank):
    return ref[start : start + rank, :]


def start_kernel(out):
    out[...] = jnp.zeros(out.shape, out.dtype)


def lift(transfer, groups, width):
    sums = [None, None]
    for i in range(2):
        for j in range(2):
            for l in range(2):
                cols = jnp.concatenate([g[l][2 * y + j] for g in groups for y in range(2)], axis=1)
                part = dot(transfer[4 * i + 2 * j + l], cols)
                sums[i] = part if sums[i] is None else sums[i] + part
    blocks = lane_blocks(sums[0].shape[0], width)
    tiles = []
    for z in range(len(groups)):
        whole = []
        for y in range(2):
            at = 128 * (z * 2 + y)
            whole.append(sums[0][:, at : at + 128] + roll(sums[1][:, at : at + 128], -width))
        packed = jnp.where(
            blocks == 0,
            whole[0],
            jnp.where(
                blocks == 1,
                roll(whole[0], -width),
                jnp.where(blocks == 2, roll(whole[1], 2 * width), roll(whole[1], width)),
            ),
        )
        tiles.append(packed.astype(BF16))
    return tiles


def fold(tile, width):
    masks = Masks(16, width)
    rows = [tile[16 * k : 16 * (k + 1)] for k in range(3)]
    return jnp.where(masks.first, rows[0], jnp.where(masks.lower, roll(rows[1], width), roll(rows[2], 2 * width)))


def unfold(rows, width):
    return jnp.concatenate([rows, roll(rows, -width), roll(rows, -2 * width)], axis=0)


def top(transfer, low, high, width):
    total = None
    for j in range(2):
        for i in range(2):
            part = dot(transfer[4 * i + 2 * j], low) + dot(transfer[4 * i + 2 * j + 1], high)
            part = roll(part, -width * (2 * j + i))
            total = part if total is None else total + part
    return total.astype(BF16)


def first_kernel(token, live, charges, basis, transfer, own, faces, mom, z_high, z_low):
    bx, by, bz, rhs, pts = charges.shape
    rank = basis.shape[0]
    width = rhs
    for x in range(bx):
        for y in range(by):
            for z in range(bz):
                value = (charges[x, y, z].astype(F32) * live[x, y, z : z + 1]).astype(BF16)
                own[z, y, x] = value
                if x == 0:
                    faces[0, z, y] = value
                if x == bx - 1:
                    faces[1, z, y] = value
    leaf = {}
    for z in range(bz):
        for y in range(0, by, 2):
            rows = own[z, y : y + 2].reshape(2 * bx * rhs, pts)
            value = dot(basis[...], rows, ((1,), (1,))).astype(BF16)
            for k in range(2):
                tile = value[:, 128 * k : 128 * (k + 1)]
                leaf[z, y + k] = tile
                mom[z * by + y + k] = tile
                at = (z % 2 * by + y + k) * rank
                (z_low if z < 2 else z_high)[at : at + rank] = tile
    one = lift(transfer, [[[leaf[2 * z + l, y] for y in range(by)] for l in range(2)] for z in range(2)], width)
    for z in range(2):
        mom[bz * by + z] = one[z]
        (z_low if z else z_high)[2 * by * rank :] = one[z]


def rest_kernel(own, mom, transfer, y_high, y_low, two):
    bz, by, bx, rhs, pts = own.shape
    rank = mom.shape[1]
    rows = bx * rhs
    base = bz * rows
    for out, y in ((y_high, by - 1), (y_low, 0)):
        start = by - 2 if y else 0
        for z in range(bz):
            out[z * rows : (z + 1) * rows] = own[z, y].reshape(rows, pts)
            for k in range(2):
                at = base + (z * 2 + k) * rank
                out[at : at + rank] = mom[z * by + start + k]
        for z in range(2):
            at = base + (2 * bz + z) * rank
            out[at : at + rank] = mom[bz * by + z]
    two[...] = fold(top(transfer, mom[bz * by], mom[bz * by + 1], rhs), rhs)


class Reader:
    def __init__(self, refs):
        self.refs = iter(refs)

    def take(self, count):
        return [next(self.refs) for _ in range(count)]

    def faces(self, geo):
        if geo["nx"] == 2:
            (both,) = self.take(1)
            return both.at[1], both.at[0]
        before, after = self.take(2)
        return before.at[0], after.at[0]


def second_kernel(geo, *refs):
    bx, by, bz, rank = (geo[k] for k in ("bx", "by", "bz", "rank"))
    read = Reader(refs)
    (own,) = read.take(1)
    before, after = read.faces(geo)
    mom, prev, nxt = read.take(3)
    c_high, c_low, wide = read.take(3)
    for z in range(bz + 4):
        for y in range(by):
            if z < 2:
                tile = tile_at(prev, (z * by + y) * rank, rank)
            elif z >= bz + 2:
                tile = tile_at(nxt, ((z - bz - 2) * by + y) * rank, rank)
            else:
                tile = mom[(z - 2) * by + y]
            wide[z * by + y] = tile
    for out, z in ((c_high, bz - 1), (c_low, 0)):
        for y in range(by):
            out[y, 0] = before[z, y]
            out[y, 1 : bx + 1] = own[z, y]
            out[y, bx + 1] = after[z, y]


def sides_kernel(geo, *refs):
    nz, _, by, bz, rhs, rank = (geo[k] for k in ("nz", "bx", "by", "bz", "rhs", "rank"))
    read = Reader(refs)
    before, after = read.faces(geo)
    transfer, prev, nxt, mine = read.take(4)
    far = read.take(geo["extra_z"])
    y_high, y_low, line, halo = read.take(4)

    def leaf(s, z, y):
        return tile_at(s, (z * by + y) * rank, rank)

    near = lift(transfer, [[[leaf(s, l, y) for y in range(by)] for l in range(2)] for s in (prev, nxt)], rhs)
    sent = [tile_at(s, 2 * by * rank, rank) for s in (prev, nxt)]
    level = [sent[0], near[0], near[1], sent[1]]
    base = 2 * bz * rhs
    for z in range(4):
        halo[z] = level[z]
        at = base + (8 + z) * rank
        y_high[at : at + rank] = level[z]
        y_low[at : at + rank] = level[z]
    for out, y in ((y_high, by - 1), (y_low, 0)):
        for k, s in enumerate((before, after)):
            for z in range(bz):
                at = (k * bz + z) * rhs
                out[at : at + rhs] = s[z, y]
        start = by - 2 if y else 0
        for zh in range(4):
            for yy in range(2):
                at = base + (zh * 2 + yy) * rank
                out[at : at + rank] = leaf(prev if zh < 2 else nxt, zh % 2, start + yy)

    def load(key):
        if key == 1:
            return top(transfer, level[2], level[3], rhs)
        if key == nz - 1:
            return top(transfer, level[0], level[1], rhs)
        return unfold(mine[...] if key == 0 else far[key - 2][...], rhs)

    for t, tile in enumerate(assemble([(k, 0) for k in range(nz)], rhs, load)):
        line[t] = tile
        at = base + (12 + t) * rank
        y_high[at : at + rank] = tile
        y_low[at : at + rank] = tile


def third_kernel(geo, *refs):
    xs, bx, by, bz, rhs, rank = (geo[k] for k in ("xs", "bx", "by", "bz", "rhs", "rank"))
    read = Reader(refs)
    prev, nxt = read.take(2)
    sources = [None] + read.take(xs - 1)
    y_high, y_low = read.take(2)
    base = 2 * (bx + 2) * rhs
    for out, y in ((y_high, by - 1), (y_low, 0)):
        for k, s in enumerate((prev, nxt)):
            at = k * (bx + 2) * rhs
            out[at : at + (bx + 2) * rhs] = s[y].reshape((bx + 2) * rhs, s.shape[3])
        start = by - 2 if y else 0
        for k in range(1, xs):
            for z in range(bz + 4):
                for yy in range(2):
                    at = base + (((k - 1) * (bz + 4) + z) * 2 + yy) * rank
                    out[at : at + rank] = sources[k][z * by + start + yy]


def sent_index(yb, z):
    left_out = [(1, k) for k in range(1, 5)]
    order = [(b, k) for b in range(3) for k in range(6) if (b, k) not in left_out]
    return order.index((yb, z)) if (yb, z) in order else None


def column_kernel(geo, *refs):
    ny, bx, by, bz, rhs, rank = (geo[k] for k in ("ny", "bx", "by", "bz", "rhs", "rank"))
    read = Reader(refs)
    mom, halo = read.take(2)
    y1, y2 = read.take(2), read.take(2)
    (line,) = read.take(1)
    far = read.take(geo["extra_y"])
    one, send = read.take(2)
    base1 = bz * bx * rhs
    base2 = 2 * bz * rhs
    for yb in range(3):
        for z in range(6):
            inside = z in (2, 3)
            if yb == 1:
                tile = mom[bz * by + z - 2] if inside else halo[z if z < 2 else z - 2]
            elif inside:
                tile = tile_at(y1[yb // 2], base1 + (2 * bz + z - 2) * rank, rank)
            else:
                tile = tile_at(y2[yb // 2], base2 + (8 + (z if z < 2 else z - 2)) * rank, rank)
            one[yb * 6 + z] = tile
            at = sent_index(yb, z)
            if at is not None:
                send[at] = tile
    tiles = line.shape[0]
    for s in range(ny):
        for t in range(tiles):
            if s == 0:
                tile = line[t]
            elif s == 1 or s == ny - 1:
                tile = tile_at(y2[1 if s == 1 else 0], base2 + (12 + t) * rank, rank)
            else:
                tile = far[s - 2][t]
            send[14 + s * tiles + t] = tile


def near_weights(inverse, near_blocks, codes):
    return jnp.concatenate([near_blocks[inverse[c]] for c in codes], axis=1)


def find_inverse(table, inverse, count):
    for s in range(count):
        ox, oy, oz = (table[d, s] + 1 for d in range(3))
        inverse[(ox * 3 + oy) * 3 + oz] = s


def store_windows(shifts, at, stride, masks, width, mid, before, after):
    shifts[at] = roll(jnp.where(masks.lower, mid, before), 2 * width)
    shifts[stride + at] = roll(jnp.where(masks.last, before, mid), width)
    shifts[2 * stride + at] = mid
    shifts[3 * stride + at] = roll(jnp.where(masks.first, after, mid), -width)
    shifts[4 * stride + at] = roll(jnp.where(masks.lower, after, mid), 2 * width)


def windows_y(masks, width, tiles):
    low, mid, high = tiles
    return [
        low,
        roll(jnp.where(masks.lower, mid, low), 2 * width),
        mid,
        roll(jnp.where(masks.lower, high, mid), 2 * width),
        high,
    ]


def near_product(geo, weights, window, out, first, planes):
    bx, by, rhs = (geo[k] for k in ("bx", "by", "rhs"))
    rows, blocks = [], ([], [])
    for plane in planes:
        for ox in range(3):
            for oy in range(3):
                rows.append(window(first + plane, oy, ox))
                for k in range(2):
                    blocks[k].append(weights(ox, oy, plane + 1 - k))
    right = jnp.concatenate([jnp.concatenate(b, axis=1) for b in blocks], axis=0)
    value = dot(jnp.concatenate(rows, axis=1), right, ((1,), (1,)))
    for k in range(2):
        out[first + k] = value[:, 128 * k : 128 * (k + 1)]


def inner_kernel(geo, *refs):
    bx, by, bz, rhs = (geo[k] for k in ("bx", "by", "bz", "rhs"))
    read = Reader(refs)
    table, near_blocks, own = read.take(3)
    before, after = read.faces(geo)
    y1 = read.take(2)
    out, wide, inverse = read.take(3)
    pts = wide.shape[3]
    find_inverse(table, inverse, near_blocks.shape[0])
    rows = (bx + 2) * rhs
    none = jnp.zeros((rhs, pts), BF16)
    for z in range(bz):
        for k, y in enumerate((0, by + 1)):
            wide[z, y, 0:rhs] = none
            wide[z, y, rhs : rows - rhs] = y1[k][z * bx * rhs : (z + 1) * bx * rhs]
            wide[z, y, rows - rhs :] = none
        for y in range(1, by + 1):
            wide[z, y, 0:rhs] = before[z, y - 1]
            wide[z, y, rhs : rows - rhs] = own[z, y - 1].reshape(bx * rhs, pts)
            wide[z, y, rows - rhs :] = after[z, y - 1]
    empty = jnp.zeros((pts, pts), BF16)

    def weights(ox, oy, oz):
        return near_blocks[inverse[(ox * 3 + oy) * 3 + oz]] if 0 <= oz < 3 else empty

    def window(z, oy, ox):
        return wide[z, oy : oy + by, ox * rhs : (ox + bx) * rhs, :].reshape(by * bx * rhs, pts)

    for first in range(0, bz, 2):
        planes = [p for p in range(-1, 3) if 0 <= first + p < bz]
        near_product(geo, weights, window, out, first, planes)


def near_kernel(geo, *refs):
    xs, bx, by, bz, rhs, rank = (geo[k] for k in ("xs", "bx", "by", "bz", "rhs", "rank"))
    read = Reader(refs)
    table, near_blocks = read.take(2)
    read.take(1)
    (transfer,) = read.take(1)
    cz_prev, cz_next = read.take(2)
    y2 = read.take(2)
    sources = read.take(xs)
    (one,) = read.take(1)
    out, shifts, ones, corner_weights, lifted, wide, inverse = read.take(7)
    pts = wide.shape[3]
    find_inverse(table, inverse, near_blocks.shape[0])
    rows = (bx + 2) * rhs
    for k, s in enumerate((cz_prev, cz_next)):
        for y in (0, by + 1):
            wide[k, y] = jnp.zeros((rows, pts), BF16)
        for y in range(by):
            wide[k, y + 1] = s[y].reshape(rows, pts)
    for k, z in enumerate((0, bz - 1)):
        codes = [(ox * 3 + oy) * 3 + 2 * k for ox in range(3) for oy in range(3)]
        left = [
            wide[k, oy : oy + by, ox * rhs : (ox + bx) * rhs, :].reshape(by * bx * rhs, pts)
            for ox in range(3)
            for oy in range(3)
        ]
        right = near_weights(inverse, near_blocks, codes)
        out[z] = out[z] + dot(jnp.concatenate(left, axis=1), right, ((1,), (1,)))
    none = jnp.zeros((rhs, pts), BF16)
    for yk, y in enumerate((0, by - 1)):
        for xk, x in enumerate((0, bx - 1)):
            at = xk * bz * rhs
            column = y2[yk][at : at + bz * rhs]
            column = jnp.concatenate([none, column, none], axis=0)
            left = jnp.concatenate([column[oz * rhs : (oz + bz) * rhs] for oz in range(3)], axis=1)
            right = near_weights(inverse, near_blocks, [(6 * xk + 2 * yk) * 3 + oz for oz in range(3)])
            value = dot(left, right, ((1,), (1,)))
            at = (y * bx + x) * rhs
            for z in range(bz):
                out[z, at : at + rhs] = out[z, at : at + rhs] + value[z * rhs : (z + 1) * rhs]
    masks = Masks(rank, rhs)
    for z in range(bz + 4):
        for y in range(by):
            tiles = [s[z * by + y] for s in sources]
            at = z * (by + 4) + y + 2
            store_windows(shifts, at, (bz + 4) * (by + 4), masks, rhs, tiles[0], tiles[1], tiles[-1])
    for k in range(1, xs):
        groups = [
            [[sources[k][(2 * z + l) * by + y] for y in range(by)] for l in range(2)] for z in range(bz // 2 + 2)
        ]
        for z, tile in enumerate(lift(transfer, groups, rhs)):
            lifted[(k - 1) * 4 + z] = tile
    for z in range(6):
        for m, mid in enumerate(windows_y(masks, rhs, [one[yb * 6 + z] for yb in range(3)])):
            ones[(10 + m) * 6 + z] = mid
            ones[(5 + m) * 6 + z] = roll(mid, rhs)
            ones[(15 + m) * 6 + z] = roll(mid, -rhs)
    for yk in range(2):
        for zk in range(2):
            codes = [(ox * 3 + 2 * yk) * 3 + 2 * zk for ox in range(3)]
            corner_weights[yk, zk] = near_weights(inverse, near_blocks, codes)


def weight_kernel(coupling_in, coarse_in, transfer, coupling, coarse, down_one, down_zero):
    entries, rank = coupling_in.shape[1:3]
    for level in range(2):
        coupling[level] = jnp.concatenate([coupling_in[level, e] for e in range(entries)], axis=1)
    nx, ny, nz = coarse_in.shape[:3]
    coarse[...] = jnp.concatenate(
        [coarse_in[x, y, z] for x in range(nx) for y in range(ny) for z in range(nz)], axis=1
    )
    turned = [transfer[c].astype(F32).T.astype(BF16) for c in range(8)]
    for c in range(8):
        down_one[c * rank : (c + 1) * rank] = turned[c]
    for k in range(4):
        down_zero[k] = jnp.concatenate([turned[k], turned[4 + k]], axis=1)


def final_kernel(geo, *refs):
    nx, ny, nz, xs, bx, by, bz, rhs, rank = (
        geo[k] for k in ("nx", "ny", "nz", "xs", "bx", "by", "bz", "rhs", "rank")
    )
    width = rhs
    read = Reader(refs)
    far_in, live, near, corner_weights, basis, coupling, coarse, down_one, down_zero = read.take(9)
    read.take(2)
    beside = read.take(xs - 1)
    y1, y2, y3 = read.take(2), read.take(2), read.take(2)
    lifted, send = read.take(2)
    far_two = read.take(geo["extra_x"])
    out, shifts, ones = read.take(3)
    corners, planes, far_table, sems = read.take(4)
    table_copy = pltpu.make_async_copy(far_in, far_table, sems.at[bz])
    table_copy.start()
    blocks = lane_blocks(rank, width)
    masks = Masks(rank, width)
    entries = coupling.shape[2] // rank
    base1 = bz * bx * rhs
    base2 = 2 * bz * rhs
    base3 = 2 * (bx + 2) * rhs

    def leaf_tile(k, z, side, yy):
        if k > 0:
            return tile_at(y3[side], base3 + (((k - 1) * (bz + 4) + z + 2) * 2 + yy) * rank, rank)
        if 0 <= z < bz:
            return tile_at(y1[side], base1 + (z * 2 + yy) * rank, rank)
        zh = z + 2 if z < 0 else z - bz + 2
        return tile_at(y2[side], base2 + (zh * 2 + yy) * rank, rank)

    for z in range(-2, bz + 2):
        for side in range(2):
            for yy in range(2):
                tiles = [leaf_tile(k, z, side, yy) for k in range(xs)]
                at = (z + 2) * (by + 4) + yy + side * (by + 2)
                store_windows(shifts, at, (bz + 4) * (by + 4), masks, width, tiles[0], tiles[1], tiles[-1])

    def one_tile(k, yb, z):
        at = sent_index(yb, z)
        return lifted[k * 4 + z - 1] if at is None else beside[k][at]

    for z in range(6):
        sides = [windows_y(masks, width, [one_tile(k, yb, z) for yb in range(3)]) for k in range(xs - 1)]
        for m in range(5):
            before, after = sides[0][m], sides[-1][m]
            ones[m * 6 + z] = before
            ones[(20 + m) * 6 + z] = after
            at = (5 + m) * 6 + z
            ones[at] = jnp.where(masks.odd, ones[at], roll(before, -width))
            at = (15 + m) * 6 + z
            ones[at] = jnp.where(masks.odd, roll(after, width), ones[at])

    per = 128 // width
    tiles = -(-nz // per)

    def two_tile(s, t):
        if s == 0:
            return send[14 + t]
        if s == 1:
            return beside[-1][14 + t]
        if s == nx - 1:
            return beside[0][14 + t]
        return far_two[s - 2][t]

    lanes = lax.broadcasted_iota(jnp.int16, (rank, 128), 1)
    quarter = [(lanes >= jnp.int16(width * b)) & (lanes < jnp.int16(width * (b + 1))) for b in range(per)]
    stacked = []
    for s in range(nx):
        for y in range(ny):
            for b in range(nz):
                tile = two_tile(s, y * tiles + b // per)
                stacked.append(jnp.where(quarter[b % per], tile, jnp.zeros_like(tile)))
    two = dot(coarse[...], jnp.concatenate(stacked, axis=0))
    two = two + roll(two, 2 * width)
    two = (two + roll(two, width)).astype(BF16)

    table_copy.wait()
    starts = []
    for e in range(entries):
        ox, oy, oz = (far_table[d, 1, e] + 2 for d in range(3))
        starts.append((ox * 5 + oy) * 6 + oz)
    columns = [jnp.concatenate([ones[s + z] for s in starts], axis=0) for z in range(2)]
    local_one = dot(coupling[1], jnp.concatenate(columns, axis=1))
    from_two = dot(down_one[...], two)
    ups = []
    for z in range(2):
        total = local_one[:, 128 * z : 128 * (z + 1)]
        for j in range(2):
            for i in range(2):
                child = 4 * i + 2 * j + z
                part = from_two[child * rank : (child + 1) * rank]
                total = total + jnp.where(blocks == 2 * j + i, part, 0.0)
        total = total.astype(BF16)
        half = roll(total, 2 * width)
        none = jnp.zeros_like(total)
        for up in (
            jnp.where(masks.first, total, jnp.where(masks.last, half, roll(total, width))),
            jnp.where(masks.first, half, jnp.where(masks.last, total, roll(total, -width))),
        ):
            ups.append(jnp.concatenate([jnp.where(masks.odd, none, up), jnp.where(masks.odd, up, none)], axis=0))
    ups = jnp.concatenate(ups, axis=1)
    local = {}
    for j in range(2):
        for l in range(2):
            part = dot(down_zero[2 * j + l], ups)
            for z in range(2):
                for y in range(2):
                    at = 128 * (2 * z + y)
                    local[2 * z + l, 2 * y + j] = part[:, at : at + 128]

    for yk in range(2):
        for zk in range(2):
            windows = []
            for ox in range(3):
                at = (zk * (bx + 2) + ox) * rhs
                windows.append(y3[yk][at : at + bx * rhs])
            corners[yk, zk] = dot(jnp.concatenate(windows, axis=1), corner_weights[yk, zk], ((1,), (1,)))

    starts = []
    for e in range(entries):
        ox, oy, oz = (far_table[d, 0, e] + 2 for d in range(3))
        starts.append((ox * (bz + 4) + oz) * (by + 4) + oy)
    totals = []
    for z in range(bz):
        for y in range(0, by, 2):
            columns = [
                jnp.concatenate([shifts[s + z * (by + 4) + y + k] for s in starts], axis=0) for k in range(2)
            ]
            total = dot(coupling[0], jnp.concatenate(columns, axis=1))
            totals.append((total + jnp.concatenate([local[z, y], local[z, y + 1]], axis=1)).astype(BF16))
    copies = []
    for z in range(bz):
        for half in range(by // 2):
            y = 2 * half
            number = z * (by // 2) + half
            result = dot(totals[number], basis[...], ((0,), (0,)))
            result = result + near[z, half * 2 * bx * rhs : (half + 1) * 2 * bx * rhs]
            for k in range(2):
                block = result[k * bx * rhs : (k + 1) * bx * rhs]
                if y + k in (0, by - 1) and z in (0, bz - 1):
                    block = block + corners[0 if y + k == 0 else 1, 0 if z == 0 else 1]
                for x in range(bx):
                    planes[z, x, y + k] = block[x * rhs : (x + 1) * rhs] * live[x, y + k, z : z + 1]
        copies.append(pltpu.make_async_copy(planes.at[z], out.at[:, :, z], sems.at[z]))
        copies[-1].start()
    for c in copies:
        c.wait()


def body(charges, counts, near_offsets, near_blocks, leaf_basis, transfer, far_offsets, coupling, coarse_coupling):
    bx, by, bz, rhs, pts = charges.shape
    rank = leaf_basis.shape[0]
    entries = far_offsets.shape[1]
    stencil = near_blocks.shape[0]
    nx, ny, nz = (lax.axis_size(a) for a in ("gx", "gy", "gz"))
    assert (bx, by, bz) == (4, 4, 4) and bx * rhs == 128 and pts == 128
    xs = 2 if nx == 2 else 3
    geo = dict(nx=nx, ny=ny, nz=nz, xs=xs, bx=bx, by=by, bz=bz, rhs=rhs, rank=rank)
    geo["extra_x"] = max(nx - 3, 0)
    geo["extra_z"] = max(nz - 3, 0)
    geo["extra_y"] = max(ny - 3, 0)
    per = 128 // rhs
    tiles_z = -(-nz // per)

    def shape(*dims, dtype=BF16):
        return jax.ShapeDtypeStruct(dims, dtype)

    def part(kernel):
        return functools.partial(kernel, geo)

    live = (jnp.arange(pts, dtype=jnp.int32) < counts[..., None]).astype(F32)
    near_table = near_offsets.T
    far_table = far_offsets.transpose(2, 0, 1)

    token = run(start_kernel, shape(8, 128, dtype=jnp.int32), (), flops=10**10)
    assert rank == 48
    side = shape((2 * by + 1) * rank, 128)
    message = shape(bz * bx * rhs + (bz * 2 + 2) * rank, 128)
    own, faces, mom, z_high, z_low = run(
        first_kernel,
        (
            shape(bz, by, bx, rhs, pts),
            shape(2, bz, by, rhs, pts),
            shape(bz * by + 2, rank, 128),
            side,
            side,
        ),
        (token, live, charges, leaf_basis, transfer),
    )
    y_high, y_low, two = run(rest_kernel, (message, message, shape(16, 128)), (own, mom, transfer))
    mz_prev = from_shift(z_high, "gz", nz, -1)
    mz_next = from_shift(z_low, "gz", nz, 1)
    if nx == 2:
        faces = [from_shift(faces, "gx", nx, 1)]
    else:
        faces = [from_shift(faces[1:], "gx", nx, -1), from_shift(faces[:1], "gx", nx, 1)]
    extra = [from_shift(two, "gz", nz, s) for s in range(2, nz - 1)]
    y1 = [from_shift(y_high, "gy", ny, -1), from_shift(y_low, "gy", ny, 1)]

    weights = run(
        weight_kernel,
        (
            shape(2, rank, entries * rank),
            shape(rank, nx * ny * nz * rank),
            shape(8 * rank, rank),
            shape(4, rank, 2 * rank),
        ),
        (coupling, coarse_coupling, transfer),
    )

    charge = shape(by, bx + 2, rhs, pts)
    c_high, c_low, wide = run(
        part(second_kernel), (charge, charge, shape((bz + 4) * by, rank, 128)), (own, *faces, mom, mz_prev, mz_next)
    )
    message = shape(2 * bz * rhs + (12 + tiles_z) * rank, 128)
    y_high, y_low, line, halo = run(
        part(sides_kernel),
        (message, message, shape(tiles_z, rank, 128), shape(4, rank, 128)),
        (*faces, transfer, mz_prev, mz_next, two, *extra),
    )
    if nx == 2:
        sources = [wide, from_shift(wide, "gx", nx, 1)]
    else:
        sources = [wide, from_shift(wide, "gx", nx, -1), from_shift(wide, "gx", nx, 1)]
    cz_prev = from_shift(c_high, "gz", nz, -1)
    cz_next = from_shift(c_low, "gz", nz, 1)
    y2 = [from_shift(y_high, "gy", ny, -1), from_shift(y_low, "gy", ny, 1)]
    extra = [from_shift(line, "gy", ny, s) for s in range(2, ny - 1)]

    field = shape(bz, by * bx * rhs, pts, dtype=F32)
    near = run(
        part(inner_kernel),
        field,
        (near_table, near_blocks, own, *faces, *y1),
        smem=(0,),
        scratch=[
            pltpu.VMEM((bz, by + 2, (bx + 2) * rhs, pts), BF16),
            pltpu.SMEM((stencil,), jnp.int32),
        ],
        limit=16,
        flops=2 * bx * by * bz * rhs * pts * pts * stencil,
    )

    message = shape(2 * (bx + 2) * rhs + (xs - 1) * 2 * (bz + 4) * rank, 128)
    y_high, y_low = run(part(third_kernel), (message, message), (cz_prev, cz_next, *sources[1:]))
    one, send = run(
        part(column_kernel),
        (shape(18, rank, 128), shape(14 + ny * tiles_z, rank, 128)),
        (mom, halo, *y1, *y2, line, *extra),
    )
    if nx == 2:
        beside = [from_shift(send, "gx", nx, 1)]
    else:
        beside = [from_shift(send, "gx", nx, -1), from_shift(send, "gx", nx, 1)]
    y3 = [from_shift(y_high, "gy", ny, -1), from_shift(y_low, "gy", ny, 1)]
    extra = [from_shift(send[14:], "gx", nx, s) for s in range(2, nx - 1)]

    windows = shape(5 * (bz + 4) * (by + 4), rank, 128)
    columns = shape(5 * 5 * 6, rank, 128)
    near, shifts, ones, corner_weights, lifted = run(
        part(near_kernel),
        (field, windows, columns, shape(2, 2, pts, 3 * pts), shape((xs - 1) * 4, rank, 128)),
        (near_table, near_blocks, near, transfer, cz_prev, cz_next, *y2, *sources, one),
        smem=(0,),
        aliases={2: 0},
        scratch=[
            pltpu.VMEM((2, by + 2, (bx + 2) * rhs, pts), BF16),
            pltpu.SMEM((stencil,), jnp.int32),
        ],
        limit=16,
        flops=2 * bx * by * bz * rhs * pts * pts * 9,
    )
    args = (
        far_table,
        live,
        near,
        corner_weights,
        leaf_basis,
        *weights,
        shifts,
        ones,
        *beside,
        *y1,
        *y2,
        *y3,
        lifted,
        send,
        *extra,
    )
    potentials, _, _ = run(
        part(final_kernel),
        (shape(bx, by, bz, rhs, pts, dtype=F32), windows, columns),
        args,
        anywhere=(0,),
        hbm_out=(0,),
        aliases={9: 1, 10: 2},
        limit=24,
        scratch=[
            pltpu.VMEM((2, 2, bx * rhs, pts), F32),
            pltpu.VMEM((bz, bx, by, rhs, pts), F32),
            pltpu.SMEM(far_table.shape, jnp.int32),
            pltpu.SemaphoreType.DMA((bz + 1,)),
        ],
    )
    return potentials


def solution(mesh):
    in_specs = (
        P("gx", "gy", "gz", None, None),
        P("gx", "gy", "gz"),
        P(),
        P(),
        P(),
        P(),
        P(),
        P(),
        P(),
    )
    out_specs = P("gx", "gy", "gz", None, None)

    return jax.shard_map(body, mesh=mesh, in_specs=in_specs, out_specs=out_specs, check_vma=False)
```
